32 devices in a mesh: shard: 2 (over x), replica: 16 (over z, y, core).
Axes of the slice: x: 2, y: 2, z: 4, core: 2. Of those that a mesh axis runs over, the one named last changes fastest.
Arguments:
- x_in: bfloat16 [32, 128, 2048], P(('shard', 'replica')), may hold values from -6 to 6
- cotangent: bfloat16 [32, 128, 2048], P(('shard', 'replica')), may hold values from -6 to 6
- w_query: bfloat16 [2048, 1024], P('shard'), may hold values from -0.088388348 to 0.088388348
- w_key: bfloat16 [2048, 1024], P('shard'), may hold values from -0.088388348 to 0.088388348
- w_value: bfloat16 [2048, 1024], P('shard'), may hold values from -0.125 to 0.125
- w_out: bfloat16 [1024, 2048], P('shard'), may hold values from -0.1875 to 0.1875
- w_gate: bfloat16 [2048, 4096], P('shard'), may hold values from -0.125 to 0.125
- w_up: bfloat16 [2048, 4096], P('shard'), may hold values from -0.125 to 0.125
- w_down: bfloat16 [4096, 2048], P('shard'), may hold values from -0.09375 to 0.09375
- gain_query: bfloat16 [1024], P('shard'), may hold values from 0.5 to 5
- gain_key: bfloat16 [1024], P('shard'), may hold values from 0.5 to 5
- gain_attn: bfloat16 [2048], P('shard'), may hold values from 0.5 to 1.5
- gain_mlp: bfloat16 [2048], P('shard'), may hold values from 0.5 to 1.5
Outputs:
- output: bfloat16 [32, 128, 2048], P(('shard', 'replica'))
- grad_input: float32 [32, 128, 2048], P(('shard', 'replica'))
- grad_w_query: float32 [2048, 1024], P(('shard', 'replica'))
- grad_w_key: float32 [2048, 1024], P(('shard', 'replica'))
- grad_w_value: float32 [2048, 1024], P(('shard', 'replica'))
- grad_w_out: float32 [1024, 2048], P(('shard', 'replica'))
- grad_w_gate: float32 [2048, 4096], P(('shard', 'replica'))
- grad_w_up: float32 [2048, 4096], P(('shard', 'replica'))
- grad_w_down: float32 [4096, 2048], P(('shard', 'replica'))
- grad_gain_query: float32 [1024], P(('shard', 'replica'))
- grad_gain_key: float32 [1024], P(('shard', 'replica'))
- grad_gain_attn: float32 [2048], P(('shard', 'replica'))
- grad_gain_mlp: float32 [2048], P(('shard', 'replica'))
The draws below stay inside these ranges and needn't reach their ends.
All inputs are finite; a program needn't handle non-finite values.
Results may differ from the reference program's by a relative error of at most 0.018.
Values may be sent and summed in bfloat16 or wider, within the bound.
A program may use at most 512 MiB of HBM per device.

```python
import math
import jax
import jax.numpy as jnp
from jax import lax

D = 2048
HD = 128
HEADS = 8
FF = 4096
LEN = 128
ATT = 1024
SEQS = 32


def query_key_weights(key):
    base = jax.random.fold_in(key, 101)
    shared = jax.random.normal(jax.random.fold_in(base, 1), (D, HEADS * HD), jnp.float32)
    independent = jax.random.normal(jax.random.fold_in(base, 2), (D, HEADS * HD), jnp.float32)
    return (shared, independent)


def draw_w_query(key, part):
    shared, independent = query_key_weights(key)
    limit = 4.0 * D ** (-0.5)
    return jnp.clip(shared * D ** (-0.5), -limit, limit).astype(jnp.bfloat16)


def draw_w_key(key, part):
    shared, independent = query_key_weights(key)
    limit = 4.0 * D ** (-0.5)
    key_mix = independent
    return jnp.clip(key_mix * D ** (-0.5), -limit, limit).astype(jnp.bfloat16)


def head_gains(key, salt):
    base = jax.random.fold_in(key, 202)
    jitter = jax.random.normal(jax.random.fold_in(base, salt), (HEADS * HD,), jnp.float32)
    values = jnp.clip(1.0 + 0.1 * jitter, 0.5, 1.5)
    return values


def draw_gain_query(key, part):
    return head_gains(key, 3).astype(jnp.bfloat16)


def draw_gain_key(key, part):
    return head_gains(key, 4).astype(jnp.bfloat16)


def spiked(array, rng, source, target, blocks, factor):
    def block_of(dim):
        return (jnp.arange(array.shape[dim]) // (array.shape[dim] // blocks)).reshape((-1,) + (1,) * (array.ndim - 1 - dim))

    one_side = jax.random.permutation(rng, blocks)[block_of(target)]
    far = (block_of(target) + blocks // 2) % blocks
    return jnp.where((block_of(source) == one_side) | (block_of(source) == far), factor * array, array)


def shard_levels(own_key, shape, split, low, largest):
    factor_of, own = 1.0, jax.random.fold_in(own_key, 6)
    for dim, parts in split:
        heights = jnp.exp(jax.random.uniform(jax.random.fold_in(own, dim), (parts,), jnp.float32, low / len(split), largest / len(split)))
        factor_of = factor_of * jnp.repeat(heights, shape[dim] // parts).reshape([-1 if axis == dim else 1 for axis in range(len(shape))])
    return factor_of


def gaussian(rng, shape, width, reach, cuts=(), dtype=jnp.bfloat16):
    array = width * jax.random.normal(rng, shape, jnp.float32)
    if cuts:
        array = array * shard_levels(rng, shape, cuts, -0.22, 0.18)
    return jnp.clip(array, -reach, reach).astype(dtype)


def gaussian_with(stream_key, dims, width, bound, cuts, heavy, dtype=jnp.bfloat16):
    array = width * jax.random.normal(stream_key, dims, jnp.float32)
    if cuts:
        array = array * shard_levels(stream_key, dims, cuts, -0.22, 0.18)
    return jnp.clip(spiked(array, jax.random.fold_in(stream_key, 3), *heavy), -bound, bound).astype(dtype)


def setup_inputs(seed: int = 0) -> dict:
    splits = jax.random.split(jax.random.key(seed), 14)
    x_in = gaussian_with(splits[0], (SEQS, LEN, D), 1.0, 6.0, ((0, 32),), (0, 2, 32, 2.75))
    cotangent = gaussian_with(splits[1], (SEQS, LEN, D), 1.0, 6.0, ((0, 32),), (0, 2, 32, 2.75))
    w_query = draw_w_query(jax.random.fold_in(splits[13], 71), 0)
    w_key = draw_w_key(jax.random.fold_in(splits[13], 71), 0)
    w_value = gaussian(splits[4], (D, ATT), D ** -0.5, 0.125, ((0, 2),))
    w_out = gaussian(splits[5], (ATT, D), ATT ** -0.5, 0.1875, ((0, 2),))
    w_gate = gaussian(splits[6], (D, FF), D ** -0.5, 0.125, ((0, 2),))
    w_up = gaussian(splits[7], (D, FF), D ** -0.5, 0.125, ((0, 2),))
    w_down = gaussian(splits[8], (FF, D), FF ** -0.5, 0.09375, ((0, 2),))
    gain_query = draw_gain_query(jax.random.fold_in(splits[13], 71), 0)
    gain_key = draw_gain_key(jax.random.fold_in(splits[13], 71), 0)
    gain_attn = jnp.clip(1.0 + 0.1 * jax.random.normal(splits[11], (D,), jnp.float32), 0.5, 1.5).astype(jnp.bfloat16)
    gain_mlp = jnp.clip(1.0 + 0.1 * jax.random.normal(splits[12], (D,), jnp.float32), 0.5, 1.5).astype(jnp.bfloat16)
    return dict(x_in=x_in, cotangent=cotangent, w_query=w_query, w_key=w_key, w_value=w_value, w_out=w_out, w_gate=w_gate, w_up=w_up, w_down=w_down, gain_query=gain_query, gain_key=gain_key, gain_attn=gain_attn, gain_mlp=gain_mlp)


eps_norm = 1e-06
rope_theta = 500000.0

def rope_tables(length, half):
    position = jnp.arange(length).astype(jnp.float32)[:, None]
    exponent = jnp.arange(half).astype(jnp.float32) * (1.0 / half)
    angle = position * rope_theta ** (-exponent)
    return (jnp.cos(angle), jnp.sin(angle))

def rotate(field, wave_cos, wave_sin):
    half = field.shape[-1] // 2
    first_half = field[..., :half]
    second_half = field[..., half:]
    cos_part = wave_cos[None, :, None, :]
    sin_part = wave_sin[None, :, None, :]
    return jnp.concatenate([first_half * cos_part - second_half * sin_part, second_half * cos_part + first_half * sin_part], axis=-1)

def unrotate(field, wave_cos, wave_sin):
    half = field.shape[-1] // 2
    first_half = field[..., :half]
    second_half = field[..., half:]
    cos_part = wave_cos[None, :, None, :]
    sin_part = wave_sin[None, :, None, :]
    return jnp.concatenate([first_half * cos_part + second_half * sin_part, second_half * cos_part - first_half * sin_part], axis=-1)

def rms_scale(field):
    return lax.rsqrt(lax.optimization_barrier(jnp.mean(field * field, axis=-1, keepdims=True)) + eps_norm)

def norm_back(grad_out, field, scale, gain):
    weighted = grad_out * gain
    inner = lax.optimization_barrier(jnp.mean(weighted * field, axis=-1, keepdims=True))
    grad_field = scale * weighted - field * scale ** 3 * inner
    grad_gain = lax.optimization_barrier(jnp.sum(grad_out * field * scale, axis=0))
    return (grad_field, grad_gain)

def matmul(left, right):
    return jnp.dot(left, right, preferred_element_type=jnp.float32)

def block_pass(x_block, cot_block, w_query, w_key, w_value, w_out, w_gate, w_up, w_down, gain_query, gain_key, gain_attn, gain_mlp):
    seq_count, length, model_width = x_block.shape
    att_width = w_query.shape[1]
    head_count = att_width // HD
    four_shape = (seq_count, length, head_count, HD)
    token_rows = x_block.reshape(seq_count * length, model_width)
    wave_cos, wave_sin = rope_tables(length, HD // 2)
    causal = jnp.arange(length)[:, None] >= jnp.arange(length)[None, :]
    g_query = gain_query.astype(jnp.float32)
    g_key = gain_key.astype(jnp.float32)
    g_attn = gain_attn.astype(jnp.float32)
    g_mlp = gain_mlp.astype(jnp.float32)
    query_proj = matmul(token_rows, w_query)
    query_scale = rms_scale(query_proj)
    query_normed = query_proj * query_scale * g_query
    key_proj = matmul(token_rows, w_key)
    key_scale = rms_scale(key_proj)
    key_normed = key_proj * key_scale * g_key
    value_four = matmul(token_rows, w_value).astype(jnp.bfloat16).reshape(four_shape)
    query_rot = rotate(query_normed.reshape(four_shape), wave_cos, wave_sin).astype(jnp.bfloat16)
    key_rot = rotate(key_normed.reshape(four_shape), wave_cos, wave_sin).astype(jnp.bfloat16)
    scores = jnp.einsum('sqhd,skhd->shqk', query_rot.astype(jnp.float32), key_rot.astype(jnp.float32)) / math.sqrt(HD)
    scores = jnp.where(causal, scores, -jnp.inf)
    row_peak = lax.optimization_barrier(jnp.max(scores, axis=-1, keepdims=True))
    log_total = row_peak + jnp.log(lax.optimization_barrier(jnp.sum(jnp.exp(scores - row_peak), axis=-1, keepdims=True)))
    probs = jnp.exp(scores - log_total)
    probs_low = probs.astype(jnp.bfloat16)
    attn_mixed = jnp.einsum('shqk,skhd->sqhd', probs_low.astype(jnp.float32), value_four.astype(jnp.float32))
    attn_mixed = attn_mixed.astype(jnp.bfloat16).reshape(-1, att_width)
    attn_proj = matmul(attn_mixed, w_out)
    attn_scale = rms_scale(attn_proj)
    residual = token_rows.astype(jnp.float32) + attn_proj * attn_scale * g_attn
    residual_low = residual.astype(jnp.bfloat16)
    gate_proj = matmul(residual_low, w_gate)
    up_proj = matmul(residual_low, w_up)
    gate_sigmoid = jax.nn.sigmoid(gate_proj)
    gate_silu = gate_proj * gate_sigmoid
    hidden = (gate_silu * up_proj).astype(jnp.bfloat16)
    down_proj = matmul(hidden, w_down)
    down_scale = rms_scale(down_proj)
    output = residual + down_proj * down_scale * g_mlp
    grad_output = cot_block.reshape(-1, model_width).astype(jnp.float32)
    grad_down, grad_gain_mlp = norm_back(grad_output, down_proj, down_scale, g_mlp)
    grad_down = grad_down.astype(jnp.bfloat16)
    grad_w_down = matmul(hidden.T, grad_down)
    grad_hidden = matmul(grad_down, w_down.T)
    grad_gate = (grad_hidden * up_proj * gate_sigmoid * (1.0 + gate_proj * (1.0 - gate_sigmoid))).astype(jnp.bfloat16)
    grad_up = (grad_hidden * gate_silu).astype(jnp.bfloat16)
    grad_w_gate = matmul(residual_low.T, grad_gate)
    grad_w_up = matmul(residual_low.T, grad_up)
    grad_residual = grad_output + matmul(grad_gate, w_gate.T) + matmul(grad_up, w_up.T)
    grad_attn, grad_gain_attn = norm_back(grad_residual, attn_proj, attn_scale, g_attn)
    grad_attn = grad_attn.astype(jnp.bfloat16)
    grad_w_out = matmul(attn_mixed.T, grad_attn)
    grad_mixed = matmul(grad_attn, w_out.T).astype(jnp.bfloat16).reshape(four_shape)
    grad_value = jnp.einsum('shqk,sqhd->skhd', probs_low.astype(jnp.float32), grad_mixed.astype(jnp.float32)).astype(jnp.bfloat16)
    grad_probs = jnp.einsum('sqhd,skhd->shqk', grad_mixed.astype(jnp.float32), value_four.astype(jnp.float32))
    grad_scores = probs * (grad_probs - lax.optimization_barrier(jnp.sum(probs * grad_probs, axis=-1, keepdims=True)))
    grad_scores = (grad_scores / math.sqrt(HD)).astype(jnp.bfloat16)
    grad_qrot = jnp.einsum('shqk,skhd->sqhd', grad_scores.astype(jnp.float32), key_rot.astype(jnp.float32))
    grad_krot = jnp.einsum('shqk,sqhd->skhd', grad_scores.astype(jnp.float32), query_rot.astype(jnp.float32))
    grad_qnormed = unrotate(grad_qrot, wave_cos, wave_sin).reshape(-1, att_width)
    grad_knormed = unrotate(grad_krot, wave_cos, wave_sin).reshape(-1, att_width)
    grad_query, grad_gain_query = norm_back(grad_qnormed, query_proj, query_scale, g_query)
    grad_key, grad_gain_key = norm_back(grad_knormed, key_proj, key_scale, g_key)
    grad_query = grad_query.astype(jnp.bfloat16)
    grad_key = grad_key.astype(jnp.bfloat16)
    grad_value = grad_value.reshape(-1, att_width)
    grad_w_query = matmul(token_rows.T, grad_query)
    grad_w_key = matmul(token_rows.T, grad_key)
    grad_w_value = matmul(token_rows.T, grad_value)
    grad_input = grad_residual + matmul(grad_query, w_query.T) + matmul(grad_key, w_key.T) + matmul(grad_value, w_value.T)
    grads = (grad_w_query, grad_w_key, grad_w_value, grad_w_out, grad_w_gate, grad_w_up, grad_w_down, grad_gain_query, grad_gain_key, grad_gain_attn, grad_gain_mlp)
    return (output.astype(jnp.bfloat16), grad_input, grads)

def reference(x_in, cotangent, w_query, w_key, w_value, w_out, w_gate, w_up, w_down, gain_query, gain_key, gain_attn, gain_mlp):
    seq_total = x_in.shape[0]
    block_size = math.gcd(seq_total, 32)
    block_count = seq_total // block_size
    x_blocks = x_in.reshape(block_count, block_size, LEN, D)
    cot_blocks = cotangent.reshape(block_count, block_size, LEN, D)
    weight_list = (w_query, w_key, w_value, w_out, w_gate, w_up, w_down, gain_query, gain_key, gain_attn, gain_mlp)
    initial = tuple((jnp.zeros(weight.shape, jnp.float32) for weight in weight_list))

    def step_block(carry, pair):
        out_block, grad_block, grads = block_pass(pair[0], pair[1], *weight_list)
        summed = jax.tree.map(lambda total, term: total + term, carry, grads)
        return (summed, (out_block, grad_block))
    totals, (out_blocks, grad_blocks) = lax.scan(step_block, initial, (x_blocks, cot_blocks))
    output = out_blocks.reshape(seq_total, LEN, D)
    grad_input = grad_blocks.reshape(seq_total, LEN, D)
    return (output, grad_input, totals[0], totals[1], totals[2], totals[3], totals[4], totals[5], totals[6], totals[7], totals[8], totals[9], totals[10])
```

```python
import math

import jax
import jax.numpy as jnp
from jax import lax
from jax.sharding import Mesh
from jax.sharding import PartitionSpec as P

HD = 128
TP = 4
CORES = 2

eps_norm = 1e-06
rope_theta = 500000.0

DATA = ("shard", "hi", "core")
ALL = ("shard", "hi", "t", "core")


def rope_tables(length, half):
    position = jnp.arange(length).astype(jnp.float32)[:, None]
    exponent = jnp.arange(half).astype(jnp.float32) * (1.0 / half)
    angle = position * rope_theta ** (-exponent)
    return (jnp.cos(angle), jnp.sin(angle))


def rotate(field, cos_part, sin_part):
    half = field.shape[-1] // 2
    a = field[..., :half]
    b = field[..., half:]
    return jnp.concatenate([a * cos_part - b * sin_part, b * cos_part + a * sin_part], axis=-1)


def matmul(left, right):
    return jnp.dot(left, right, preferred_element_type=jnp.float32)


def matmul_nt(left, right):
    return lax.dot_general(left, right, (((1,), (1,)), ((), ())), preferred_element_type=jnp.float32)


def matmul_tn(left, right):
    return lax.dot_general(left, right, (((0,), (0,)), ((), ())), preferred_element_type=jnp.float32)


def body(x_in, cotangent, w_query, w_key, w_value, w_out, w_gate, w_up, w_down,
         gain_query, gain_key, gain_attn, gain_mlp):
    bf16, f32 = jnp.bfloat16, jnp.float32
    t = lax.axis_index("t")
    core = lax.axis_index("core")
    shards = lax.axis_size("shard")
    his = lax.axis_size("hi")
    seqs, length, width = x_in.shape
    tokens = seqs * length
    att = w_query.shape[1]
    ff = w_gate.shape[1]
    heads_here = att // HD // TP

    def at(array, axis, index):
        return lax.dynamic_index_in_dim(array, index, axis, keepdims=False)

    def head_cols(w):
        return at(w.reshape(w.shape[0], heads_here, TP, HD), 2, t).reshape(w.shape[0], heads_here * HD)

    def hidden_cols(w):
        return at(w.reshape(w.shape[0], shards, his, TP, -1), 3, t).reshape(w.shape[0], ff // TP)

    def whole(block):
        rows = block.shape[0] // CORES
        piece = lax.dynamic_slice_in_dim(block, core * rows, rows, 0)
        return lax.all_gather(piece, ("shard", "core"), axis=0, tiled=True)

    gains = lax.all_gather(jnp.concatenate([gain_query, gain_key, gain_attn, gain_mlp]), "shard", axis=0)
    na, nd = gain_query.shape[0], gain_attn.shape[0]
    g_query = gains[:, :na].reshape(-1).astype(f32)
    g_key = gains[:, na:2 * na].reshape(-1).astype(f32)
    g_attn = gains[:, 2 * na:2 * na + nd].reshape(-1).astype(f32)
    g_mlp = gains[:, 2 * na + nd:].reshape(-1).astype(f32)
    g_query = at(g_query.reshape(heads_here, TP, HD), 1, t).reshape(-1)
    g_key = at(g_key.reshape(heads_here, TP, HD), 1, t).reshape(-1)

    rows = x_in.reshape(tokens, width)
    x_all = lax.all_gather(rows, "t", axis=0, tiled=True)
    w_qkv = whole(jnp.concatenate([head_cols(w_query), head_cols(w_key), head_cols(w_value)], axis=1))
    w_o = whole(at(w_out.reshape(heads_here // shards, TP, HD, width), 1, t).reshape(-1, width))
    w_gu = whole(jnp.concatenate([hidden_cols(w_gate), hidden_cols(w_up)], axis=1))
    w_d = whole(at(w_down.reshape(his, TP, -1, width), 1, t).reshape(-1, width))

    ha = heads_here * HD
    four = (TP * seqs, length, heads_here, HD)
    wave_cos, wave_sin = rope_tables(length, HD // 2)
    wave_cos = wave_cos[None, :, None, :]
    wave_sin = wave_sin[None, :, None, :]
    causal = jnp.arange(length)[:, None] >= jnp.arange(length)[None, :]

    qkv = matmul(x_all, w_qkv)
    q_proj, k_proj = qkv[:, :ha], qkv[:, ha:2 * ha]
    value = qkv[:, 2 * ha:].astype(bf16).reshape(four)
    squares = jnp.stack([jnp.sum(q_proj * q_proj, -1), jnp.sum(k_proj * k_proj, -1)])
    squares = lax.psum(squares, "t")
    scales = lax.rsqrt(squares / att + eps_norm)
    q_scale, k_scale = scales[0][:, None], scales[1][:, None]
    q_rot = rotate((q_proj * q_scale * g_query).reshape(four), wave_cos, wave_sin).astype(bf16)
    k_rot = rotate((k_proj * k_scale * g_key).reshape(four), wave_cos, wave_sin).astype(bf16)
    scores = jnp.einsum("sqhd,skhd->shqk", q_rot, k_rot, preferred_element_type=f32) / math.sqrt(HD)
    scores = jnp.where(causal, scores, -jnp.inf)
    peak = jnp.max(scores, axis=-1, keepdims=True)
    log_total = peak + jnp.log(jnp.sum(jnp.exp(scores - peak), axis=-1, keepdims=True))
    probs = jnp.exp(scores - log_total)
    probs_low = probs.astype(bf16)
    mixed = jnp.einsum("shqk,skhd->sqhd", probs_low, value, preferred_element_type=f32)
    mixed = mixed.astype(bf16).reshape(-1, ha)

    def scatter(partial):
        return lax.psum_scatter(partial.astype(bf16), "t", scatter_dimension=0, tiled=True).astype(f32)

    def rms_scale(field):
        return lax.rsqrt(jnp.mean(field * field, axis=-1, keepdims=True) + eps_norm)

    def norm_back(grad_out, field, scale, gain):
        weighted = grad_out * gain
        inner = jnp.mean(weighted * field, axis=-1, keepdims=True)
        return scale * weighted - field * scale**3 * inner, jnp.sum(grad_out * field * scale, axis=0)

    attn_proj = scatter(matmul(mixed, w_o))
    attn_scale = rms_scale(attn_proj)
    residual = rows.astype(f32) + attn_proj * attn_scale * g_attn
    res_all = lax.all_gather(residual.astype(bf16), "t", axis=0, tiled=True)
    gu = matmul(res_all, w_gu)
    fh = ff // TP
    gate, up = gu[:, :fh], gu[:, fh:]
    sig = jax.nn.sigmoid(gate)
    silu = gate * sig
    hidden = (silu * up).astype(bf16)
    down = scatter(matmul(hidden, w_d))
    down_scale = rms_scale(down)
    output = residual + down * down_scale * g_mlp

    cot = cotangent.reshape(tokens, width).astype(f32)
    grad_down, gg_mlp = norm_back(cot, down, down_scale, g_mlp)
    gd_all = lax.all_gather(grad_down.astype(bf16), "t", axis=0, tiled=True)
    gw_down = matmul_tn(hidden, gd_all)
    grad_hidden = matmul_nt(gd_all, w_d)
    grad_gate = (grad_hidden * up * sig * (1.0 + gate * (1.0 - sig))).astype(bf16)
    grad_up = (grad_hidden * silu).astype(bf16)
    grad_gu = jnp.concatenate([grad_gate, grad_up], axis=1)
    gw_gu = matmul_tn(res_all, grad_gu)
    grad_res = cot + scatter(matmul_nt(grad_gu, w_gu))

    grad_attn, gg_attn = norm_back(grad_res, attn_proj, attn_scale, g_attn)
    ga_all = lax.all_gather(grad_attn.astype(bf16), "t", axis=0, tiled=True)
    gw_out = matmul_tn(mixed, ga_all)
    grad_mixed = matmul_nt(ga_all, w_o).astype(bf16).reshape(four)
    grad_value = jnp.einsum("shqk,sqhd->skhd", probs_low, grad_mixed, preferred_element_type=f32).astype(bf16)
    grad_probs = jnp.einsum("sqhd,skhd->shqk", grad_mixed, value, preferred_element_type=f32)
    grad_scores = probs * (grad_probs - jnp.sum(probs * grad_probs, axis=-1, keepdims=True))
    grad_scores = (grad_scores / math.sqrt(HD)).astype(bf16)
    grad_q = jnp.einsum("shqk,skhd->sqhd", grad_scores, k_rot, preferred_element_type=f32)
    grad_k = jnp.einsum("shqk,sqhd->skhd", grad_scores, q_rot, preferred_element_type=f32)
    grad_q = rotate(grad_q, wave_cos, -wave_sin).reshape(-1, ha)
    grad_k = rotate(grad_k, wave_cos, -wave_sin).reshape(-1, ha)
    gg_query = jnp.sum(grad_q * q_proj * q_scale, axis=0)
    gg_key = jnp.sum(grad_k * k_proj * k_scale, axis=0)
    wq_, wk_ = grad_q * g_query, grad_k * g_key
    inner = lax.psum(jnp.stack([jnp.sum(wq_ * q_proj, -1), jnp.sum(wk_ * k_proj, -1)]), "t") / att
    gq = (q_scale * wq_ - q_proj * q_scale**3 * inner[0][:, None]).astype(bf16)
    gk = (k_scale * wk_ - k_proj * k_scale**3 * inner[1][:, None]).astype(bf16)
    grad_qkv = jnp.concatenate([gq, gk, grad_value.reshape(-1, ha)], axis=1)
    gw_qkv = matmul_tn(x_all, grad_qkv)
    grad_input = grad_res + scatter(matmul_nt(grad_qkv, w_qkv))

    def reduce_rows(grad):
        own = grad.shape[0] // (shards * his * TP * CORES)
        pieces = grad.astype(bf16).reshape(shards, his, TP, CORES, own, -1).transpose(0, 1, 3, 2, 4, 5)
        pieces = pieces.reshape(shards * his * CORES * TP * own, -1)
        mine = lax.psum_scatter(pieces, DATA, scatter_dimension=0, tiled=True)
        mine = lax.all_to_all(mine.reshape(TP, own, -1), "t", 0, 0)
        return mine.astype(f32)

    r_gu = reduce_rows(gw_gu)
    own = r_gu.shape[1]

    def hidden_out(block):
        return block.reshape(TP, own, shards, his, -1).transpose(1, 2, 3, 0, 4).reshape(own, ff)

    r_gate, r_up = hidden_out(r_gu[..., :fh]), hidden_out(r_gu[..., fh:])
    r_qkv = reduce_rows(gw_qkv)

    def head_out(block):
        return block.reshape(TP, own, heads_here, HD).transpose(1, 2, 0, 3).reshape(own, att)

    r_down = lax.psum_scatter(gw_down.astype(bf16), DATA, scatter_dimension=0, tiled=True).astype(f32)
    padded = jnp.zeros((shards, heads_here // shards, TP, HD, width), bf16)
    padded = lax.dynamic_update_index_in_dim(
        padded, gw_out.astype(bf16).reshape(shards, heads_here // shards, HD, width), t, 2)
    r_out = lax.psum_scatter(padded.reshape(att, width), ALL, scatter_dimension=0, tiled=True).astype(f32)

    def spread(vec):
        wide = jnp.zeros((heads_here, TP, HD), f32)
        return lax.dynamic_update_index_in_dim(wide, vec.reshape(heads_here, HD), t, 1).reshape(-1)

    devices = shards * his * TP * CORES
    small = jnp.concatenate([v.reshape(devices, -1) for v in (spread(gg_query), spread(gg_key), gg_attn, gg_mlp)], axis=1)
    small = lax.psum_scatter(small, ALL, scatter_dimension=0, tiled=True)[0]
    na, nd = att // devices, width // devices
    return (
        output.astype(bf16).reshape(x_in.shape),
        grad_input.reshape(x_in.shape),
        head_out(r_qkv[..., :ha]),
        head_out(r_qkv[..., ha:2 * ha]),
        head_out(r_qkv[..., 2 * ha:]),
        r_out,
        r_gate,
        r_up,
        r_down,
        small[:na],
        small[na:2 * na],
        small[2 * na:2 * na + nd],
        small[2 * na + nd:],
    )


def solution(mesh):
    shards, replicas = mesh.shape["shard"], mesh.shape["replica"]
    inner = Mesh(mesh.devices.reshape(shards, replicas // (TP * CORES), TP, CORES), ALL)
    token = P(ALL, None, None)
    weight = P("shard", None)
    return jax.shard_map(
        body,
        mesh=inner,
        in_specs=(token, token) + (weight,) * 7 + (P("shard"),) * 4,
        out_specs=(token, token) + (P(ALL, None),) * 7 + (P(ALL),) * 4,
        check_vma=False,
    )
```

```python
import functools
import math

import jax
import jax.numpy as jnp
from jax import lax
from jax.experimental import pallas as pl
from jax.experimental.pallas import tpu as pltpu
from jax.sharding import PartitionSpec as P

HD = 128
TP = 4
CORES = 2
CHUNKS = 4

eps_norm = 1e-06
rope_theta = 500000.0

bf16 = jnp.bfloat16
f32 = jnp.float32


def rope_tables(length, half):
    position = jnp.arange(length).astype(f32)[:, None]
    exponent = jnp.arange(half).astype(f32) * (1.0 / half)
    angle = position * rope_theta ** (-exponent)
    return (jnp.cos(angle), jnp.sin(angle))


def dot_nn(left, right):
    return lax.dot_general(left, right, (((1,), (0,)), ((), ())), preferred_element_type=f32)


def dot_nt(left, right, precision=None):
    return lax.dot_general(
        left, right, (((1,), (1,)), ((), ())), preferred_element_type=f32, precision=precision)


def dot_tn(left, right):
    return lax.dot_general(left, right, (((0,), (0,)), ((), ())), preferred_element_type=f32)


def mul_of(index, step):
    return pl.ds(pl.multiple_of(index * step, step), step)


def loop(count, step):
    lax.fori_loop(0, count, lambda i, c: (step(i), c)[1], 0)


class Dims:
    def __init__(self, length, width, att, ff, shards, replicas):
        self.L, self.D, self.att, self.ff = length, width, att, ff
        self.S, self.R = shards, replicas
        self.his = replicas // (TP * CORES)
        self.T = TP * length
        self.ha = att // TP
        self.fh = ff // TP
        self.unit = ff // (shards * replicas)
        self.own = width // (shards * replicas)
        self.own_o = att // (shards * replicas)
        self.pieces = HD // self.own_o
        self.levels = self.his.bit_length() - 1
        self.gains = 2 * HD + width
        self.ggs = 2 * width + 2 * att
        assert shards == 2 and self.his == 1 << self.levels and self.ha == shards * HD


def kernel(
    d,
    x_h, cot_h, wqkv_h, wo_h, wgu_h, wd_h, gain_v, cos_v, sin_v,
    out_h, gin_h, gu_h, qkv_h, down_h, o_h, gg_o,
    wqkv, wo, wgu, wd, gbuf, gat, gml,
    xall, rall, gdall, gaall, cot,
    qk, vb, qkrot, probs, mixed, gqkv, stat, statr,
    gu, hid, gg2,
    abuf, bbuf, cbuf, outb,
    acc, s1, s2, r1, r2, k2,
    stage, rc_gu, rc_d, rc_q, rc_o, rx_gu, rx_d, rx_q, rx_o, rh_gu, rh_d, rh_q, o_pc,
    gsum, grecv,
    ag_s, ag_r, rs_s, rs_r, w_s, w_r, wf_s, wf_r, loc, st_s, st_r,
    stg_s, c_s, c_r, x_s, x_r, h_s, h_r, a_s, a_r, o_s, o_r, gn_s, gn_r,
):
    L, D, T, ha, fh = d.L, d.D, d.T, d.ha, d.fh
    CW = D // CHUNKS
    HW = CW // 2
    s = lax.axis_index("shard")
    r = lax.axis_index("replica")
    hi, t, core = r // (TP * CORES), (r // CORES) % TP, r % CORES
    tz, ty = t // 2, t % 2
    t_y, t_z, t_d = tz * 2 + 1 - ty, (1 - tz) * 2 + ty, (1 - tz) * 2 + 1 - ty

    def rep(hi_, t_, core_):
        return hi_ * (TP * CORES) + t_ * CORES + core_

    dev_y, dev_z, dev_d = ((s, rep(hi, q, core)) for q in (t_y, t_z, t_d))
    dev_x = (1 - s, r)
    dev_c = (s, rep(hi, t, 1 - core))

    def send(src, dst, ssem, rsem, dev):
        return pltpu.make_async_remote_copy(
            src_ref=src, dst_ref=dst, send_sem=ssem, recv_sem=rsem, device_id=dev,
            device_id_type=pl.DeviceIdType.MESH)

    def blk(q):
        return mul_of(q, L)

    barrier = pltpu.get_barrier_semaphore()

    def greet(q):
        @pl.when(q != r)
        def _():
            pl.semaphore_signal(barrier, inc=1, device_id=(s, q), device_id_type=pl.DeviceIdType.MESH)

    loop(d.R, greet)
    pl.semaphore_signal(barrier, inc=1, device_id=dev_x, device_id_type=pl.DeviceIdType.MESH)
    pl.semaphore_wait(barrier, d.R)

    def ag_copies(buf, inst, i, src=None):
        own = buf.at[blk(t), pl.ds(i * CW, CW)]
        first = own if src is None else src.at[:, pl.ds(i * CW, CW)]
        ca, cb = pl.ds(i * CW, HW), pl.ds(i * CW + HW, HW)
        fy, fz = buf.at[blk(t_y), ca], buf.at[blk(t_z), cb]
        ends = ((first, own, dev_y), (first, own, dev_z), (fy, fy, dev_z), (fz, fz, dev_y))

        def copy(j):
            return send(ends[j][0], ends[j][1], ag_s.at[inst, i, j], ag_r.at[inst, i, j], ends[j][2])

        return copy

    def ag_start(buf, inst, i, src=None):
        c = ag_copies(buf, inst, i, src)
        c(0).start()
        c(1).start()

    def ag_fwd(buf, inst, i):
        c = ag_copies(buf, inst, i)
        c(0).wait_recv()
        c(2).start()
        c(1).wait_recv()
        c(3).start()

    def ag_done(buf, inst, i):
        c = ag_copies(buf, inst, i)
        c(2).wait_recv()
        c(3).wait_recv()

    def ag_drain(buf, inst):
        for i in range(CHUNKS):
            c = ag_copies(buf, inst, i)
            for j in range(4):
                c(j).wait_send()

    def ag(buf, inst, src=None, between=lambda i: None):
        ag_start(buf, inst, 0, src)
        ag_start(buf, inst, 1, src)
        for i in range(CHUNKS):
            ag_fwd(buf, inst, i)
            if i + 2 < CHUNKS:
                ag_start(buf, inst, i + 2, src)
            between(i)
        for i in range(CHUNKS):
            ag_done(buf, inst, i)
        ag_drain(buf, inst)

    def rs_copies(inst, i):
        ends = ((s1.at[i, 0:2], r1.at[i, 0:2], dev_y), (s1.at[i, 2:4], r1.at[i, 2:4], dev_z),
                (s2.at[i, 0], r2.at[i, 0], dev_z), (s2.at[i, 1], r2.at[i, 1], dev_y))

        def copy(j):
            return send(ends[j][0], ends[j][1], rs_s.at[inst, i, j], rs_r.at[inst, i, j], ends[j][2])

        return copy

    def rs_send(inst, i, dest):
        c = rs_copies(inst, i)
        step = L // 4

        def part(j):
            def rows(q):
                return pl.ds(pl.multiple_of(q * L + j * step, step), step)

            here = mul_of(j, step)
            s1[i, 0, here] = acc[rows(t_y), 0:HW].astype(bf16)
            s1[i, 1, here] = acc[rows(t_d), 0:HW].astype(bf16)
            s1[i, 2, here] = acc[rows(t_z), HW:CW].astype(bf16)
            s1[i, 3, here] = acc[rows(t_d), HW:CW].astype(bf16)
            k2[i, 0, here] = acc[rows(t_z), 0:HW]
            k2[i, 1, here] = acc[rows(t_y), HW:CW]
            dest[here, i * CW:(i + 1) * CW] = acc[rows(t), :]

        loop(4, part)
        c(0).start()
        c(1).start()

    def rs_fwd(inst, i, dest):
        c = rs_copies(inst, i)
        c(0).wait_recv()
        s2[i, 0] = (k2[i, 0] + r1[i, 1].astype(f32)).astype(bf16)
        c(2).start()
        c(1).wait_recv()
        s2[i, 1] = (k2[i, 1] + r1[i, 3].astype(f32)).astype(bf16)
        c(3).start()
        dest[:, i * CW:i * CW + HW] += r1[i, 0].astype(f32)
        dest[:, i * CW + HW:(i + 1) * CW] += r1[i, 2].astype(f32)

    def rs_done(inst, i, dest):
        c = rs_copies(inst, i)
        c(2).wait_recv()
        c(3).wait_recv()
        dest[:, i * CW:i * CW + HW] += r2[i, 0].astype(f32)
        dest[:, i * CW + HW:(i + 1) * CW] += r2[i, 1].astype(f32)

    def rs_drain(inst):
        for i in range(CHUNKS):
            c = rs_copies(inst, i)
            for j in range(4):
                c(j).wait_send()

    def rs(inst, dest, compute, between=lambda i: None):
        for i in range(CHUNKS):
            compute(i)
            rs_send(inst, i, dest)
        for i in range(CHUNKS):
            between(i)
            rs_fwd(inst, i, dest)
        between(CHUNKS)
        for i in range(CHUNKS):
            rs_done(inst, i, dest)
        rs_drain(inst)

    def split_place(half):
        return lambda s_, piece: s_ * half + piece * (half // 2)

    def down_place(s_, piece):
        return (piece * 2 + s_) * (d.his * d.unit)

    tables = (
        (wqkv_h, wqkv, split_place(D // 2), D // 4),
        (wo_h, wo, split_place(HD), HD // 2),
        (wgu_h, wgu, split_place(D // 2), D // 4),
        (wd_h, wd, down_place, d.his * d.unit),
    )

    def w_local(k, piece):
        src, buf, place, n = tables[k]
        return pltpu.make_async_copy(
            src.at[pl.ds(piece * n, n)], buf.at[pl.ds(pl.multiple_of(place(s, piece), n), n)], loc.at[k, piece])

    def w_cross(k):
        src, buf, place, n = tables[k]
        return send(src.at[mul_of(core, n)], buf.at[pl.ds(pl.multiple_of(place(s, core), n), n)],
                    w_s.at[k], w_r.at[k], dev_x)

    def w_share(k):
        _, buf, place, n = tables[k]
        here = buf.at[pl.ds(pl.multiple_of(place(1 - s, core), n), n)]
        return send(here, here, wf_s.at[k], wf_r.at[k], dev_c)

    own_x = pltpu.make_async_copy(x_h, xall.at[blk(t)], loc.at[4, 0])
    own_cot = pltpu.make_async_copy(cot_h, cot, loc.at[4, 1])
    own_gain = pltpu.make_async_copy(gain_v, gbuf.at[s], loc.at[5, 0])
    far_gain = send(gain_v, gbuf.at[s], w_s.at[4], w_r.at[4], dev_x)
    own_x.start()
    far_gain.start()
    w_cross(0).start()
    ag_start(xall, 0, 0, x_h)
    ag_start(xall, 0, 1, x_h)
    own_gain.start()
    for k in range(4):
        if k:
            w_cross(k).start()
        w_local(k, 0).start()
        w_local(k, 1).start()
    own_cot.start()

    def w_forward(k):
        w_cross(k).wait_recv()
        w_share(k).start()

    def w_ready(k):
        w_local(k, 0).wait()
        w_local(k, 1).wait()
        w_share(k).wait_recv()

    for i in range(CHUNKS):
        ag_fwd(xall, 0, i)
        if i + 2 < CHUNKS:
            ag_start(xall, 0, i + 2, x_h)
    w_forward(0)
    own_x.wait()
    own_gain.wait()
    far_gain.wait_recv()
    for q in range(2):
        gat[:, q * (D // 2):(q + 1) * (D // 2)] = gbuf[q, :, 2 * HD:2 * HD + D // 2]
        gml[:, q * (D // 2):(q + 1) * (D // 2)] = gbuf[q, :, 2 * HD + D // 2:]
    gsum[...] = jnp.zeros_like(gsum)
    for i in range(CHUNKS):
        ag_done(xall, 0, i)
    ag_drain(xall, 0)
    w_ready(0)
    w_forward(1)

    qk[:, 0:ha] = dot_nn(xall[...], wqkv[:, 0:ha])
    qk[:, ha:2 * ha] = dot_nn(xall[...], wqkv[:, ha:2 * ha])
    vb[...] = dot_nn(xall[...], wqkv[:, 2 * ha:]).astype(bf16)

    row8 = lax.broadcasted_iota(jnp.int32, (8, 2 * ha), 0)
    col8 = lax.broadcasted_iota(jnp.int32, (8, 2 * ha), 1)
    pick = jnp.where((row8 < 4) == (col8 < ha), 1.0, 0.0).astype(f32)
    HIGH = lax.Precision.HIGHEST

    def stat_sum(k, values):
        def part(b):
            stat[k, :, blk(b)] = dot_nt(pick, values(blk(b)), HIGH)

        loop(TP, part)
        copies = [send(stat.at[k], statr.at[k, j], st_s.at[k, j], st_r.at[k, j], dev)
                  for j, dev in enumerate((dev_y, dev_z, dev_d))]
        for c in copies:
            c.start()
        for c in copies:
            c.wait_recv()
        for c in copies:
            c.wait_send()
        return stat[k] + statr[k, 0] + statr[k, 1] + statr[k, 2]

    def squares(rows):
        v = qk[rows, :]
        return v * v

    stat[2] = lax.rsqrt(stat_sum(0, squares) / d.att + eps_norm)

    def columns(k, b):
        flat = stat[k, :, blk(b)]
        wide = jnp.concatenate([flat] * (L // 8), axis=0).T
        return wide[:, 0:1], wide[:, 4:5]

    def gain_of(which, h):
        return gbuf[h, :, which * HD:(which + 1) * HD]

    inv = 1.0 / math.sqrt(HD)
    heads = ha // HD

    def attend(b):
        rows = blk(b)
        scale = columns(2, b)
        cos, sin = cos_v[...], sin_v[...]
        above = lax.broadcasted_iota(jnp.int32, (L, L), 0) < lax.broadcasted_iota(jnp.int32, (L, L), 1)
        for h in range(heads):
            rot = []
            for which in range(2):
                at = pl.ds(which * ha + h * HD, HD)
                normed = qk[rows, at] * scale[which] * gain_of(which, h)
                turned = (normed * cos + pltpu.roll(normed, HD // 2, 1) * sin).astype(bf16)
                qkrot[rows, at] = turned
                rot.append(turned)
            scores = jnp.where(above, -jnp.inf, dot_nt(rot[0], rot[1]) * inv)
            peak = jnp.max(scores, axis=-1, keepdims=True)
            log_total = peak + jnp.log(jnp.sum(jnp.exp(scores - peak), axis=-1, keepdims=True))
            p = jnp.exp(scores - log_total)
            probs[b * heads + h] = p
            head = pl.ds(h * HD, HD)
            mixed[rows, head] = dot_nn(p.astype(bf16), vb[rows, head]).astype(bf16)

    loop(TP, attend)
    w_ready(1)

    def attn_chunk(i):
        acc[...] = dot_nn(mixed[...], wo[:, i * CW:(i + 1) * CW])

    rs(0, abuf, attn_chunk)

    BL = 16

    def residual_rows(j):
        rows = mul_of(j, BL)
        a = abuf[rows, :]
        scale = lax.rsqrt(jnp.mean(a * a, axis=-1, keepdims=True) + eps_norm)
        xr = xall[pl.ds(pl.multiple_of(t * L + j * BL, BL), BL), :].astype(f32)
        res = xr + a * scale * gat[...]
        cbuf[rows, :] = res
        rall[pl.ds(pl.multiple_of(t * L + j * BL, BL), BL), :] = res.astype(bf16)

    loop(L // BL, residual_rows)
    ag(rall, 1)
    w_forward(2)
    w_ready(2)

    NT = 256

    def gate_up(n):
        g_at, u_at = mul_of(n, NT), pl.ds(pl.multiple_of(fh + n * NT, NT), NT)
        gu[:, g_at] = dot_nn(rall[...], wgu[:, g_at])
        gu[:, u_at] = dot_nn(rall[...], wgu[:, u_at])

        def rows_of(j):
            rows = mul_of(j, 64)
            g, u = gu[rows, g_at], gu[rows, u_at]
            hid[rows, g_at] = (g * jax.nn.sigmoid(g) * u).astype(bf16)

        loop(T // 64, rows_of)

    loop(fh // NT, gate_up)
    w_forward(3)
    w_ready(3)

    def down_chunk(i):
        acc[...] = dot_nn(hid[...], wd[:, i * CW:(i + 1) * CW])

    rs(1, bbuf, down_chunk)
    own_cot.wait()

    def output_rows(j):
        rows = mul_of(j, BL)
        dn = bbuf[rows, :]
        scale = lax.rsqrt(jnp.mean(dn * dn, axis=-1, keepdims=True) + eps_norm)
        outb[rows, :] = (cbuf[rows, :] + dn * scale * gml[...]).astype(bf16)
        co = cot[rows, :].astype(f32)
        weighted = co * gml[...]
        inner = jnp.mean(weighted * dn, axis=-1, keepdims=True)
        gd = scale * weighted - dn * scale**3 * inner
        gdall[pl.ds(pl.multiple_of(t * L + j * BL, BL), BL), :] = gd.astype(bf16)
        gsum[:, D:2 * D] += jnp.sum(co * dn * scale, axis=0, keepdims=True)

    loop(L // BL, output_rows)
    put_out = pltpu.make_async_copy(outb, out_h, loc.at[5, 1])
    put_out.start()
    ag(gdall, 2)

    def hidden_back(n):
        g_at, u_at = mul_of(n, NT), pl.ds(pl.multiple_of(fh + n * NT, NT), NT)
        acc[:, 0:NT] = dot_nt(gdall[...], wd[mul_of(n, NT), :])

        def rows_of(j):
            rows = mul_of(j, 64)
            g, u, gh = gu[rows, g_at], gu[rows, u_at], acc[rows, 0:NT]
            sig = jax.nn.sigmoid(g)
            gg2[rows, g_at] = (gh * u * sig * (1.0 + g * (1.0 - sig))).astype(bf16)
            gg2[rows, u_at] = (gh * (g * sig)).astype(bf16)

        loop(T // 64, rows_of)

    loop(fh // NT, hidden_back)

    def res_chunk(i):
        acc[...] = dot_nt(gg2[...], wgu[i * CW:(i + 1) * CW, :])

    rs(2, cbuf, res_chunk)

    def attn_grad_rows(j):
        rows = mul_of(j, BL)
        gr = cbuf[rows, :] + cot[rows, :].astype(f32)
        cbuf[rows, :] = gr
        a = abuf[rows, :]
        scale = lax.rsqrt(jnp.mean(a * a, axis=-1, keepdims=True) + eps_norm)
        weighted = gr * gat[...]
        inner = jnp.mean(weighted * a, axis=-1, keepdims=True)
        ga = scale * weighted - a * scale**3 * inner
        gaall[pl.ds(pl.multiple_of(t * L + j * BL, BL), BL), :] = ga.astype(bf16)
        gsum[:, 0:D] += jnp.sum(gr * a * scale, axis=0, keepdims=True)

    loop(L // BL, attn_grad_rows)
    ag(gaall, 3)

    acc[:, 0:ha] = dot_nt(gaall[...], wo[...])

    def attend_back(b):
        rows = blk(b)
        scale = columns(2, b)
        cos, sin = cos_v[...], sin_v[...]
        for h in range(heads):
            head = pl.ds(h * HD, HD)
            gm = acc[rows, head].astype(bf16)
            p = probs[b * heads + h]
            gqkv[rows, pl.ds(2 * ha + h * HD, HD)] = dot_tn(p.astype(bf16), gm).astype(bf16)
            gp = dot_nt(gm, vb[rows, head])
            gs = p * (gp - jnp.sum(p * gp, axis=-1, keepdims=True))
            gs = (gs * inv).astype(bf16)
            turned = (dot_nn(gs, qkrot[rows, pl.ds(ha + h * HD, HD)]), dot_tn(gs, qkrot[rows, head]))
            for which in range(2):
                at = pl.ds(which * ha + h * HD, HD)
                gn = turned[which] * cos - pltpu.roll(turned[which], HD // 2, 1) * sin
                field = qk[rows, at]
                spot = pl.ds(pl.multiple_of(2 * D + which * d.att + t * ha + h * HD, HD), HD)
                gsum[:, spot] += jnp.sum(gn * field * scale[which], axis=0, keepdims=True)
                gu[rows, at] = gn * gain_of(which, h)

    loop(TP, attend_back)

    def products(rows):
        return gu[rows, 0:2 * ha] * qk[rows, :]

    stat[3] = stat_sum(1, products) / d.att

    def qk_back(b):
        rows = blk(b)
        scale, inner = columns(2, b), columns(3, b)
        for which in range(2):
            at = pl.ds(which * ha, ha)
            sc = scale[which]
            gqkv[rows, at] = (sc * gu[rows, at] - qk[rows, at] * (sc**3 * inner[which])).astype(bf16)

    loop(TP, qk_back)

    def in_chunk(i):
        acc[...] = dot_nt(gqkv[...], wqkv[i * CW:(i + 1) * CW, :])

    rs(3, bbuf, in_chunk)

    def input_rows(j):
        rows = mul_of(j, BL)
        bbuf[rows, :] += cbuf[rows, :]

    loop(L // BL, input_rows)
    put_gin = pltpu.make_async_copy(bbuf, gin_h, loc.at[6, 0])
    put_gin.start()

    half_q = 3 * ha // 2

    def left_of(ref):
        return lambda row, n: ref[:, pl.ds(pl.multiple_of(row, n), n)]

    def by_cols(left, right, width):
        def make(row, n, core_):
            return dot_tn(left(row, n), right[:, mul_of(core_, width)])
        return make

    def by_rows(left, right, height):
        def make(row, n, core_):
            return dot_tn(left(core_ * height + row, n), right[...])
        return make

    sets = (
        (by_rows(left_of(hid), gdall, fh // 2), rc_d, rx_d, rh_d, fh // 2, 128),
        (by_cols(left_of(rall), gg2, fh), rc_gu, rx_gu, rh_gu, D, 256),
        (by_cols(left_of(xall), gqkv, half_q), rc_q, rx_q, rh_q, D, 256),
        (by_cols(left_of(mixed), gaall, D // 2), rc_o, rx_o, None, ha, 128),
    )
    top = hi // max(d.his // 2, 1)

    def tile_row(k, j):
        rows, n = sets[k][4], sets[k][5]
        tiles = rows // 2 // n
        if k == 3 or tiles < 2:
            return j * n
        return ((j + (1 - top) * (tiles // 2)) % tiles) * n

    def core_copy(k, row, slot):
        buf, n = sets[k][1], sets[k][5]
        dst = buf.at[pl.ds(pl.multiple_of(row, n), n)]
        return send(stage_view(k, slot), dst, stg_s.at[slot], c_r.at[k, row // n], dev_c)

    def stage_view(k, slot):
        buf, n = sets[k][1], sets[k][5]
        return stage.at[slot, 0:n, 0:buf.shape[1]]

    def order(k):
        rows, n = sets[k][4], sets[k][5]
        half = rows // 2
        tiles = half // n
        out = [(1 - s) * half + tile_row(k, j) for j in range(tiles)]
        return out + [s * half + tile_row(k, j) for j in range(tiles)]

    slots = stage.shape[0]
    used = [0]

    def give(k):
        for row in order(k):
            slot = used[0] % slots
            c = core_copy(k, row, slot)
            if used[0] >= slots:
                c_prev = pending[used[0] - slots]
                c_prev.wait_send()
            n = sets[k][5]
            w = sets[k][1].shape[1]
            stage[slot, 0:n, 0:w] = sets[k][0](row, n, 1 - core).astype(bf16)
            c.start()
            pending.append(c)
            used[0] += 1

    pending = []

    def x_copy(k, j):
        buf, far, n = sets[k][1], sets[k][2], sets[k][5]
        half = sets[k][4] // 2
        row = tile_row(k, j)
        src = buf.at[pl.ds(pl.multiple_of((1 - s) * half + row, n), n)]
        return send(src, far.at[pl.ds(pl.multiple_of(row, n), n)], x_s.at[k, j], x_r.at[k, j], dev_x)

    def own_tile(k, row):
        buf, n = sets[k][1], sets[k][5]
        rows = pl.ds(pl.multiple_of(row, n), n)
        core_copy(k, row, 0).wait_recv()
        buf[rows, :] = (sets[k][0](row, n, core) + buf[rows, :].astype(f32)).astype(bf16)

    def take(k):
        rows, n = sets[k][4], sets[k][5]
        half = rows // 2
        tiles = half // n
        for j in range(tiles):
            own_tile(k, (1 - s) * half + tile_row(k, j))
            x_copy(k, j).start()
        for j in range(tiles):
            own_tile(k, s * half + tile_row(k, j))

    def x_add(k, j):
        buf, far, n = sets[k][1], sets[k][2], sets[k][5]
        half = sets[k][4] // 2
        row = tile_row(k, j)
        rows = pl.ds(pl.multiple_of(s * half + row, n), n)
        x_copy(k, j).wait_recv()
        buf[rows, :] = (buf[rows, :].astype(f32) + far[pl.ds(pl.multiple_of(row, n), n), :].astype(f32)).astype(bf16)

    def hi_parts(k):
        half = sets[k][4] // 2
        parts = []
        base, size, at = 0, half, 0
        for level in range(d.levels):
            size //= 2
            weight = d.his >> (level + 1)
            bit = (hi // weight) % 2
            parts.append((level, base + (1 - bit) * size, base + bit * size, size, at, hi + weight * (1 - 2 * bit)))
            base = base + bit * size
            at += size
        return parts, base, size

    def hi_copy(k, part):
        level, far_row, _, size, at, other = part
        half = sets[k][4] // 2
        src = sets[k][1].at[pl.ds(pl.multiple_of(s * half + far_row, size), size)]
        return send(src, sets[k][3].at[pl.ds(at, size)], h_s.at[k, level], h_r.at[k, level], (s, rep(other, t, core)))

    def hi_add(k, part, final=None):
        level, _, row, size, at, _ = part
        half = sets[k][4] // 2
        hi_copy(k, part).wait_recv()
        n = min(size, 64)

        def step(j):
            rows = pl.ds(pl.multiple_of(s * half + row + j * n, n), n)
            total = sets[k][1][rows, :].astype(f32) + sets[k][3][pl.ds(pl.multiple_of(at + j * n, n), n), :].astype(f32)
            if final is None:
                sets[k][1][rows, :] = total.astype(bf16)
            else:
                final[mul_of(j, n), :] = total

        loop(size // n, step)

    def a2a_copies(k, p):
        half = sets[k][4] // 2
        _, base, size = hi_parts(k)
        src = sets[k][1].at[pl.ds(pl.multiple_of(s * half + base + p * d.own, d.own), d.own)]
        dst = (gu_h if k == 1 else qkv_h).at[t * CORES + core]
        return src, dst

    me = t * CORES + core

    def a2a_start(k):
        for p in range(TP * CORES):
            src, dst = a2a_copies(k, p)

            @pl.when(me != p)
            def _():
                send(src, dst, a_s.at[k - 1, p], a_r.at[k - 1, me], (s, rep(hi, p // CORES, p % CORES))).start()

            @pl.when(me == p)
            def _():
                pltpu.make_async_copy(src, dst, a_r.at[k - 1, me]).start()

    def a2a_wait(k):
        for p in range(TP * CORES):
            src, _ = a2a_copies(k, p)
            target = (gu_h if k == 1 else qkv_h).at[p]
            pltpu.make_async_copy(src, target, a_r.at[k - 1, p]).wait()

            @pl.when(me != p)
            def _():
                send(src, target, a_s.at[k - 1, p], a_r.at[k - 1, me], (s, rep(hi, p // CORES, p % CORES))).wait_send()

    for k in range(4):
        give(k)
    for k in range(4):
        take(k)
    for c in pending[-slots:]:
        c.wait_send()
    for k in range(4):
        for j in range(sets[k][4] // 2 // sets[k][5]):
            x_add(k, j)
    parts = [hi_parts(k)[0] for k in range(3)]
    for level in range(d.levels):
        for k in range(3):
            hi_copy(k, parts[k][level]).start()
        for k in range(3):
            last = k == 0 and level == d.levels - 1
            hi_add(k, parts[k][level], abuf if last else None)
    if not d.levels:
        abuf[0:d.unit, :] = rc_d[pl.ds(pl.multiple_of(s * d.unit, d.unit), d.unit), :].astype(f32)
    put_down = pltpu.make_async_copy(abuf.at[0:d.unit], down_h, loc.at[6, 1])
    put_down.start()
    a2a_start(1)
    a2a_start(2)

    for p in range(d.pieces):
        o_pc[p] = rc_o[pl.ds(pl.multiple_of(s * HD + p * d.own_o, d.own_o), d.own_o), :]
    o_slot = hi * CORES + core
    for p in range(d.pieces):
        goal = t * d.pieces + p

        @pl.when(goal != r)
        def _():
            send(o_pc.at[p], o_h.at[o_slot], o_s.at[p], o_r.at[o_slot], (s, goal)).start()

        @pl.when(goal == r)
        def _():
            pltpu.make_async_copy(o_pc.at[p], o_h.at[o_slot], o_r.at[o_slot]).start()

    partners = [dev_c, dev_x]
    for level in range(d.levels):
        weight = d.his >> (level + 1)
        bit = (hi // weight) % 2
        partners.append((s, rep(hi + weight * (1 - 2 * bit), t, core)))
    partners += [dev_y, dev_z]
    for n, dev in enumerate(partners):
        c = send(gsum, grecv.at[n], gn_s.at[n], gn_r.at[n], dev)
        c.start()
        c.wait_send()
        c.wait_recv()
        gsum[...] += grecv[n]
    gg_o[...] = gsum[...]

    a2a_wait(1)
    a2a_wait(2)
    for q in range(d.his * CORES):
        pltpu.make_async_copy(o_pc.at[0], o_h.at[q], o_r.at[q]).wait()
    for p in range(d.pieces):
        goal = t * d.pieces + p

        @pl.when(goal != r)
        def _():
            send(o_pc.at[p], o_h.at[o_slot], o_s.at[p], o_r.at[o_slot], (s, goal)).wait_send()

    far_gain.wait_send()
    for k in range(4):
        w_cross(k).wait_send()
        w_share(k).wait_send()
        for j in range(sets[k][4] // 2 // sets[k][5]):
            x_copy(k, j).wait_send()
    for k in range(3):
        for part in parts[k]:
            hi_copy(k, part).wait_send()
    put_out.wait()
    put_gin.wait()
    put_down.wait()


def body(shards, replicas, x_in, cotangent, w_query, w_key, w_value, w_out, w_gate, w_up, w_down,
         gain_query, gain_key, gain_attn, gain_mlp):
    seqs, length, width = x_in.shape
    assert seqs == 1
    d = Dims(length, width, w_query.shape[1], w_gate.shape[1], shards, replicas)
    r = lax.axis_index("replica")
    s = lax.axis_index("shard")
    t = (r // CORES) % TP

    def at(array, axis, index):
        return lax.dynamic_index_in_dim(array, index, axis, keepdims=False)

    def head_cols(w):
        return at(w.reshape(w.shape[0], d.S, TP, HD), 2, t).reshape(w.shape[0], d.ha)

    def hidden_cols(w):
        picked = at(w.reshape(w.shape[0], d.S, d.his, TP, CORES, d.unit), 3, t)
        return picked.transpose(0, 3, 1, 2, 4).reshape(w.shape[0], d.fh)

    wqkv = jnp.concatenate([head_cols(w_query), head_cols(w_key), head_cols(w_value)], axis=1)
    wo = at(w_out.reshape(TP, HD, width), 0, t)
    wgu = jnp.concatenate([hidden_cols(w_gate), hidden_cols(w_up)], axis=1)
    wd = at(w_down.reshape(d.his, TP, CORES, d.unit, width), 1, t).transpose(1, 0, 2, 3).reshape(-1, width)
    gain = jnp.concatenate([at(gain_query.reshape(TP, HD), 0, t), at(gain_key.reshape(TP, HD), 0, t),
                            gain_attn, gain_mlp]).astype(f32)[None]
    cos, sin = rope_tables(length, HD // 2)
    cos = jnp.concatenate([cos, cos], axis=1)
    sin = jnp.concatenate([-sin, sin], axis=1)

    L, D, T, ha, fh = d.L, d.D, d.T, d.ha, d.fh
    CW = D // CHUNKS
    vm = pltpu.VMEM
    dma = pltpu.SemaphoreType.DMA
    any_ = pl.BlockSpec(memory_space=pl.ANY)
    vmem = pl.BlockSpec(memory_space=pltpu.VMEM)
    hi_rows = lambda n: max(n - n // d.his, 16)
    steps = 4 + d.levels
    scratch = [
        vm((D, 3 * ha), bf16), vm((ha, D), bf16), vm((D, 2 * fh), bf16), vm((fh, D), bf16),
        vm((2, 1, d.gains), f32), vm((1, D), f32), vm((1, D), f32),
        vm((T, D), bf16), vm((T, D), bf16), vm((T, D), bf16), vm((T, D), bf16), vm((L, D), bf16),
        vm((T, 2 * ha), f32), vm((T, ha), bf16), vm((T, 2 * ha), bf16), vm((TP * ha // HD, L, L), f32),
        vm((T, ha), bf16), vm((T, 3 * ha), bf16), vm((4, 8, T), f32), vm((2, 3, 8, T), f32),
        vm((T, 2 * fh), f32), vm((T, fh), bf16), vm((T, 2 * fh), bf16),
        vm((L, D), f32), vm((L, D), f32), vm((L, D), f32), vm((L, D), bf16),
        vm((T, CW), f32), vm((CHUNKS, 4, L, CW // 2), bf16), vm((CHUNKS, 2, L, CW // 2), bf16),
        vm((CHUNKS, 4, L, CW // 2), bf16), vm((CHUNKS, 2, L, CW // 2), bf16), vm((CHUNKS, 2, L, CW // 2), f32),
        vm((2, 256, D), bf16),
        vm((D, fh), bf16), vm((fh // 2, D), bf16), vm((D, 3 * ha // 2), bf16), vm((ha, D // 2), bf16),
        vm((D // 2, fh), bf16), vm((fh // 4, D), bf16), vm((D // 2, 3 * ha // 2), bf16), vm((ha // 2, D // 2), bf16),
        vm((hi_rows(D // 2), fh), bf16), vm((hi_rows(fh // 4), D), bf16), vm((hi_rows(D // 2), 3 * ha // 2), bf16),
        vm((d.pieces, d.own_o, D // 2), bf16),
        vm((1, d.ggs), f32), vm((steps, 1, d.ggs), f32),
        dma((4, CHUNKS, 4)), dma((4, CHUNKS, 4)), dma((4, CHUNKS, 4)), dma((4, CHUNKS, 4)),
        dma((5,)), dma((5,)), dma((4,)), dma((4,)), dma((7, 2)), dma((2, 3)), dma((2, 3)),
        dma((2,)), dma((4,)), dma((4, 8)), dma((4, 4)), dma((4, 4)),
        dma((3, max(d.levels, 1))), dma((3, max(d.levels, 1))),
        dma((2, TP * CORES)), dma((2, TP * CORES)), dma((d.pieces,)), dma((d.his * CORES,)), dma((steps,)), dma((steps,)),
    ]
    struct = jax.ShapeDtypeStruct
    results = pl.pallas_call(
        functools.partial(kernel, d),
        out_shape=(
            struct((L, D), bf16), struct((L, D), f32), struct((TP * CORES, d.own, fh), bf16),
            struct((TP * CORES, d.own, 3 * ha // 2), bf16), struct((d.unit, D), f32),
            struct((d.his * CORES, d.own_o, D // 2), bf16), struct((1, d.ggs), f32),
        ),
        in_specs=[any_] * 6 + [vmem] * 3,
        out_specs=(any_,) * 6 + (vmem,),
        scratch_shapes=scratch,
        compiler_params=pltpu.CompilerParams(
            collective_id=0, has_side_effects=True, vmem_limit_bytes=67043328),
        name="layer",
    )(x_in[0], cotangent[0], wqkv, wo, wgu, wd, gain, cos, sin)
    out, gin, gu, qkv, down, o, gg = results

    def hidden_out(block):
        spread = block.reshape(TP, d.own, CORES, d.S, d.his, d.unit).transpose(1, 3, 4, 0, 2, 5)
        return spread.reshape(d.own, d.ff).astype(f32)

    gu = gu.reshape(TP, CORES, d.own, fh)
    qkv = qkv.reshape(TP, CORES, d.own, 3, HD).transpose(2, 1, 3, 0, 4).reshape(d.own, 3, d.S, TP, HD)

    def head_out(k):
        return qkv[:, k].reshape(d.own, d.att).astype(f32)

    o = o.reshape(d.his, CORES, d.own_o, D // 2).astype(f32).sum(0).transpose(1, 0, 2).reshape(d.own_o, D)
    gg = gg[0]
    here = s * d.R + r

    def share(vec):
        n = vec.shape[0] // (d.S * d.R)
        return lax.dynamic_slice_in_dim(vec, here * n, n)

    def head_gain(vec):
        return share(vec.reshape(TP, d.S, HD).transpose(1, 0, 2).reshape(-1))

    return (
        out[None], gin[None], head_out(0), head_out(1), head_out(2), o,
        hidden_out(gu[:, 0]), hidden_out(gu[:, 1]), down,
        head_gain(gg[2 * D:2 * D + d.att]), head_gain(gg[2 * D + d.att:]), share(gg[:D]), share(gg[D:2 * D]),
    )


def solution(mesh):
    both = ("shard", "replica")
    token = P(both, None, None)
    weight = P("shard", None)
    return jax.shard_map(
        functools.partial(body, mesh.shape["shard"], mesh.shape["replica"]),
        mesh=mesh,
        in_specs=(token, token) + (weight,) * 7 + (P("shard"),) * 4,
        out_specs=(token, token) + (P(both, None),) * 7 + (P(both),) * 4,
        check_vma=False,
    )
```

```python
import functools
import math

import jax
import jax.numpy as jnp
import numpy as np
from jax import lax
from jax.experimental import pallas as pl
from jax.experimental.pallas import tpu as pltpu
from jax.sharding import PartitionSpec as P

HD = 128
TP = 4
CORES = 2
CHUNKS = 4

eps_norm = 1e-06
rope_theta = 500000.0

bf16 = jnp.bfloat16
f32 = jnp.float32


def rope_tables(length, half):
    position = np.arange(length).astype(np.float32)[:, None]
    exponent = np.arange(half).astype(np.float32) * np.float32(1.0 / half)
    angle = position * np.float32(rope_theta) ** (-exponent)
    return (np.cos(angle).astype(np.float32), np.sin(angle).astype(np.float32))


def dot_nn(left, right):
    return lax.dot_general(left, right, (((1,), (0,)), ((), ())), preferred_element_type=f32)


def dot_nt(left, right, precision=None):
    return lax.dot_general(
        left, right, (((1,), (1,)), ((), ())), preferred_element_type=f32, precision=precision)


def dot_tn(left, right):
    return lax.dot_general(left, right, (((0,), (0,)), ((), ())), preferred_element_type=f32)


def mul_of(index, step):
    return pl.ds(pl.multiple_of(index * step, step), step)


def loop(count, step, start=0):
    lax.fori_loop(start, count, lambda i, c: (step(i), c)[1], 0)


class Dims:
    def __init__(self, length, width, att, ff, shards, replicas):
        self.L, self.D, self.att, self.ff = length, width, att, ff
        self.S, self.R = shards, replicas
        self.his = replicas // (TP * CORES)
        self.T = TP * length
        self.ha = att // TP
        self.fh = ff // TP
        self.unit = ff // (shards * replicas)
        self.own = width // (shards * replicas)
        self.own_o = att // (shards * replicas)
        self.pieces = HD // self.own_o
        self.levels = self.his.bit_length() - 1
        self.gains = 2 * HD + width
        self.ggs = 2 * width + 2 * att
        self.direct = self.unit % 128 == 0
        assert shards == 2 and self.his == 1 << self.levels and self.levels > 0 and self.ha == shards * HD


def kernel(
    d,
    x_h, cot_h, wq_h, wk_h, wv_h, wo_h, wg_h, wu_h, wd_h, gain_v, cos_v, sin_v,
    out_h, gin_h, gu_h, qkv_h, down_h, o_h, gg_o,
    wqkv, wo, wgu, wd, gbuf, gat, gml,
    xall, rall, gdall, gaall, cot,
    qk, vb, qkrot, probs, mixed, gqkv, stat, statr,
    gu, hid, gg2,
    abuf, bbuf, cbuf, outb,
    acc, s1, s2, r1, r2, k2,
    stage_d, stage, rc_gu, rc_d, rc_q, rc_o, rx_gu, rx_d, rx_q, rx_o, rh_gu, rh_d, rh_q, o_pc,
    gsum, grecv,
    ag_s, ag_r, rs_s, rs_r, w_s, w_r, wf_s, wf_r, w_l, loc, st_s, st_r,
    stg_s, c_r, x_s, x_r, h0_s, h0_r, h_s, h_r, a_s, a_r, o_s, o_r, gn_s, gn_r,
):
    L, D, T, ha, fh, his, unit = d.L, d.D, d.T, d.ha, d.fh, d.his, d.unit
    CW = D // CHUNKS
    HW = CW // 2
    s = lax.axis_index("shard")
    r = lax.axis_index("replica")
    hi, t, core = r // (TP * CORES), (r // CORES) % TP, r % CORES
    tz, ty = t // 2, t % 2
    t_y, t_z, t_d = tz * 2 + 1 - ty, (1 - tz) * 2 + ty, (1 - tz) * 2 + 1 - ty

    def rep(hi_, t_, core_):
        return hi_ * (TP * CORES) + t_ * CORES + core_

    dev_y, dev_z, dev_d = ((s, rep(hi, q, core)) for q in (t_y, t_z, t_d))
    dev_x = (1 - s, r)
    dev_c = (s, rep(hi, t, 1 - core))

    def send(src, dst, ssem, rsem, dev):
        return pltpu.make_async_remote_copy(
            src_ref=src, dst_ref=dst, send_sem=ssem, recv_sem=rsem, device_id=dev,
            device_id_type=pl.DeviceIdType.MESH)

    def blk(q):
        return mul_of(q, L)

    def part(base, n):
        return pl.ds(pl.multiple_of(base, n), n)

    barrier = pltpu.get_barrier_semaphore()

    def greet(q):
        @pl.when(q != r)
        def _():
            pl.semaphore_signal(barrier, inc=1, device_id=(s, q), device_id_type=pl.DeviceIdType.MESH)

    loop(d.R, greet)
    pl.semaphore_signal(barrier, inc=1, device_id=dev_x, device_id_type=pl.DeviceIdType.MESH)
    pl.semaphore_wait(barrier, d.R)

    def ag_copies(buf, inst, i, src=None):
        own = buf.at[blk(t), mul_of(i, CW)]
        first = own if src is None else src.at[:, mul_of(i, CW)]
        ca, cb = mul_of(2 * i, HW), mul_of(2 * i + 1, HW)
        fy, fz = buf.at[blk(t_y), ca], buf.at[blk(t_z), cb]
        ends = ((first, own, dev_y), (first, own, dev_z), (fy, fy, dev_z), (fz, fz, dev_y))

        def copy(j):
            return send(ends[j][0], ends[j][1], ag_s.at[inst, i, j], ag_r.at[inst, i, j], ends[j][2])

        return copy

    def ag_start(buf, inst, i, src=None):
        c = ag_copies(buf, inst, i, src)
        c(0).start()
        c(1).start()

    def ag_fwd(buf, inst, i):
        c = ag_copies(buf, inst, i)
        c(0).wait_recv()
        c(2).start()
        c(1).wait_recv()
        c(3).start()

    def ag_done(buf, inst, i):
        c = ag_copies(buf, inst, i)
        c(2).wait_recv()
        c(3).wait_recv()

    def ag_drain(buf, inst):
        def wait(i):
            c = ag_copies(buf, inst, i)
            for j in range(4):
                c(j).wait_send()

        loop(CHUNKS, wait)

    def ag(buf, inst, src=None, between=lambda i: None):
        ag_start(buf, inst, 0, src)
        ag_start(buf, inst, 1, src)
        for i in range(CHUNKS):
            ag_fwd(buf, inst, i)
            if i + 2 < CHUNKS:
                ag_start(buf, inst, i + 2, src)
            between(i)
        for i in range(CHUNKS):
            ag_done(buf, inst, i)
        ag_drain(buf, inst)

    def rs_copies(inst, i):
        ends = ((s1.at[i, 0:2], r1.at[i, 0:2], dev_y), (s1.at[i, 2:4], r1.at[i, 2:4], dev_z),
                (s2.at[i, 0], r2.at[i, 0], dev_z), (s2.at[i, 1], r2.at[i, 1], dev_y))

        def copy(j):
            return send(ends[j][0], ends[j][1], rs_s.at[inst, i, j], rs_r.at[inst, i, j], ends[j][2])

        return copy

    def rs_send(inst, i, dest):
        c = rs_copies(inst, i)
        step = L // 4

        def rows_of(j):
            def rows(q):
                return part(q * L + j * step, step)

            here = mul_of(j, step)
            s1[i, 0, here] = acc[rows(t_y), 0:HW].astype(bf16)
            s1[i, 1, here] = acc[rows(t_d), 0:HW].astype(bf16)
            s1[i, 2, here] = acc[rows(t_z), HW:CW].astype(bf16)
            s1[i, 3, here] = acc[rows(t_d), HW:CW].astype(bf16)
            k2[i, 0, here] = acc[rows(t_z), 0:HW]
            k2[i, 1, here] = acc[rows(t_y), HW:CW]
            dest[here, mul_of(i, CW)] = acc[rows(t), :]

        loop(4, rows_of)
        c(0).start()
        c(1).start()

    def rs_fwd(inst, i, dest):
        c = rs_copies(inst, i)
        c(0).wait_recv()
        s2[i, 0] = (k2[i, 0] + r1[i, 1].astype(f32)).astype(bf16)
        c(2).start()
        c(1).wait_recv()
        s2[i, 1] = (k2[i, 1] + r1[i, 3].astype(f32)).astype(bf16)
        c(3).start()
        dest[:, mul_of(2 * i, HW)] += r1[i, 0].astype(f32)
        dest[:, mul_of(2 * i + 1, HW)] += r1[i, 2].astype(f32)

    def rs_done(inst, i, dest):
        c = rs_copies(inst, i)
        c(2).wait_recv()
        c(3).wait_recv()
        dest[:, mul_of(2 * i, HW)] += r2[i, 0].astype(f32)
        dest[:, mul_of(2 * i + 1, HW)] += r2[i, 1].astype(f32)

    def rs(inst, dest, compute, between=lambda i: None):
        def first(i):
            compute(i)
            rs_send(inst, i, dest)

        loop(CHUNKS, first)
        between(0)
        loop(CHUNKS // 2, lambda i: rs_fwd(inst, i, dest))
        between(1)
        loop(CHUNKS, lambda i: rs_fwd(inst, i, dest), CHUNKS // 2)
        between(2)
        loop(CHUNKS, lambda i: rs_done(inst, i, dest))

        def wait(i):
            c = rs_copies(inst, i)
            for j in range(4):
                c(j).wait_send()

        loop(CHUNKS, wait)

    def qkv_region(s_, piece):
        return wqkv.at[part(s_ * (D // 2) + piece * (D // 4), D // 4)]

    def qkv_parts(s_, piece):
        rows, to = part(piece * (D // 4), D // 4), part(s_ * (D // 2) + piece * (D // 4), D // 4)
        for which, src in enumerate((wq_h, wk_h, wv_h)):
            for h in range(d.S):
                yield src.at[rows, part((h * TP + t) * HD, HD)], wqkv.at[to, pl.ds(which * ha + h * HD, HD)]

    def o_region(s_, piece):
        return wo.at[part(s_ * HD + piece * (HD // 2), HD // 2)]

    def o_parts(s_, piece):
        yield wo_h.at[part(t * HD + piece * (HD // 2), HD // 2)], o_region(s_, piece)

    def gu_group(sub):
        n = D // 8

        def region(s_, piece):
            return wgu.at[part(s_ * (D // 2) + piece * (D // 4) + sub * n, n)]

        def parts(s_, piece):
            rows = part(piece * (D // 4) + sub * n, n)
            to = part(s_ * (D // 2) + piece * (D // 4) + sub * n, n)
            w = 2 * unit
            if not d.direct:
                yield wg_h.at[rows], wgu.at[to]
                return
            for m, src in enumerate((wg_h, wu_h)):
                for c in range(d.S * his):
                    yield src.at[rows, part((c * TP + t) * w, w)], wgu.at[to, pl.ds(m * fh + c * w, w)]

        return parts, region

    def d_region(s_, piece):
        n = fh // 4
        return wd.at[part(((s_ * 2 + piece) if d.direct else (piece * 2 + s_)) * n, n)]

    def d_parts(s_, piece):
        w = 2 * unit
        if not d.direct:
            yield wd_h.at[part(piece * (fh // 4), fh // 4)], d_region(s_, piece)
            return
        for e in range(his // 2):
            block = piece * (his // 2) + e
            yield wd_h.at[part((block * TP + t) * w, w)], wd.at[part((s_ * his + block) * w, w)]

    groups = ((qkv_parts, qkv_region), (o_parts, o_region), gu_group(0), gu_group(1), (d_parts, d_region))
    NG = len(groups)

    def local_start(k):
        for piece in range(2):
            for src, dst in groups[k][0](s, piece):
                pltpu.make_async_copy(src, dst, w_l.at[k, piece]).start()

    def local_wait(k):
        for piece in range(2):
            here = groups[k][1](s, piece)
            pltpu.make_async_copy(here, here, w_l.at[k, piece]).wait()

    def cross_start(k):
        for src, dst in groups[k][0](s, core):
            send(src, dst, w_s.at[k], w_r.at[k], dev_x).start()

    def cross(k):
        here = groups[k][1](s, core)
        return send(here, here, w_s.at[k], w_r.at[k], dev_x)

    def share(k):
        here = groups[k][1](1 - s, core)
        return send(here, here, wf_s.at[k], wf_r.at[k], dev_c)

    def w_forward(k):
        cross(k).wait_recv()
        share(k).start()

    def w_ready(k):
        local_wait(k)
        share(k).wait_recv()

    own_x = pltpu.make_async_copy(x_h, xall.at[blk(t)], loc.at[0])
    own_cot = pltpu.make_async_copy(cot_h, cot, loc.at[1])
    own_gain = pltpu.make_async_copy(gain_v, gbuf.at[s], loc.at[2])
    far_gain = send(gain_v, gbuf.at[s], w_s.at[NG], w_r.at[NG], dev_x)
    ag_start(xall, 0, 0, x_h)
    cross_start(0)
    ag_start(xall, 0, 1, x_h)
    own_x.start()
    far_gain.start()
    own_gain.start()
    local_start(0)
    for k in range(1, NG):
        cross_start(k)
    for k in range(1, NG):
        local_start(k)
    own_cot.start()

    for i in range(CHUNKS):
        ag_fwd(xall, 0, i)
        if i + 2 < CHUNKS:
            ag_start(xall, 0, i + 2, x_h)
    w_forward(0)
    own_x.wait()
    own_gain.wait()
    far_gain.wait_recv()
    for q in range(2):
        gat[:, q * (D // 2):(q + 1) * (D // 2)] = gbuf[q, :, 2 * HD:2 * HD + D // 2]
        gml[:, q * (D // 2):(q + 1) * (D // 2)] = gbuf[q, :, 2 * HD + D // 2:]
    gsum[...] = jnp.zeros_like(gsum)
    for i in range(CHUNKS):
        ag_done(xall, 0, i)
    ag_drain(xall, 0)
    w_ready(0)

    qk[:, 0:ha] = dot_nn(xall[...], wqkv[:, 0:ha])
    qk[:, ha:2 * ha] = dot_nn(xall[...], wqkv[:, ha:2 * ha])
    vb[...] = dot_nn(xall[...], wqkv[:, 2 * ha:]).astype(bf16)
    w_forward(1)

    row8 = lax.broadcasted_iota(jnp.int32, (8, 2 * ha), 0)
    col8 = lax.broadcasted_iota(jnp.int32, (8, 2 * ha), 1)
    pick = jnp.where((row8 < 4) == (col8 < ha), 1.0, 0.0).astype(f32)
    HIGH = lax.Precision.HIGHEST

    def stat_sum(k, values, between=lambda: None):
        def sequence(b):
            stat[k, :, blk(b)] = dot_nt(pick, values(blk(b)), HIGH)

        loop(TP, sequence)
        copies = [send(stat.at[k], statr.at[k, j], st_s.at[k, j], st_r.at[k, j], dev)
                  for j, dev in enumerate((dev_y, dev_z, dev_d))]
        for c in copies:
            c.start()
        between()
        for c in copies:
            c.wait_recv()
        for c in copies:
            c.wait_send()
        return stat[k] + statr[k, 0] + statr[k, 1] + statr[k, 2]

    def squares(rows):
        v = qk[rows, :]
        return v * v

    stat[2] = lax.rsqrt(stat_sum(0, squares) / d.att + eps_norm)

    def columns(k, b):
        flat = stat[k, :, blk(b)]
        wide = jnp.concatenate([flat] * (L // 8), axis=0).T
        return wide[:, 0:1], wide[:, 4:5]

    def gain_of(which, h):
        return gbuf[h, :, which * HD:(which + 1) * HD]

    inv = 1.0 / math.sqrt(HD)
    heads = ha // HD

    def attend(b):
        rows = blk(b)
        scale = columns(2, b)
        cos, sin = cos_v[...], sin_v[...]
        above = lax.broadcasted_iota(jnp.int32, (L, L), 0) < lax.broadcasted_iota(jnp.int32, (L, L), 1)
        for h in range(heads):
            rot = []
            for which in range(2):
                at = pl.ds(which * ha + h * HD, HD)
                normed = qk[rows, at] * scale[which] * gain_of(which, h)
                turned = (normed * cos + pltpu.roll(normed, HD // 2, 1) * sin).astype(bf16)
                qkrot[rows, at] = turned
                rot.append(turned)
            scores = jnp.where(above, -jnp.inf, dot_nt(rot[0], rot[1]) * inv)
            peak = jnp.max(scores, axis=-1, keepdims=True)
            log_total = peak + jnp.log(jnp.sum(jnp.exp(scores - peak), axis=-1, keepdims=True))
            p = jnp.exp(scores - log_total)
            probs[b * heads + h] = p
            head = pl.ds(h * HD, HD)
            mixed[rows, head] = dot_nn(p.astype(bf16), vb[rows, head]).astype(bf16)

    loop(TP, attend)
    w_ready(1)

    def attn_chunk(i):
        acc[...] = dot_nn(mixed[...], wo[:, mul_of(i, CW)])

    rs(0, abuf, attn_chunk)

    BL = 16

    def residual_rows(j):
        rows = mul_of(j, BL)
        a = abuf[rows, :]
        scale = lax.rsqrt(jnp.mean(a * a, axis=-1, keepdims=True) + eps_norm)
        mine = part(t * L + j * BL, BL)
        res = xall[mine, :].astype(f32) + a * scale * gat[...]
        cbuf[rows, :] = res
        rall[mine, :] = res.astype(bf16)

    loop(L // BL, residual_rows)
    w_forward(2)
    ag(rall, 1)
    w_forward(3)
    w_ready(2)
    w_ready(3)

    NT = 256

    def gate_up(n):
        g_at, u_at = mul_of(n, NT), part(fh + n * NT, NT)
        gu[:, g_at] = dot_nn(rall[...], wgu[:, g_at])
        gu[:, u_at] = dot_nn(rall[...], wgu[:, u_at])

        def rows_of(j):
            rows = mul_of(j, 64)
            g, u = gu[rows, g_at], gu[rows, u_at]
            hid[rows, g_at] = (g * jax.nn.sigmoid(g) * u).astype(bf16)

        loop(T // 64, rows_of)

    loop(fh // NT, gate_up)
    w_forward(4)
    w_ready(4)

    def down_chunk(i):
        acc[...] = dot_nn(hid[...], wd[:, mul_of(i, CW)])

    rs(1, bbuf, down_chunk)
    own_cot.wait()

    def output_rows(j):
        rows = mul_of(j, BL)
        dn = bbuf[rows, :]
        scale = lax.rsqrt(jnp.mean(dn * dn, axis=-1, keepdims=True) + eps_norm)
        outb[rows, :] = (cbuf[rows, :] + dn * scale * gml[...]).astype(bf16)
        co = cot[rows, :].astype(f32)
        weighted = co * gml[...]
        inner = jnp.mean(weighted * dn, axis=-1, keepdims=True)
        gd = scale * weighted - dn * scale**3 * inner
        gdall[part(t * L + j * BL, BL), :] = gd.astype(bf16)
        gsum[:, D:2 * D] += jnp.sum(co * dn * scale, axis=0, keepdims=True)

    loop(L // BL, output_rows)
    put_out = pltpu.make_async_copy(outb, out_h, loc.at[3])
    put_out.start()
    ag(gdall, 2)

    half_q = 3 * ha // 2

    def by_cols(left, right, width):
        def make(row, n, core_):
            return dot_tn(left[:, part(row, n)], right[:, mul_of(core_, width)])
        return make

    def down_grad(row, n, core_):
        start = (row // unit) * 2 * unit + core_ * unit if d.direct else core_ * (fh // 2) + row
        return dot_tn(hid[:, part(start, n)], gdall[...])

    ND, NG2, NQ, NO = range(4)
    sets = (
        (down_grad, rc_d, rx_d, rh_d, fh // 2, 128, stage_d),
        (by_cols(rall, gg2, fh), rc_gu, rx_gu, rh_gu, D, 256, stage),
        (by_cols(xall, gqkv, half_q), rc_q, rx_q, rh_q, D, 256, stage),
        (by_cols(mixed, gaall, D // 2), rc_o, rx_o, None, ha, 128, stage),
    )
    top = hi // (his // 2)

    def tiles_of(k):
        return sets[k][4] // 2 // sets[k][5]

    def tile_row(k, j):
        tiles, n = tiles_of(k), sets[k][5]
        if tiles < 2:
            return j * n
        return ((j + (1 - top) * (tiles // 2)) % tiles) * n

    def whole_row(k, j):
        tiles = tiles_of(k)
        late = j // tiles
        return (late * s + (1 - late) * (1 - s)) * (sets[k][4] // 2) + tile_row(k, j % tiles)

    def core_copy(k, j, slot):
        _, buf, _, _, _, n, st = sets[k]
        row = whole_row(k, j)
        view = st.at[slot, :, 0:buf.shape[1]] if st.shape[1] == n else st.at[slot, 0:n, 0:buf.shape[1]]
        return send(view, buf.at[part(row, n)], stg_s.at[0 if k == ND else 1, slot], c_r.at[k, row // n], dev_c)

    def give(k):
        make, buf, _, _, _, n, st = sets[k]
        slots, w, count = st.shape[0], buf.shape[1], 2 * tiles_of(k)

        def tile(j):
            slot = j % slots

            @pl.when(j >= slots)
            def _():
                core_copy(k, j, slot).wait_send()

            st[slot, 0:n, 0:w] = make(whole_row(k, j), n, 1 - core).astype(bf16)
            core_copy(k, j, slot).start()

        loop(count, tile)
        for slot in range(min(slots, count)):
            core_copy(k, 0, slot).wait_send()

    def x_copy(k, j):
        _, buf, far, _, rows, n, _ = sets[k]
        row = tile_row(k, j)
        return send(buf.at[part((1 - s) * (rows // 2) + row, n)], far.at[part(row, n)], x_s.at[k, j], x_r.at[k, j], dev_x)

    def take(k, late):
        make, buf, _, _, _, n, _ = sets[k]
        tiles = tiles_of(k)

        def tile(j):
            row = whole_row(k, j)
            core_copy(k, j, 0).wait_recv()
            buf[part(row, n), :] = (make(row, n, core) + buf[part(row, n), :].astype(f32)).astype(bf16)
            if not late:
                x_copy(k, j).start()

        loop(2 * tiles if late else tiles, tile, tiles if late else 0)

    def hi_first(k, j):
        _, buf, _, back, rows, n, _ = sets[k]
        other = hi + (his // 2) * (1 - 2 * top)
        return send(buf.at[part(s * (rows // 2) + tile_row(k, j), n)], back.at[mul_of(j, n)],
                    h0_s.at[k, j], h0_r.at[k, j], (s, rep(other, t, core)))

    def add_rows(buf, row, far, far_row, n, final=None):
        step = min(n, 64)

        def rows_of(j):
            rows = part(row + j * step, step)
            total = buf[rows, :].astype(f32) + far[part(far_row + j * step, step), :].astype(f32)
            if final is None:
                buf[rows, :] = total.astype(bf16)
            else:
                final[mul_of(j, step), :] = total

        loop(n // step, rows_of)

    def x_add(k, j0, j1):
        _, buf, far, _, rows, n, _ = sets[k]
        tiles = tiles_of(k)

        def tile(j):
            row = tile_row(k, j)
            x_copy(k, j).wait_recv()
            add_rows(buf, s * (rows // 2) + row, far, row, n)
            if k != NO:
                @pl.when(j < tiles // 2)
                def _():
                    hi_first(k, j).start()

        loop(j1, tile, j0)

    def hi_later(k):
        half = sets[k][4] // 2
        base, size, at, out = top * (half // 2), half // 2, half // 2, []
        for level in range(1, d.levels):
            size //= 2
            weight = his >> (level + 1)
            bit = (hi // weight) % 2
            out.append((level - 1, base + (1 - bit) * size, base + bit * size, size, at, hi + weight * (1 - 2 * bit)))
            base = base + bit * size
            at += size
        return out, base, size

    def hi_copy(k, step):
        level, far_row, _, size, at, other = step
        half = sets[k][4] // 2
        return send(sets[k][1].at[part(s * half + far_row, size)], sets[k][3].at[pl.ds(at, size)],
                    h_s.at[k, level], h_r.at[k, level], (s, rep(other, t, core)))

    def hi_finish(k, final=None):
        _, buf, _, back, rows, n, _ = sets[k]
        tiles, half = tiles_of(k), rows // 2
        last = final if d.levels == 1 else None

        def tile(j):
            hi_first(k, j).wait_recv()
            add_rows(buf, s * half + tile_row(k, j + tiles // 2), back, j * n, n, last)

        loop(tiles // 2, tile)
        later = hi_later(k)[0]
        for step in later:
            hi_copy(k, step).start()
            hi_copy(k, step).wait_recv()
            add_rows(buf, s * half + step[2], back, step[4], step[3], final if step is later[-1] else None)

    me = t * CORES + core

    def keep_parts(k, p, slot_t, slot_core):
        half = sets[k][4] // 2
        _, base, _ = hi_later(k)
        rows = part(s * half + base + p * d.own, d.own)
        if k == NQ:
            for c in range(3):
                e = slot_core * 3 + c
                yield (rc_q.at[rows, pl.ds(c * HD, HD)],
                       qkv_h.at[e // 2, :, part(((e % 2) * TP + slot_t) * HD, HD)])
        elif d.direct:
            w = 2 * unit
            for c in range(d.S * his):
                yield rc_gu.at[rows, pl.ds(c * w, w)], gu_h.at[slot_core, :, part((c * TP + slot_t) * w, w)]
        else:
            yield rc_gu.at[rows], gu_h.at[slot_t * CORES + slot_core]

    def keep_start(k):
        def piece(p):
            @pl.when(me != p)
            def _():
                for src, dst in keep_parts(k, p, t, core):
                    send(src, dst, a_s.at[k - 1, p], a_r.at[k - 1, me], (s, rep(hi, p // CORES, p % CORES))).start()

            @pl.when(me == p)
            def _():
                for src, dst in keep_parts(k, p, t, core):
                    pltpu.make_async_copy(src, dst, a_r.at[k - 1, me]).start()

        loop(TP * CORES, piece)

    def keep_wait(k):
        def piece(p):
            whole = sets[k][1].at[pl.ds(0, d.own)]
            pltpu.make_async_copy(whole, whole, a_r.at[k - 1, p]).wait()

            @pl.when(me != p)
            def _():
                send(whole, whole, a_s.at[k - 1, p], a_r.at[k - 1, me], (s, rep(hi, p // CORES, p % CORES))).wait_send()

        loop(TP * CORES, piece)

    partners = [dev_c, dev_x]
    for level in range(d.levels):
        weight = his >> (level + 1)
        bit = (hi // weight) % 2
        partners.append((s, rep(hi + weight * (1 - 2 * bit), t, core)))
    partners += [dev_y, dev_z]

    def gain_copy(n):
        return send(gsum, grecv.at[n], gn_s.at[n], gn_r.at[n], partners[n])

    def gain_step(n):
        if n:
            gain_copy(n - 1).wait_send()
            gain_copy(n - 1).wait_recv()
            gsum[...] += grecv[n - 1]
        if n < len(partners):
            gain_copy(n).start()

    give(ND)

    def hidden_back(n):
        g_at, u_at = mul_of(n, NT), part(fh + n * NT, NT)
        acc[:, 0:NT] = dot_nt(gdall[...], wd[mul_of(n, NT), :])

        def rows_of(j):
            rows = mul_of(j, 64)
            g, u, gh = gu[rows, g_at], gu[rows, u_at], acc[rows, 0:NT]
            sig = jax.nn.sigmoid(g)
            gg2[rows, g_at] = (gh * u * sig * (1.0 + g * (1.0 - sig))).astype(bf16)
            gg2[rows, u_at] = (gh * (g * sig)).astype(bf16)

        loop(T // 64, rows_of)

    loop(fh // NT, hidden_back)
    take(ND, False)

    def res_chunk(i):
        acc[...] = dot_nt(gg2[...], wgu[mul_of(i, CW), :])

    def res_between(i):
        if i == 0:
            give(NG2)
        elif i == 1:
            take(NG2, False)
        else:
            take(ND, True)
            take(NG2, True)

    rs(2, cbuf, res_chunk, res_between)

    def attn_grad_rows(j):
        rows = mul_of(j, BL)
        gr = cbuf[rows, :] + cot[rows, :].astype(f32)
        cbuf[rows, :] = gr
        a = abuf[rows, :]
        scale = lax.rsqrt(jnp.mean(a * a, axis=-1, keepdims=True) + eps_norm)
        weighted = gr * gat[...]
        inner = jnp.mean(weighted * a, axis=-1, keepdims=True)
        ga = scale * weighted - a * scale**3 * inner
        gaall[part(t * L + j * BL, BL), :] = ga.astype(bf16)
        gsum[:, 0:D] += jnp.sum(gr * a * scale, axis=0, keepdims=True)

    loop(L // BL, attn_grad_rows)

    def ga_between(i):
        if i == 1:
            x_add(ND, 0, 1)
        if i == 3:
            x_add(ND, 1, 2)

    ag(gaall, 3, None, ga_between)

    give(NO)
    acc[:, 0:ha] = dot_nt(gaall[...], wo[...])
    x_add(NG2, 0, 1)

    def attend_back(b):
        rows = blk(b)
        scale = columns(2, b)
        cos, sin = cos_v[...], sin_v[...]
        for h in range(heads):
            head = pl.ds(h * HD, HD)
            gm = acc[rows, head].astype(bf16)
            p = probs[b * heads + h]
            gqkv[rows, pl.ds(2 * ha + h * HD, HD)] = dot_tn(p.astype(bf16), gm).astype(bf16)
            gp = dot_nt(gm, vb[rows, head])
            gs = p * (gp - jnp.sum(p * gp, axis=-1, keepdims=True))
            gs = (gs * inv).astype(bf16)
            turned = (dot_nn(gs, qkrot[rows, pl.ds(ha + h * HD, HD)]), dot_tn(gs, qkrot[rows, head]))
            for which in range(2):
                at = pl.ds(which * ha + h * HD, HD)
                gn = turned[which] * cos - pltpu.roll(turned[which], HD // 2, 1) * sin
                field = qk[rows, at]
                spot = part(2 * D + which * d.att + t * ha + h * HD, HD)
                gsum[:, spot] += jnp.sum(gn * field * scale[which], axis=0, keepdims=True)
                gu[rows, at] = gn * gain_of(which, h)

    loop(TP, attend_back)

    def products(rows):
        return gu[rows, 0:2 * ha] * qk[rows, :]

    stat[3] = stat_sum(1, products, lambda: take(NO, False)) / d.att
    gain_step(0)

    def qk_back(b):
        rows = blk(b)
        scale, inner = columns(2, b), columns(3, b)
        for which in range(2):
            at = pl.ds(which * ha, ha)
            sc = scale[which]
            gqkv[rows, at] = (sc * gu[rows, at] - qk[rows, at] * (sc**3 * inner[which])).astype(bf16)

    loop(TP, qk_back)
    give(NQ)
    gain_step(1)

    def in_chunk(i):
        acc[...] = dot_nt(gqkv[...], wqkv[mul_of(i, CW), :])

    def in_between(i):
        if i == 0:
            take(NQ, False)
            x_add(NG2, 1, 2)
            gain_step(2)
        elif i == 1:
            take(NQ, True)
            take(NO, True)
        else:
            hi_finish(ND, abuf)
            pltpu.make_async_copy(abuf.at[0:unit], down_h, loc.at[4]).start()
            gain_step(3)

    rs(3, bbuf, in_chunk, in_between)

    def input_rows(j):
        rows = mul_of(j, BL)
        bbuf[rows, :] += cbuf[rows, :]

    loop(L // BL, input_rows)
    put_gin = pltpu.make_async_copy(bbuf, gin_h, loc.at[5])
    put_gin.start()

    gain_step(4)
    x_add(NG2, 2, 4)
    for n in range(5, len(partners) + 1):
        gain_step(n)
    gg_o[...] = gsum[...]
    x_add(NO, 0, 1)

    for p in range(d.pieces):
        o_pc[p] = rc_o[part(s * HD + p * d.own_o, d.own_o), :]
    o_slot = hi * CORES + core

    def o_start(p):
        goal = t * d.pieces + p

        @pl.when(goal != r)
        def _():
            send(o_pc.at[p], o_h.at[o_slot], o_s.at[p], o_r.at[o_slot], (s, goal)).start()

        @pl.when(goal == r)
        def _():
            pltpu.make_async_copy(o_pc.at[p], o_h.at[o_slot], o_r.at[o_slot]).start()

    loop(d.pieces, o_start)
    x_add(NQ, 0, 4)
    hi_finish(NG2)
    keep_start(NG2)
    hi_finish(NQ)
    keep_start(NQ)

    keep_wait(NG2)
    keep_wait(NQ)

    def o_wait(q):
        pltpu.make_async_copy(o_pc.at[0], o_pc.at[0], o_r.at[q]).wait()

    loop(his * CORES, o_wait)

    def o_sent(p):
        goal = t * d.pieces + p

        @pl.when(goal != r)
        def _():
            send(o_pc.at[p], o_h.at[o_slot], o_s.at[p], o_r.at[o_slot], (s, goal)).wait_send()

    loop(d.pieces, o_sent)
    far_gain.wait_send()
    for k in range(NG):
        cross(k).wait_send()
        share(k).wait_send()
    for k in range(4):
        loop(tiles_of(k), lambda j: x_copy(k, j).wait_send())
    for k in range(3):
        loop(tiles_of(k) // 2, lambda j: hi_first(k, j).wait_send())
        for step in hi_later(k)[0]:
            hi_copy(k, step).wait_send()
    put_out.wait()
    put_gin.wait()
    pltpu.make_async_copy(abuf.at[0:unit], down_h, loc.at[4]).wait()


def body(shards, replicas, x_in, cotangent, w_query, w_key, w_value, w_out, w_gate, w_up, w_down,
         gain_query, gain_key, gain_attn, gain_mlp):
    seqs, length, width = x_in.shape
    assert seqs == 1
    d = Dims(length, width, w_query.shape[1], w_gate.shape[1], shards, replicas)
    r = lax.axis_index("replica")
    s = lax.axis_index("shard")
    t = (r // CORES) % TP

    def at(array, axis, index):
        return lax.dynamic_index_in_dim(array, index, axis, keepdims=False)

    def hidden_cols(w):
        picked = at(w.reshape(w.shape[0], d.S, d.his, TP, CORES, d.unit), 3, t)
        return picked.transpose(0, 3, 1, 2, 4).reshape(w.shape[0], d.fh)

    if not d.direct:
        w_gate = jnp.concatenate([hidden_cols(w_gate), hidden_cols(w_up)], axis=1)
        w_down = at(w_down.reshape(d.his, TP, CORES, d.unit, width), 1, t).transpose(1, 0, 2, 3).reshape(-1, width)
    gain = jnp.concatenate([at(gain_query.reshape(TP, HD), 0, t), at(gain_key.reshape(TP, HD), 0, t),
                            gain_attn, gain_mlp]).astype(f32)[None]
    cos, sin = rope_tables(length, HD // 2)
    cos = np.concatenate([cos, cos], axis=1)
    sin = np.concatenate([-sin, sin], axis=1)

    L, D, T, ha, fh = d.L, d.D, d.T, d.ha, d.fh
    CW = D // CHUNKS
    vm = pltpu.VMEM
    dma = pltpu.SemaphoreType.DMA
    any_ = pl.BlockSpec(memory_space=pl.ANY)
    vmem = pl.BlockSpec(memory_space=pltpu.VMEM)
    hi_rows = lambda n: max(n - n // d.his, 16)
    steps = 4 + d.levels
    later = max(d.levels - 1, 1)
    scratch = [
        vm((D, 3 * ha), bf16), vm((ha, D), bf16), vm((D, 2 * fh), bf16), vm((fh, D), bf16),
        vm((2, 1, d.gains), f32), vm((1, D), f32), vm((1, D), f32),
        vm((T, D), bf16), vm((T, D), bf16), vm((T, D), bf16), vm((T, D), bf16), vm((L, D), bf16),
        vm((T, 2 * ha), f32), vm((T, ha), bf16), vm((T, 2 * ha), bf16), vm((TP * ha // HD, L, L), f32),
        vm((T, ha), bf16), vm((T, 3 * ha), bf16), vm((4, 8, T), f32), vm((2, 3, 8, T), f32),
        vm((T, 2 * fh), f32), vm((T, fh), bf16), vm((T, 2 * fh), bf16),
        vm((L, D), f32), vm((L, D), f32), vm((L, D), f32), vm((L, D), bf16),
        vm((T, CW), f32), vm((CHUNKS, 4, L, CW // 2), bf16), vm((CHUNKS, 2, L, CW // 2), bf16),
        vm((CHUNKS, 4, L, CW // 2), bf16), vm((CHUNKS, 2, L, CW // 2), bf16), vm((CHUNKS, 2, L, CW // 2), f32),
        vm((2, 128, D), bf16), vm((2, 256, fh), bf16),
        vm((D, fh), bf16), vm((fh // 2, D), bf16), vm((D, 3 * ha // 2), bf16), vm((ha, D // 2), bf16),
        vm((D // 2, fh), bf16), vm((fh // 4, D), bf16), vm((D // 2, 3 * ha // 2), bf16), vm((ha // 2, D // 2), bf16),
        vm((hi_rows(D // 2), fh), bf16), vm((hi_rows(fh // 4), D), bf16), vm((hi_rows(D // 2), 3 * ha // 2), bf16),
        vm((d.pieces, d.own_o, D // 2), bf16),
        vm((1, d.ggs), f32), vm((steps, 1, d.ggs), f32),
        dma((4, CHUNKS, 4)), dma((4, CHUNKS, 4)), dma((4, CHUNKS, 4)), dma((4, CHUNKS, 4)),
        dma((6,)), dma((6,)), dma((5,)), dma((5,)), dma((5, 2)), dma((6,)), dma((2, 3)), dma((2, 3)),
        dma((2, 2)), dma((4, 8)), dma((4, 4)), dma((4, 4)), dma((3, 4)), dma((3, 4)),
        dma((3, later)), dma((3, later)),
        dma((2, TP * CORES)), dma((2, TP * CORES)), dma((d.pieces,)), dma((d.his * CORES,)), dma((steps,)), dma((steps,)),
    ]
    struct = jax.ShapeDtypeStruct
    gu_shape = (2, d.own, d.ff) if d.direct else (TP * CORES, d.own, fh)
    results = pl.pallas_call(
        functools.partial(kernel, d),
        out_shape=(
            struct((L, D), bf16), struct((L, D), f32), struct(gu_shape, bf16), struct((3, d.own, d.att), bf16),
            struct((d.unit, D), f32), struct((d.his * CORES, d.own_o, D // 2), bf16), struct((1, d.ggs), f32),
        ),
        in_specs=[any_] * 9 + [vmem] * 3,
        out_specs=(any_,) * 6 + (vmem,),
        scratch_shapes=scratch,
        compiler_params=pltpu.CompilerParams(
            collective_id=0, has_side_effects=True, vmem_limit_bytes=67043328),
        name="layer",
    )(x_in[0], cotangent[0], w_query, w_key, w_value, w_out, w_gate, w_up, w_down, gain, cos, sin)
    out, gin, gu, qkv, down, o, gg = results

    def hidden_out(k):
        if d.direct:
            return gu[k].astype(f32)
        block = gu.reshape(TP, CORES, d.own, fh)[:, k]
        spread = block.reshape(TP, d.own, CORES, d.S, d.his, d.unit).transpose(1, 3, 4, 0, 2, 5)
        return spread.reshape(d.own, d.ff).astype(f32)

    o = o.reshape(d.his, CORES, d.own_o, D // 2).astype(f32).sum(0).transpose(1, 0, 2).reshape(d.own_o, D)
    gg = gg[0]
    here = s * d.R + r

    def share(vec):
        n = vec.shape[0] // (d.S * d.R)
        return lax.dynamic_slice_in_dim(vec, here * n, n)

    def head_gain(vec):
        return share(vec.reshape(TP, d.S, HD).transpose(1, 0, 2).reshape(-1))

    return (
        out[None], gin[None], qkv[0].astype(f32), qkv[1].astype(f32), qkv[2].astype(f32), o,
        hidden_out(0), hidden_out(1), down,
        head_gain(gg[2 * D:2 * D + d.att]), head_gain(gg[2 * D + d.att:]), share(gg[:D]), share(gg[D:2 * D]),
    )


def solution(mesh):
    both = ("shard", "replica")
    token = P(both, None, None)
    weight = P("shard", None)
    return jax.shard_map(
        functools.partial(body, mesh.shape["shard"], mesh.shape["replica"]),
        mesh=mesh,
        in_specs=(token, token) + (weight,) * 7 + (P("shard"),) * 4,
        out_specs=(token, token) + (P(both, None),) * 7 + (P(both),) * 4,
        check_vma=False,
    )
```

```python
import functools
import math

import jax
import jax.numpy as jnp
import numpy as np
from jax import lax
from jax.experimental import pallas as pl
from jax.experimental.pallas import tpu as pltpu
from jax.sharding import PartitionSpec as P

HD = 128
TP = 4
CORES = 2
CHUNKS = 4
Z_AG = (256, 256, 256, 0)
Z_RS = (256, 256, 256, 128)

eps_norm = 1e-06
rope_theta = 500000.0

bf16 = jnp.bfloat16
f32 = jnp.float32


def rope_tables(length, half):
    position = np.arange(length).astype(np.float32)[:, None]
    exponent = np.arange(half).astype(np.float32) * np.float32(1.0 / half)
    angle = position * np.float32(rope_theta) ** (-exponent)
    return (np.cos(angle).astype(np.float32), np.sin(angle).astype(np.float32))


def dot_nn(left, right):
    return lax.dot_general(left, right, (((1,), (0,)), ((), ())), preferred_element_type=f32)


def dot_nt(left, right, precision=None):
    return lax.dot_general(
        left, right, (((1,), (1,)), ((), ())), preferred_element_type=f32, precision=precision)


def dot_tn(left, right):
    return lax.dot_general(left, right, (((0,), (0,)), ((), ())), preferred_element_type=f32)


def mul_of(index, step):
    return pl.ds(pl.multiple_of(index * step, step), step)


def loop(count, step, start=0):
    lax.fori_loop(start, count, lambda i, c: (step(i), c)[1], 0)


class Dims:
    def __init__(self, length, width, att, ff, shards, replicas):
        self.L, self.D, self.att, self.ff = length, width, att, ff
        self.S, self.R = shards, replicas
        self.his = replicas // (TP * CORES)
        self.T = TP * length
        self.ha = att // TP
        self.fh = ff // TP
        self.unit = ff // (shards * replicas)
        self.own = width // (shards * replicas)
        self.own_o = att // (shards * replicas)
        self.pieces = HD // self.own_o
        self.levels = self.his.bit_length() - 1
        self.gains = 2 * HD + width
        self.ggs = 2 * width + 2 * att
        self.direct = self.unit % 128 == 0
        assert shards == 2 and self.his == 1 << self.levels and self.levels > 0 and self.ha == shards * HD
        assert self.fh == 2 * (width // CHUNKS)


def kernel(
    d,
    x_h, cot_h, wq_h, wk_h, wv_h, wo_h, wg_h, wu_h, wd_h, gain_v, cos_v, sin_v,
    out_h, gin_h, gu_h, qkv_h, down_h, o_h, relay_d, relay_gu, relay_q, gg_o,
    wqkv, wo, wgu, wd, gbuf, gat, gml,
    xall, rall, gdall, gaall, cot,
    qk, vb, qkrot, probs, mixed, gqkv, stat, statr,
    gu, hid, gg2,
    abuf, bbuf, cbuf, outb,
    acc, s1, s2, r1, r2, k2,
    stage_d, stage, rc_gu, rc_d, rc_q, rc_o, rx_gu, rx_d, rx_q, rx_o, rh_gu, rh_d, rh_q, o_pc,
    gsum, grecv,
    ag_s, ag_r, rs_s, rs_r, w_s, w_r, wf_s, wf_r, w_l, loc, st_s, st_r,
    stg_s, c_r, x_s, x_r, h0_s, h0_r, rl_s, rl_r, rf_s, h_s, h_r, a_s, a_r, ko, o_s, o_r, gn_s, gn_r,
):
    L, D, T, ha, fh, his, unit = d.L, d.D, d.T, d.ha, d.fh, d.his, d.unit
    CW = D // CHUNKS
    HW = CW // 2
    s = lax.axis_index("shard")
    r = lax.axis_index("replica")
    hi, t, core = r // (TP * CORES), (r // CORES) % TP, r % CORES
    tz, ty = t // 2, t % 2
    t_y, t_z, t_d = tz * 2 + 1 - ty, (1 - tz) * 2 + ty, (1 - tz) * 2 + 1 - ty

    def rep(hi_, t_, core_):
        return hi_ * (TP * CORES) + t_ * CORES + core_

    dev_y, dev_z, dev_d = ((s, rep(hi, q, core)) for q in (t_y, t_z, t_d))
    dev_x = (1 - s, r)
    dev_c = (s, rep(hi, t, 1 - core))

    def send(src, dst, ssem, rsem, dev):
        return pltpu.make_async_remote_copy(
            src_ref=src, dst_ref=dst, send_sem=ssem, recv_sem=rsem, device_id=dev,
            device_id_type=pl.DeviceIdType.MESH)

    def blk(q):
        return mul_of(q, L)

    def part(base, n):
        return pl.ds(pl.multiple_of(base, n), n)

    def ag_copies(buf, inst, i, src=None):
        own = buf.at[blk(t), mul_of(i, CW)]
        first = own if src is None else src.at[:, mul_of(i, CW)]
        wz = Z_AG[inst]
        fy = buf.at[blk(t_y), pl.ds(pl.multiple_of(i * CW + CW - wz, 128), wz)] if wz else None
        fz = buf.at[blk(t_z), pl.ds(pl.multiple_of(i * CW, 128), CW - wz)]
        ends = ((first, own, dev_y), (first, own, dev_z), (fy, fy, dev_z), (fz, fz, dev_y))

        def copy(j):
            return send(ends[j][0], ends[j][1], ag_s.at[inst, i, j], ag_r.at[inst, i, j], ends[j][2])

        return copy

    def ag_start(buf, inst, i, src=None):
        c = ag_copies(buf, inst, i, src)
        c(0).start()
        c(1).start()

    def ag_fwd(buf, inst, i):
        c = ag_copies(buf, inst, i)
        c(1).wait_recv()
        c(3).start()
        c(0).wait_recv()
        if Z_AG[inst]:
            c(2).start()

    def ag_done(buf, inst, i):
        c = ag_copies(buf, inst, i)
        if Z_AG[inst]:
            c(2).wait_recv()
        c(3).wait_recv()

    def ag_drain(buf, inst):
        def wait(i):
            c = ag_copies(buf, inst, i)
            for j in range(4):
                if j != 2 or Z_AG[inst]:
                    c(j).wait_send()

        loop(CHUNKS, wait)

    def ag(buf, inst, src=None, between=lambda i: None):
        ag_start(buf, inst, 0, src)
        ag_start(buf, inst, 1, src)
        for i in range(CHUNKS):
            ag_fwd(buf, inst, i)
            if i + 2 < CHUNKS:
                ag_start(buf, inst, i + 2, src)
            between(i)
        for i in range(CHUNKS):
            ag_done(buf, inst, i)
        ag_drain(buf, inst)

    def rs_copies(inst, i):
        wa = CW - Z_RS[inst]
        ya, zb = pl.ds(0, wa), pl.ds(wa, CW - wa)

        def copy(j):
            if j == 0:
                a, b, dev = s1.at[i, :, :, ya], r1.at[i, :, :, ya], dev_y
            elif j == 1:
                a, b, dev = s1.at[i, :, :, zb], r1.at[i, :, :, zb], dev_z
            elif j == 2:
                a, b, dev = s2.at[i, :, ya], r2.at[i, :, ya], dev_z
            else:
                a, b, dev = s2.at[i, :, zb], r2.at[i, :, zb], dev_y
            return send(a, b, rs_s.at[inst, i, j], rs_r.at[inst, i, j], dev)

        return copy

    def rs_send(inst, i, dest):
        c = rs_copies(inst, i)
        wa = CW - Z_RS[inst]
        step = L // 4

        def rows_of(j):
            def rows(q):
                return part(q * L + j * step, step)

            here = mul_of(j, step)
            s1[i, 0, here, 0:wa] = acc[rows(t_y), 0:wa].astype(bf16)
            k2[i, here, 0:wa] = acc[rows(t_z), 0:wa]
            if wa < CW:
                s1[i, 0, here, wa:CW] = acc[rows(t_z), wa:CW].astype(bf16)
                k2[i, here, wa:CW] = acc[rows(t_y), wa:CW]
            s1[i, 1, here] = acc[rows(t_d), :].astype(bf16)
            dest[here, mul_of(i, CW)] = acc[rows(t), :]

        loop(4, rows_of)
        c(0).start()
        if wa < CW:
            c(1).start()

    def rs_fwd(inst, i, dest):
        c = rs_copies(inst, i)
        wa = CW - Z_RS[inst]
        c(0).wait_recv()
        s2[i, :, 0:wa] = (k2[i, :, 0:wa] + r1[i, 1, :, 0:wa].astype(f32)).astype(bf16)
        c(2).start()
        if wa < CW:
            c(1).wait_recv()
            s2[i, :, wa:CW] = (k2[i, :, wa:CW] + r1[i, 1, :, wa:CW].astype(f32)).astype(bf16)
            c(3).start()
        dest[:, mul_of(i, CW)] += r1[i, 0].astype(f32)

    def rs_done(inst, i, dest):
        c = rs_copies(inst, i)
        c(2).wait_recv()
        if Z_RS[inst]:
            c(3).wait_recv()
        dest[:, mul_of(i, CW)] += r2[i].astype(f32)

    def rs(inst, dest, compute, between=lambda i: None, extra=lambda i: None):
        def first(i):
            compute(i)
            rs_send(inst, i, dest)
            extra(i)

            @pl.when(i >= 2)
            def _():
                rs_fwd(inst, i - 2, dest)

        loop(CHUNKS, first)
        between(0)
        rs_fwd(inst, CHUNKS - 2, dest)
        between(1)
        rs_fwd(inst, CHUNKS - 1, dest)
        between(2)
        loop(CHUNKS, lambda i: rs_done(inst, i, dest))

        def wait(i):
            c = rs_copies(inst, i)
            for j in range(4):
                if j % 2 == 0 or Z_RS[inst]:
                    c(j).wait_send()

        loop(CHUNKS, wait)

    def qkv_region(s_, piece):
        return wqkv.at[part(s_ * (D // 2) + piece * (D // 4), D // 4)]

    def qkv_parts(s_, piece):
        rows, to = part(piece * (D // 4), D // 4), part(s_ * (D // 2) + piece * (D // 4), D // 4)
        for which, src in enumerate((wq_h, wk_h, wv_h)):
            for h in range(d.S):
                yield src.at[rows, part((h * TP + t) * HD, HD)], wqkv.at[to, pl.ds(which * ha + h * HD, HD)]

    def o_region(s_, piece):
        return wo.at[part(s_ * HD + piece * (HD // 2), HD // 2)]

    def o_parts(s_, piece):
        yield wo_h.at[part(t * HD + piece * (HD // 2), HD // 2)], o_region(s_, piece)

    SUBS = 4

    def gu_group(sub):
        n = D // 4 // SUBS

        def region(s_, piece):
            return wgu.at[part(s_ * (D // 2) + piece * (D // 4) + sub * n, n)]

        def parts(s_, piece):
            rows = part(piece * (D // 4) + sub * n, n)
            to = part(s_ * (D // 2) + piece * (D // 4) + sub * n, n)
            w = 2 * unit
            if not d.direct:
                yield wg_h.at[rows], wgu.at[to]
                return
            for m, src in enumerate((wg_h, wu_h)):
                for c in range(d.S * his):
                    yield src.at[rows, part((c * TP + t) * w, w)], wgu.at[to, pl.ds(m * fh + c * w, w)]

        return parts, region

    def d_group(sub):
        at = mul_of(sub, CW)
        n = fh // 4

        def region(s_, piece):
            return wd.at[part(((s_ * 2 + piece) if d.direct else (piece * 2 + s_)) * n, n), at]

        def parts(s_, piece):
            w = 2 * unit
            if not d.direct:
                yield wd_h.at[part(piece * n, n), at], region(s_, piece)
                return
            step = min(w, n)
            for e in range(n // step):
                first = piece * n + e * step
                src = (first // w) * (TP * w) + t * w + first % w
                yield wd_h.at[part(src, step), at], wd.at[part(s_ * (fh // 2) + first, step), at]

        return parts, region

    GU0, DN0 = 2, 2 + SUBS
    NG = DN0 + CHUNKS

    def group_of(k):
        if isinstance(k, int) and k < DN0:
            return ((qkv_parts, qkv_region), (o_parts, o_region))[k] if k < GU0 else gu_group(k - GU0)
        return d_group(k - DN0)

    def local_start(k):
        for piece in range(2):
            for src, dst in group_of(k)[0](s, piece):
                pltpu.make_async_copy(src, dst, w_l.at[k, piece]).start()

    def local_wait(k):
        for piece in range(2):
            here = group_of(k)[1](s, piece)
            pltpu.make_async_copy(here, here, w_l.at[k, piece]).wait()

    def cross_start(k):
        for src, dst in group_of(k)[0](s, core):
            send(src, dst, w_s.at[k], w_r.at[k], dev_x).start()

    def cross(k):
        here = group_of(k)[1](s, core)
        return send(here, here, w_s.at[k], w_r.at[k], dev_x)

    def share(k):
        here = group_of(k)[1](1 - s, core)
        return send(here, here, wf_s.at[k], wf_r.at[k], dev_c)

    def w_forward(k):
        cross(k).wait_recv()
        share(k).start()

    def w_ready(k):
        local_wait(k)
        share(k).wait_recv()

    own_x = pltpu.make_async_copy(x_h, xall.at[blk(t)], loc.at[0])
    own_cot = pltpu.make_async_copy(cot_h, cot, loc.at[1])
    own_gain = pltpu.make_async_copy(gain_v, gbuf.at[s], loc.at[2])
    far_gain = send(gain_v, gbuf.at[s], w_s.at[NG], w_r.at[NG], dev_x)
    own_x.start()
    local_start(0)
    own_gain.start()
    own_cot.start()

    barrier = pltpu.get_barrier_semaphore()

    def greet(q):
        @pl.when(q != r)
        def _():
            pl.semaphore_signal(barrier, inc=1, device_id=(s, q), device_id_type=pl.DeviceIdType.MESH)

    loop(d.R, greet)
    pl.semaphore_signal(barrier, inc=1, device_id=dev_x, device_id_type=pl.DeviceIdType.MESH)
    pl.semaphore_wait(barrier, d.R)

    ag_start(xall, 0, 0, x_h)
    cross_start(0)
    ag_start(xall, 0, 1, x_h)
    far_gain.start()
    for k in range(1, NG):
        cross_start(k)
    for k in range(1, NG):
        local_start(k)

    for i in range(CHUNKS):
        ag_fwd(xall, 0, i)
        if i + 2 < CHUNKS:
            ag_start(xall, 0, i + 2, x_h)
    w_forward(0)
    own_x.wait()
    own_gain.wait()
    far_gain.wait_recv()
    for q in range(2):
        gat[:, q * (D // 2):(q + 1) * (D // 2)] = gbuf[q, :, 2 * HD:2 * HD + D // 2]
        gml[:, q * (D // 2):(q + 1) * (D // 2)] = gbuf[q, :, 2 * HD + D // 2:]
    gsum[...] = jnp.zeros_like(gsum)
    for i in range(CHUNKS):
        ag_done(xall, 0, i)
    ag_drain(xall, 0)
    w_ready(0)

    qk[:, 0:ha] = dot_nn(xall[...], wqkv[:, 0:ha])
    qk[:, ha:2 * ha] = dot_nn(xall[...], wqkv[:, ha:2 * ha])
    vb[...] = dot_nn(xall[...], wqkv[:, 2 * ha:]).astype(bf16)

    row8 = lax.broadcasted_iota(jnp.int32, (8, 2 * ha), 0)
    col8 = lax.broadcasted_iota(jnp.int32, (8, 2 * ha), 1)
    pick = jnp.where((row8 < 4) == (col8 < ha), 1.0, 0.0).astype(f32)
    HIGH = lax.Precision.HIGHEST

    def stat_sum(k, values, between=lambda: None):
        def sequence(b):
            stat[k, :, blk(b)] = dot_nt(pick, values(blk(b)), HIGH)

        loop(TP, sequence)
        copies = [send(stat.at[k], statr.at[k, j], st_s.at[k, j], st_r.at[k, j], dev)
                  for j, dev in enumerate((dev_y, dev_z, dev_d))]
        for c in copies:
            c.start()
        between()
        for c in copies:
            c.wait_recv()
        for c in copies:
            c.wait_send()
        return stat[k] + statr[k, 0] + statr[k, 1] + statr[k, 2]

    def squares(rows):
        v = qk[rows, :]
        return v * v

    stat[2] = lax.rsqrt(stat_sum(0, squares) / d.att + eps_norm)

    def columns(k, b):
        flat = stat[k, :, blk(b)]
        wide = jnp.concatenate([flat] * (L // 8), axis=0).T
        return wide[:, 0:1], wide[:, 4:5]

    def gain_of(which, h):
        return gbuf[h, :, which * HD:(which + 1) * HD]

    inv = 1.0 / math.sqrt(HD)
    heads = ha // HD

    def attend(b):
        rows = blk(b)
        scale = columns(2, b)
        cos, sin = cos_v[...], sin_v[...]
        above = lax.broadcasted_iota(jnp.int32, (L, L), 0) < lax.broadcasted_iota(jnp.int32, (L, L), 1)
        for h in range(heads):
            rot = []
            for which in range(2):
                at = pl.ds(which * ha + h * HD, HD)
                normed = qk[rows, at] * scale[which] * gain_of(which, h)
                turned = (normed * cos + pltpu.roll(normed, HD // 2, 1) * sin).astype(bf16)
                qkrot[rows, at] = turned
                rot.append(turned)
            scores = jnp.where(above, -jnp.inf, dot_nt(rot[0], rot[1]) * inv)
            peak = jnp.max(scores, axis=-1, keepdims=True)
            log_total = peak + jnp.log(jnp.sum(jnp.exp(scores - peak), axis=-1, keepdims=True))
            p = jnp.exp(scores - log_total)
            probs[b * heads + h] = p
            head = pl.ds(h * HD, HD)
            mixed[rows, head] = dot_nn(p.astype(bf16), vb[rows, head]).astype(bf16)

    loop(TP, attend)
    w_forward(1)
    w_ready(1)

    def attn_chunk(i):
        acc[...] = dot_nn(mixed[...], wo[:, mul_of(i, CW)])

    def attn_between(i):
        if i == 2:
            w_forward(GU0)

    rs(0, abuf, attn_chunk, attn_between)

    BL = 16

    def residual_rows(j):
        rows = mul_of(j, BL)
        a = abuf[rows, :]
        scale = lax.rsqrt(jnp.mean(a * a, axis=-1, keepdims=True) + eps_norm)
        mine = part(t * L + j * BL, BL)
        res = xall[mine, :].astype(f32) + a * scale * gat[...]
        cbuf[rows, :] = res
        rall[mine, :] = res.astype(bf16)

    loop(L // BL, residual_rows)
    NT = 256

    def turn(i):
        return ((i // 2 + s) % 2) * 2 + i % 2

    def gate_up(i):
        chunk = mul_of(turn(i), CW)

        def tile(n):
            at = mul_of(n, NT)
            value = dot_nn(rall[:, chunk], wgu[chunk, at])
            gu[:, at] = value if i == 0 else gu[:, at] + value

        loop(2 * fh // NT, tile)

    ag_start(rall, 1, turn(0))
    ag_start(rall, 1, turn(1))
    w_forward(GU0 + 1)
    ag_fwd(rall, 1, turn(0))
    ag_start(rall, 1, turn(2))
    ag_fwd(rall, 1, turn(1))
    ag_start(rall, 1, turn(3))
    for k in range(GU0, DN0):
        local_wait(k)
    ag_done(rall, 1, turn(0))
    w_forward(GU0 + 2)
    gate_up(0)
    ag_fwd(rall, 1, turn(2))
    ag_done(rall, 1, turn(1))
    ag_fwd(rall, 1, turn(3))
    gate_up(1)
    ag_done(rall, 1, turn(2))
    w_forward(GU0 + 3)
    for k in range(GU0, DN0):
        share(k).wait_recv()
    gate_up(2)
    ag_done(rall, 1, turn(3))
    gate_up(3)
    ag_drain(rall, 1)

    def hidden(n):
        g_at, u_at = mul_of(n, NT), part(fh + n * NT, NT)

        def rows_of(j):
            rows = mul_of(j, 64)
            g, u = gu[rows, g_at], gu[rows, u_at]
            hid[rows, g_at] = (g * jax.nn.sigmoid(g) * u).astype(bf16)

        loop(T // 64, rows_of)

    loop(fh // NT, hidden)
    def down_chunk(i):
        w_forward(DN0 + i)
        w_ready(DN0 + i)
        acc[...] = dot_nn(hid[...], wd[:, mul_of(i, CW)])

    rs(1, bbuf, down_chunk)
    own_cot.wait()

    def output_rows(j):
        rows = mul_of(j, BL)
        dn = bbuf[rows, :]
        scale = lax.rsqrt(jnp.mean(dn * dn, axis=-1, keepdims=True) + eps_norm)
        outb[rows, :] = (cbuf[rows, :] + dn * scale * gml[...]).astype(bf16)
        co = cot[rows, :].astype(f32)
        weighted = co * gml[...]
        inner = jnp.mean(weighted * dn, axis=-1, keepdims=True)
        gd = scale * weighted - dn * scale**3 * inner
        gdall[part(t * L + j * BL, BL), :] = gd.astype(bf16)
        gsum[:, D:2 * D] += jnp.sum(co * dn * scale, axis=0, keepdims=True)

    loop(L // BL, output_rows)
    put_out = pltpu.make_async_copy(outb, out_h, loc.at[3])
    put_out.start()
    half_q = 3 * ha // 2

    def by_cols(left, right, width):
        def make(row, n, core_, i):
            return dot_tn(left[:, part(row, n)], right[:, mul_of(core_, width)])
        return make

    def down_grad(row, n, core_, i):
        start = (row // unit) * 2 * unit + core_ * unit if d.direct else core_ * (fh // 2) + row
        return dot_tn(hid[:, part(start, n)], gdall[:, mul_of(i, CW)])

    ND, NG2, NQ, NO = range(4)
    sets = (
        (down_grad, rc_d, rx_d, rh_d, fh // 2, 128, 128, CHUNKS, stage_d),
        (by_cols(rall, gg2, fh), rc_gu, rx_gu, rh_gu, D, 256, 128, 1, stage),
        (by_cols(xall, gqkv, half_q), rc_q, rx_q, rh_q, D, 256, 256, 1, stage),
        (by_cols(mixed, gaall, D // 2), rc_o, rx_o, None, ha, 128, 128, 1, stage),
    )
    top = hi // (his // 2)

    def half_of(k):
        return sets[k][4] // 2

    def tiles_of(k):
        return half_of(k) // sets[k][5]

    def moves_of(k):
        return half_of(k) // sets[k][6]

    def place(k, j, n):
        count = half_of(k) // n
        if count < 2:
            return j * n
        return ((j + (1 - top) * (count // 2)) % count) * n

    def whole_row(k, j):
        tiles = tiles_of(k)
        late = j // tiles
        return (late * s + (1 - late) * (1 - s)) * half_of(k) + place(k, j % tiles, sets[k][5])

    def cols(k, i):
        return mul_of(i, CW) if sets[k][7] > 1 else pl.ds(0, sets[k][1].shape[1])

    def core_copy(k, j, i, slot):
        buf, n, st = sets[k][1], sets[k][5], sets[k][8]
        row = whole_row(k, j)
        w = CW if sets[k][7] > 1 else buf.shape[1]
        return send(st.at[slot, 0:n, 0:w], buf.at[part(row, n), cols(k, i)], stg_s.at[0 if k == ND else 1, slot],
                    c_r.at[k, (row // n) * sets[k][7] + i], dev_c)

    def give_down(late, i):
        def tile(j):
            slot = 4 * (i % 2) + j
            if i >= 2:
                core_copy(ND, j, i - 2, slot).wait_send()
            stage_d[slot] = down_grad(whole_row(ND, j), 128, 1 - core, i).astype(bf16)
            core_copy(ND, j, i, slot).start()

        n = tiles_of(ND)
        loop(n * (late + 1), tile, n * late)

    before = {NG2: None, NO: NG2, NQ: NO}

    def give(k, j):
        make, buf, n = sets[k][0], sets[k][1], sets[k][5]
        slot = j % 2
        if before[k] is not None:
            @pl.when(j < 2)
            def _():
                core_copy(before[k], j, 0, slot).wait_send()

        if 2 * tiles_of(k) > 2:
            @pl.when(j >= 2)
            def _():
                core_copy(k, j, 0, slot).wait_send()

        stage[slot, 0:n, 0:buf.shape[1]] = make(whole_row(k, j), n, 1 - core, 0).astype(bf16)
        core_copy(k, j, 0, slot).start()

    def x_copy(k, q):
        _, buf, far, _, _, _, m, _, _ = sets[k]
        i, j = q // moves_of(k), q % moves_of(k)
        row = place(k, j, m)
        return send(buf.at[part((1 - s) * half_of(k) + row, m), cols(k, i)], far.at[part(row, m), cols(k, i)],
                    x_s.at[k, q], x_r.at[k, q], dev_x)

    def take(k, j, i=0):
        make, buf, n, m = sets[k][0], sets[k][1], sets[k][5], sets[k][6]
        rows, at = part(whole_row(k, j), n), cols(k, i)
        core_copy(k, j, i, 0).wait_recv()
        buf[rows, at] = (make(whole_row(k, j), n, core, i) + buf[rows, at].astype(f32)).astype(bf16)

        @pl.when(j < tiles_of(k))
        def _():
            for e in range(n // m):
                x_copy(k, i * moves_of(k) + j * (n // m) + e).start()

    def takes(k, j0, j1, i=0):
        loop(j1, lambda j: take(k, j, i), j0)

    def gives(k, j0, j1):
        loop(j1, lambda j: give(k, j), j0)

    def hi_first(k, q):
        _, buf, _, back, _, _, m, _, _ = sets[k]
        per = moves_of(k) // 2
        i, j = q // per, q % per
        other = hi + (his // 2) * (1 - 2 * top)
        return send(buf.at[part(s * half_of(k) + place(k, j, m), m), cols(k, i)], back.at[mul_of(j, m), cols(k, i)],
                    h0_s.at[k, q], h0_r.at[k, q], (s, rep(other, t, core)))

    edge = tz == top
    relays = (relay_d, relay_gu, relay_q)

    def relay_in(k, q):
        _, buf, _, _, _, _, m, _, _ = sets[k]
        per = moves_of(k) // 2
        i, j = q // per, q % per
        return send(buf.at[part(s * half_of(k) + place(k, j, m), m), cols(k, i)], relays[k].at[mul_of(j, m), cols(k, i)],
                    rl_s.at[k, q], rl_r.at[k, q], dev_z)

    def relay_out(k, q):
        _, _, _, back, _, _, m, _, _ = sets[k]
        per = moves_of(k) // 2
        i, j = q // per, q % per
        other = hi + (his // 2) * (1 - 2 * top)
        at = (mul_of(j, m), cols(k, i))
        return send(relays[k].at[at], back.at[at], rf_s.at[k, q], h0_r.at[k, q], (s, rep(other, t_z, core)))

    def hi_send(k, q):
        @pl.when(edge)
        def _():
            relay_in(k, q).start()

        @pl.when(jnp.logical_not(edge))
        def _():
            hi_first(k, q).start()

    def relay(k, q0, q1):
        @pl.when(jnp.logical_not(edge))
        def _():
            def piece(q):
                relay_in(k, q).wait_recv()
                relay_out(k, q).start()

            loop(q1, piece, q0)

    def add_rows(buf, row, far, far_row, n, at, final=None):
        step = min(n, 64)

        def rows_of(j):
            rows = part(row + j * step, step)
            ours, theirs_ = buf[rows, at], far[part(far_row + j * step, step), at]
            if final is None:
                buf[rows, at] = ours + theirs_
            else:
                final[mul_of(j, step), at] = ours.astype(f32) + theirs_.astype(f32)

        loop(n // step, rows_of)

    def x_add(k, q0, q1):
        _, buf, far, _, _, _, m, _, _ = sets[k]

        def piece(q):
            i, j = q // moves_of(k), q % moves_of(k)
            row = place(k, j, m)
            x_copy(k, q).wait_recv()
            add_rows(buf, s * half_of(k) + row, far, row, m, cols(k, i))
            if k != NO:
                @pl.when(j < moves_of(k) // 2)
                def _():
                    hi_send(k, i * (moves_of(k) // 2) + j)

        loop(q1, piece, q0)

    def hi_later(k):
        half = half_of(k)
        base, size, at, out = top * (half // 2), half // 2, half // 2, []
        for level in range(1, d.levels):
            size //= 2
            weight = his >> (level + 1)
            bit = (hi // weight) % 2
            out.append((level - 1, base + (1 - bit) * size, base + bit * size, size, at, hi + weight * (1 - 2 * bit)))
            base = base + bit * size
            at += size
        return out, base, size

    def hi_copy(k, step):
        level, far_row, _, size, at, other = step
        return send(sets[k][1].at[part(s * half_of(k) + far_row, size)], sets[k][3].at[pl.ds(at, size)],
                    h_s.at[k, level], h_r.at[k, level], (s, rep(other, t, core)))

    def hi_finish(k, final=None):
        _, buf, _, back, _, _, m, chunks, _ = sets[k]
        per = moves_of(k) // 2
        last = final if d.levels == 1 else None

        def piece(q):
            i, j = q // per, q % per
            hi_first(k, q).wait_recv()
            add_rows(buf, s * half_of(k) + place(k, j + per, m), back, j * m, m, cols(k, i), last)

        assert last is None or per == 1
        loop(per * chunks, piece)
        later = hi_later(k)[0]
        for step in later:
            hi_copy(k, step).start()
            hi_copy(k, step).wait_recv()
            add_rows(buf, s * half_of(k) + step[2], back, step[4], step[3], pl.ds(0, buf.shape[1]),
                     final if step is later[-1] else None)

    me = t * CORES + core

    def kept(k, slot):
        return gg2.at[part(slot * d.own, d.own), pl.ds(0, fh) if k == NG2 else pl.ds(fh, half_q)]

    def keep_start(k):
        base = hi_later(k)[1]

        def piece(p):
            src = sets[k][1].at[part(s * half_of(k) + base + p * d.own, d.own)]

            @pl.when(me != p)
            def _():
                send(src, kept(k, me), a_s.at[k - 1, p], a_r.at[k - 1, me], (s, rep(hi, p // CORES, p % CORES))).start()

            @pl.when(me == p)
            def _():
                pltpu.make_async_copy(src, kept(k, me), a_r.at[k - 1, me]).start()

        loop(TP * CORES, piece)

    def keep_out(k, p):
        rows = part(p * d.own, d.own)
        if k == NQ:
            for c in range(3):
                e = (p % CORES) * 3 + c
                yield (gg2.at[rows, pl.ds(fh + c * HD, HD)],
                       qkv_h.at[e // 2, :, part(((e % 2) * TP + p // CORES) * HD, HD)])
        elif d.direct:
            w = 2 * unit
            for c in range(d.S * his):
                yield gg2.at[rows, pl.ds(c * w, w)], gu_h.at[p % CORES, :, part((c * TP + p // CORES) * w, w)]
        else:
            yield gg2.at[rows, pl.ds(0, fh)], gu_h.at[p]

    def keep_wait(k):
        def piece(p):
            pltpu.make_async_copy(kept(k, p), kept(k, p), a_r.at[k - 1, p]).wait()
            for src, dst in keep_out(k, p):
                pltpu.make_async_copy(src, dst, ko.at[k - 1, p]).start()

        loop(TP * CORES, piece)

    def keep_end(k):
        def piece(p):
            pltpu.make_async_copy(kept(k, p), kept(k, p), ko.at[k - 1, p]).wait()

            @pl.when(me != p)
            def _():
                send(kept(k, p), kept(k, p), a_s.at[k - 1, p], a_r.at[k - 1, me], (s, rep(hi, p // CORES, p % CORES))).wait_send()

        loop(TP * CORES, piece)

    partners = [dev_c, dev_x]
    for level in range(d.levels):
        weight = his >> (level + 1)
        bit = (hi // weight) % 2
        partners.append((s, rep(hi + weight * (1 - 2 * bit), t, core)))
    partners += [dev_y, dev_z]

    def gain_copy(n):
        return send(gsum, grecv.at[n], gn_s.at[n], gn_r.at[n], partners[n])

    def gain_step(n):
        if n:
            gain_copy(n - 1).wait_send()
            gain_copy(n - 1).wait_recv()
            gsum[...] += grecv[n - 1]
        if n < len(partners):
            gain_copy(n).start()

    ag_start(gdall, 2, 0)
    ag_start(gdall, 2, 1)
    ag_fwd(gdall, 2, 0)
    ag_start(gdall, 2, 2)
    ag_fwd(gdall, 2, 1)
    ag_start(gdall, 2, 3)
    def grad_hidden(i):
        chunk = pl.ds(i * CW, CW)

        def tile(n):
            at = mul_of(n, NT)
            value = dot_nt(gdall[:, chunk], wd[at, chunk])
            acc[:, at] = value if i == 0 else acc[:, at] + value
            value = dot_nt(gdall[:, chunk], wd[part(CW + n * NT, NT), chunk]).reshape(TP, L, NT)
            k2[:, :, at] = value if i == 0 else k2[:, :, at] + value

        loop(CW // NT, tile)

    for i in range(CHUNKS):
        ag_done(gdall, 2, i)
        if i + 2 < CHUNKS:
            ag_fwd(gdall, 2, i + 2)
        give_down(0, i)
        grad_hidden(i)
        if i:
            takes(ND, 0, 2, i - 1)
    ag_drain(gdall, 2)

    def hidden_back(half):
        step = L // 2

        def tile(n):
            at = mul_of(n, NT)
            g_at, u_at = part(half * CW + n * NT, NT), part(fh + half * CW + n * NT, NT)

            def rows_of(j):
                rows = mul_of(j, step)
                g, u = gu[rows, g_at], gu[rows, u_at]
                gh = k2[j // 2, mul_of(j % 2, step), at] if half else acc[rows, at]
                sig = jax.nn.sigmoid(g)
                gg2[rows, g_at] = (gh * u * sig * (1.0 + g * (1.0 - sig))).astype(bf16)
                gg2[rows, u_at] = (gh * (g * sig)).astype(bf16)

            loop(T // step, rows_of)

        loop(CW // NT, tile)

    hidden_back(0)
    hidden_back(1)
    takes(ND, 0, 2, CHUNKS - 1)

    def res_chunk(i):
        acc[...] = dot_nt(gg2[...], wgu[mul_of(i, CW), :])

    def res_extra(i):
        give(NG2, i)

        @pl.when(i > 0)
        def _():
            take(NG2, i - 1)

    def res_between(i):
        if i == 0:
            take(NG2, 3)
            give_down(1, 0)
            give_down(1, 1)
        elif i == 1:
            give_down(1, 2)
            give_down(1, 3)
        else:
            for c in range(CHUNKS):
                takes(ND, 2, 4, c)
            x_add(ND, 0, 4)
            gives(NG2, 4, 8)

    rs(2, cbuf, res_chunk, res_between, res_extra)

    def attn_grad_rows(j):
        rows = mul_of(j, BL)
        gr = cbuf[rows, :] + cot[rows, :].astype(f32)
        cbuf[rows, :] = gr
        a = abuf[rows, :]
        scale = lax.rsqrt(jnp.mean(a * a, axis=-1, keepdims=True) + eps_norm)
        weighted = gr * gat[...]
        inner = jnp.mean(weighted * a, axis=-1, keepdims=True)
        ga = scale * weighted - a * scale**3 * inner
        gaall[part(t * L + j * BL, BL), :] = ga.astype(bf16)
        gsum[:, 0:D] += jnp.sum(gr * a * scale, axis=0, keepdims=True)

    loop(L // BL, attn_grad_rows)

    def attend_back(b):
        rows = blk(b)
        acc[rows, 0:ha] = dot_nt(gaall[rows, :], wo[...])
        scale = columns(2, b)
        cos, sin = cos_v[...], sin_v[...]
        for h in range(heads):
            head = pl.ds(h * HD, HD)
            gm = acc[rows, head].astype(bf16)
            p = probs[b * heads + h]
            gqkv[rows, pl.ds(2 * ha + h * HD, HD)] = dot_tn(p.astype(bf16), gm).astype(bf16)
            gp = dot_nt(gm, vb[rows, head])
            gs = p * (gp - jnp.sum(p * gp, axis=-1, keepdims=True))
            gs = (gs * inv).astype(bf16)
            turned = (dot_nn(gs, qkrot[rows, pl.ds(ha + h * HD, HD)]), dot_tn(gs, qkrot[rows, head]))
            for which in range(2):
                at = pl.ds(which * ha + h * HD, HD)
                gn = turned[which] * cos - pltpu.roll(turned[which], HD // 2, 1) * sin
                field = qk[rows, at]
                spot = part(2 * D + which * d.att + t * ha + h * HD, HD)
                gsum[:, spot] += jnp.sum(gn * field * scale[which], axis=0, keepdims=True)
                gu[rows, at] = gn * gain_of(which, h)

    for i in range(CHUNKS):
        ag_start(gaall, 3, i)
    attend_back(t)
    ag_fwd(gaall, 3, 0)
    takes(NG2, 4, 6)
    ag_fwd(gaall, 3, 1)
    takes(NG2, 6, 8)
    ag_fwd(gaall, 3, 2)
    ag_fwd(gaall, 3, 3)
    x_add(ND, 4, 8)
    relay(ND, 0, 2)
    x_add(NG2, 0, 1)
    loop(2, lambda j: attend_back(t_y + j * (t_z - t_y)))
    for i in range(CHUNKS):
        ag_done(gaall, 3, i)
    attend_back(t_d)
    gives(NO, 0, 2)
    relay(ND, 2, 4)
    ag_drain(gaall, 3)

    def products(rows):
        return gu[rows, 0:2 * ha] * qk[rows, :]

    def in_stat():
        takes(NO, 0, 2)
        x_add(NG2, 1, 2)

    stat[3] = stat_sum(1, products, in_stat) / d.att
    gain_step(0)

    def qk_back(b):
        rows = blk(b)
        scale, inner = columns(2, b), columns(3, b)
        for which in range(2):
            at = pl.ds(which * ha, ha)
            sc = scale[which]
            gqkv[rows, at] = (sc * gu[rows, at] - qk[rows, at] * (sc**3 * inner[which])).astype(bf16)

    loop(TP, qk_back)
    gain_step(1)

    def in_chunk(i):
        acc[...] = dot_nt(gqkv[...], wqkv[mul_of(i, CW), :])

    def in_extra(i):
        give(NQ, i)

        @pl.when(i == 2)
        def _():
            x_add(NG2, 2, 3)

        @pl.when(i > 0)
        def _():
            take(NQ, i - 1)

    def in_between(i):
        if i == 0:
            take(NQ, 3)
            relay(NG2, 0, 2)
            gives(NQ, 4, 8)
            gain_step(2)
        elif i == 1:
            takes(NQ, 4, 8)
            gain_step(3)
        else:
            x_add(NG2, 3, 8)
            x_add(NQ, 0, 2)
            relay(NG2, 2, 3)
            hi_finish(ND, abuf)
            pltpu.make_async_copy(abuf.at[0:unit], down_h, loc.at[4]).start()
            gain_step(4)

    rs(3, bbuf, in_chunk, in_between, in_extra)

    def input_rows(j):
        rows = mul_of(j, BL)
        bbuf[rows, :] += cbuf[rows, :]

    loop(L // BL, input_rows)
    put_gin = pltpu.make_async_copy(bbuf, gin_h, loc.at[5])
    put_gin.start()

    relay(NG2, 3, 4)
    x_add(NQ, 2, 4)
    relay(NQ, 0, 2)
    x_add(NO, 0, 1)
    hi_finish(NG2)
    keep_start(NG2)

    for p in range(d.pieces):
        o_pc[p] = rc_o[part(s * HD + p * d.own_o, d.own_o), :]
    o_slot = hi * CORES + core

    def o_start(p):
        goal = t * d.pieces + p

        @pl.when(goal != r)
        def _():
            send(o_pc.at[p], o_h.at[o_slot], o_s.at[p], o_r.at[o_slot], (s, goal)).start()

        @pl.when(goal == r)
        def _():
            pltpu.make_async_copy(o_pc.at[p], o_h.at[o_slot], o_r.at[o_slot]).start()

    loop(d.pieces, o_start)
    hi_finish(NQ)
    keep_start(NQ)
    for n in range(5, len(partners) + 1):
        gain_step(n)
    gg_o[...] = gsum[...]

    keep_wait(NG2)
    keep_wait(NQ)
    keep_end(NG2)
    keep_end(NQ)

    def o_wait(q):
        pltpu.make_async_copy(o_pc.at[0], o_pc.at[0], o_r.at[q]).wait()

    loop(his * CORES, o_wait)

    def o_sent(p):
        goal = t * d.pieces + p

        @pl.when(goal != r)
        def _():
            send(o_pc.at[p], o_h.at[o_slot], o_s.at[p], o_r.at[o_slot], (s, goal)).wait_send()

    loop(d.pieces, o_sent)
    far_gain.wait_send()
    for k in range(NG):
        cross(k).wait_send()
        share(k).wait_send()
    for i in range(CHUNKS - 2, CHUNKS):
        loop(2 * tiles_of(ND), lambda j: core_copy(ND, j, i, 4 * (i % 2) + j).wait_send())
    for slot in range(2):
        core_copy(NQ, slot, 0, slot).wait_send()
    for k in range(4):
        loop(moves_of(k) * sets[k][7], lambda q: x_copy(k, q).wait_send())
    for k in range(3):
        @pl.when(edge)
        def _():
            loop(moves_of(k) // 2 * sets[k][7], lambda q: relay_in(k, q).wait_send())

        @pl.when(jnp.logical_not(edge))
        def _():
            loop(moves_of(k) // 2 * sets[k][7], lambda q: (hi_first(k, q).wait_send(), relay_out(k, q).wait_send()))

        for step in hi_later(k)[0]:
            hi_copy(k, step).wait_send()
    put_out.wait()
    put_gin.wait()
    pltpu.make_async_copy(abuf.at[0:unit], down_h, loc.at[4]).wait()


def body(shards, replicas, x_in, cotangent, w_query, w_key, w_value, w_out, w_gate, w_up, w_down,
         gain_query, gain_key, gain_attn, gain_mlp):
    seqs, length, width = x_in.shape
    assert seqs == 1
    d = Dims(length, width, w_query.shape[1], w_gate.shape[1], shards, replicas)
    r = lax.axis_index("replica")
    s = lax.axis_index("shard")
    t = (r // CORES) % TP

    def at(array, axis, index):
        return lax.dynamic_index_in_dim(array, index, axis, keepdims=False)

    def hidden_cols(w):
        picked = at(w.reshape(w.shape[0], d.S, d.his, TP, CORES, d.unit), 3, t)
        return picked.transpose(0, 3, 1, 2, 4).reshape(w.shape[0], d.fh)

    if not d.direct:
        w_gate = jnp.concatenate([hidden_cols(w_gate), hidden_cols(w_up)], axis=1)
        w_down = at(w_down.reshape(d.his, TP, CORES, d.unit, width), 1, t).transpose(1, 0, 2, 3).reshape(-1, width)
    gain = jnp.concatenate([at(gain_query.reshape(TP, HD), 0, t), at(gain_key.reshape(TP, HD), 0, t),
                            gain_attn, gain_mlp]).astype(f32)[None]
    cos, sin = rope_tables(length, HD // 2)
    cos = np.concatenate([cos, cos], axis=1)
    sin = np.concatenate([-sin, sin], axis=1)

    L, D, T, ha, fh = d.L, d.D, d.T, d.ha, d.fh
    CW = D // CHUNKS
    vm = pltpu.VMEM
    dma = pltpu.SemaphoreType.DMA
    any_ = pl.BlockSpec(memory_space=pl.ANY)
    vmem = pl.BlockSpec(memory_space=pltpu.VMEM)
    hi_rows = lambda n: max(n - n // d.his, 16)
    steps = 4 + d.levels
    later = max(d.levels - 1, 1)
    scratch = [
        vm((D, 3 * ha), bf16), vm((ha, D), bf16), vm((D, 2 * fh), bf16), vm((fh, D), bf16),
        vm((2, 1, d.gains), f32), vm((1, D), f32), vm((1, D), f32),
        vm((T, D), bf16), vm((T, D), bf16), vm((T, D), bf16), vm((T, D), bf16), vm((L, D), bf16),
        vm((T, 2 * ha), f32), vm((T, ha), bf16), vm((T, 2 * ha), bf16), vm((TP * ha // HD, L, L), f32),
        vm((T, ha), bf16), vm((T, 3 * ha), bf16), vm((4, 8, T), f32), vm((2, 3, 8, T), f32),
        vm((T, 2 * fh), f32), vm((T, fh), bf16), vm((T, 2 * fh), bf16),
        vm((L, D), f32), vm((L, D), f32), vm((L, D), f32), vm((L, D), bf16),
        vm((T, CW), f32), vm((CHUNKS, 2, L, CW), bf16), vm((CHUNKS, L, CW), bf16),
        vm((CHUNKS, 2, L, CW), bf16), vm((CHUNKS, L, CW), bf16), vm((CHUNKS, L, CW), f32),
        vm((8, 128, CW), bf16), vm((2, 256, fh), bf16),
        vm((D, fh), bf16), vm((fh // 2, D), bf16), vm((D, 3 * ha // 2), bf16), vm((ha, D // 2), bf16),
        vm((D // 2, fh), bf16), vm((fh // 4, D), bf16), vm((D // 2, 3 * ha // 2), bf16), vm((ha // 2, D // 2), bf16),
        vm((hi_rows(D // 2), fh), bf16), vm((hi_rows(fh // 4), D), bf16), vm((hi_rows(D // 2), 3 * ha // 2), bf16),
        vm((d.pieces, d.own_o, D // 2), bf16),
        vm((1, d.ggs), f32), vm((steps, 1, d.ggs), f32),
        dma((4, CHUNKS, 4)), dma((4, CHUNKS, 4)), dma((4, CHUNKS, 4)), dma((4, CHUNKS, 4)),
        dma((11,)), dma((11,)), dma((10,)), dma((10,)), dma((10, 2)), dma((6,)), dma((2, 3)), dma((2, 3)),
        dma((2, 8)), dma((4, 16)), dma((4, 8)), dma((4, 8)), dma((3, 4)), dma((3, 4)), dma((3, 4)), dma((3, 4)), dma((3, 4)),
        dma((3, later)), dma((3, later)),
        dma((2, TP * CORES)), dma((2, TP * CORES)), dma((2, TP * CORES)), dma((d.pieces,)), dma((d.his * CORES,)), dma((steps,)), dma((steps,)),
    ]
    struct = jax.ShapeDtypeStruct
    gu_shape = (2, d.own, d.ff) if d.direct else (TP * CORES, d.own, fh)
    results = pl.pallas_call(
        functools.partial(kernel, d),
        out_shape=(
            struct((L, D), bf16), struct((L, D), f32), struct(gu_shape, bf16), struct((3, d.own, d.att), bf16),
            struct((d.unit, D), f32), struct((d.his * CORES, d.own_o, D // 2), bf16),
            struct((fh // 8, D), bf16), struct((D // 4, fh), bf16), struct((D // 4, 3 * ha // 2), bf16),
            struct((1, d.ggs), f32),
        ),
        in_specs=[any_] * 9 + [vmem] * 3,
        out_specs=(any_,) * 9 + (vmem,),
        scratch_shapes=scratch,
        compiler_params=pltpu.CompilerParams(
            collective_id=0, has_side_effects=True, vmem_limit_bytes=67043328),
        name="layer",
    )(x_in[0], cotangent[0], w_query, w_key, w_value, w_out, w_gate, w_up, w_down, gain, cos, sin)
    out, gin, gu, qkv, down, o = results[:6]
    gg = results[-1]

    def hidden_out(k):
        if d.direct:
            return gu[k].astype(f32)
        block = gu.reshape(TP, CORES, d.own, fh)[:, k]
        spread = block.reshape(TP, d.own, CORES, d.S, d.his, d.unit).transpose(1, 3, 4, 0, 2, 5)
        return spread.reshape(d.own, d.ff).astype(f32)

    o = o.reshape(d.his, CORES, d.own_o, D // 2).astype(f32).sum(0).transpose(1, 0, 2).reshape(d.own_o, D)
    gg = gg[0]
    here = s * d.R + r

    def share(vec):
        n = vec.shape[0] // (d.S * d.R)
        return lax.dynamic_slice_in_dim(vec, here * n, n)

    def head_gain(vec):
        return share(vec.reshape(TP, d.S, HD).transpose(1, 0, 2).reshape(-1))

    return (
        out[None], gin[None], qkv[0].astype(f32), qkv[1].astype(f32), qkv[2].astype(f32), o,
        hidden_out(0), hidden_out(1), down,
        head_gain(gg[2 * D:2 * D + d.att]), head_gain(gg[2 * D + d.att:]), share(gg[:D]), share(gg[D:2 * D]),
    )


def solution(mesh):
    both = ("shard", "replica")
    token = P(both, None, None)
    weight = P("shard", None)
    return jax.shard_map(
        functools.partial(body, mesh.shape["shard"], mesh.shape["replica"]),
        mesh=mesh,
        in_specs=(token, token) + (weight,) * 7 + (P("shard"),) * 4,
        out_specs=(token, token) + (P(both, None),) * 7 + (P(both),) * 4,
        check_vma=False,
    )
```

```python
import functools
import math

import jax
import jax.numpy as jnp
import numpy as np
from jax import lax
from jax.experimental import pallas as pl
from jax.experimental.pallas import tpu as pltpu
from jax.sharding import PartitionSpec as P

HD = 128
TP = 4
CORES = 2
CHUNKS = 4
Z_AG = (256, 256, 256, 0)
Z_RS = (256, 256, 256, 128)

eps_norm = 1e-06
rope_theta = 500000.0

bf16 = jnp.bfloat16
f32 = jnp.float32


def rope_tables(length, half):
    position = np.arange(length).astype(np.float32)[:, None]
    exponent = np.arange(half).astype(np.float32) * np.float32(1.0 / half)
    angle = position * np.float32(rope_theta) ** (-exponent)
    return (np.cos(angle).astype(np.float32), np.sin(angle).astype(np.float32))


def dot_nn(left, right):
    return lax.dot_general(left, right, (((1,), (0,)), ((), ())), preferred_element_type=f32)


def dot_nt(left, right, precision=None):
    return lax.dot_general(
        left, right, (((1,), (1,)), ((), ())), preferred_element_type=f32, precision=precision)


def dot_tn(left, right):
    return lax.dot_general(left, right, (((0,), (0,)), ((), ())), preferred_element_type=f32)


def mul_of(index, step):
    return pl.ds(pl.multiple_of(index * step, step), step)


def loop(count, step, start=0):
    lax.fori_loop(start, count, lambda i, c: (step(i), c)[1], 0)


class Dims:
    def __init__(self, length, width, att, ff, shards, replicas):
        self.L, self.D, self.att, self.ff = length, width, att, ff
        self.S, self.R = shards, replicas
        self.his = replicas // (TP * CORES)
        self.T = TP * length
        self.ha = att // TP
        self.fh = ff // TP
        self.unit = ff // (shards * replicas)
        self.own = width // (shards * replicas)
        self.own_o = att // (shards * replicas)
        self.pieces = HD // self.own_o
        self.levels = self.his.bit_length() - 1
        self.gains = 2 * HD + width
        self.ggs = 2 * width + 2 * att
        self.direct = self.unit % 128 == 0
        assert shards == 2 and self.his == 1 << self.levels and self.levels > 0 and self.ha == shards * HD
        assert self.fh == 2 * (width // CHUNKS)


def kernel(
    d,
    x_h, cot_h, wq_h, wk_h, wv_h, wo_h, wg_h, wu_h, wd_h, gain_v, cos_v, sin_v,
    out_h, gin_h, gu_h, qkv_h, down_h, o_h, relay_d, relay_gu, relay_q, gg_o,
    wqkv, wo, wgu, wd, gbuf, gat, gml,
    xall, rall, gdall, gaall, cot,
    qk, vb, qkrot, probs, mixed, gqkv, stat, statr,
    gu, hid, gg2,
    abuf, bbuf, cbuf, outb,
    acc, s1, s2, r1, r2, k2,
    stage_d, stage, rc_gu, rc_d, rc_q, rc_o, rx_gu, rx_d, rx_q, rx_o, rh_gu, rh_d, rh_q, o_pc,
    gsum, grecv,
    ag_s, ag_r, rs_s, rs_r, w_s, w_r, wf_s, wf_r, w_l, loc, st_s, st_r,
    stg_s, c_r, x_s, x_r, h0_s, h0_r, rl_s, rl_r, rf_s, h_s, h_r, a_s, a_r, ko, o_s, o_r, gn_s, gn_r,
):
    L, D, T, ha, fh, his, unit = d.L, d.D, d.T, d.ha, d.fh, d.his, d.unit
    CW = D // CHUNKS
    HW = CW // 2
    s = lax.axis_index("shard")
    r = lax.axis_index("replica")
    hi, t, core = r // (TP * CORES), (r // CORES) % TP, r % CORES
    tz, ty = t // 2, t % 2
    t_y, t_z, t_d = tz * 2 + 1 - ty, (1 - tz) * 2 + ty, (1 - tz) * 2 + 1 - ty

    def rep(hi_, t_, core_):
        return hi_ * (TP * CORES) + t_ * CORES + core_

    dev_y, dev_z, dev_d = ((s, rep(hi, q, core)) for q in (t_y, t_z, t_d))
    dev_x = (1 - s, r)
    dev_c = (s, rep(hi, t, 1 - core))

    def send(src, dst, ssem, rsem, dev):
        return pltpu.make_async_remote_copy(
            src_ref=src, dst_ref=dst, send_sem=ssem, recv_sem=rsem, device_id=dev,
            device_id_type=pl.DeviceIdType.MESH)

    def blk(q):
        return mul_of(q, L)

    def part(base, n):
        return pl.ds(pl.multiple_of(base, n), n)

    def ag_copies(buf, inst, i, src=None):
        own = buf.at[blk(t), mul_of(i, CW)]
        first = own if src is None else src.at[:, mul_of(i, CW)]
        wz = Z_AG[inst]
        fy = buf.at[blk(t_y), pl.ds(pl.multiple_of(i * CW + CW - wz, 128), wz)] if wz else None
        fz = buf.at[blk(t_z), pl.ds(pl.multiple_of(i * CW, 128), CW - wz)]
        ends = ((first, own, dev_y), (first, own, dev_z), (fy, fy, dev_z), (fz, fz, dev_y))

        def copy(j):
            return send(ends[j][0], ends[j][1], ag_s.at[inst, i, j], ag_r.at[inst, i, j], ends[j][2])

        return copy

    def ag_start(buf, inst, i, src=None):
        c = ag_copies(buf, inst, i, src)
        c(0).start()
        c(1).start()

    def ag_fwd(buf, inst, i):
        c = ag_copies(buf, inst, i)
        c(1).wait_recv()
        c(3).start()
        c(0).wait_recv()
        if Z_AG[inst]:
            c(2).start()

    def ag_done(buf, inst, i):
        c = ag_copies(buf, inst, i)
        if Z_AG[inst]:
            c(2).wait_recv()
        c(3).wait_recv()

    def ag_drain(buf, inst):
        def wait(i):
            c = ag_copies(buf, inst, i)
            for j in range(4):
                if j != 2 or Z_AG[inst]:
                    c(j).wait_send()

        loop(CHUNKS, wait)

    def ag(buf, inst, src=None, between=lambda i: None):
        ag_start(buf, inst, 0, src)
        ag_start(buf, inst, 1, src)
        for i in range(CHUNKS):
            ag_fwd(buf, inst, i)
            if i + 2 < CHUNKS:
                ag_start(buf, inst, i + 2, src)
            between(i)
        for i in range(CHUNKS):
            ag_done(buf, inst, i)
        ag_drain(buf, inst)

    def rs_copies(inst, i):
        wa = CW - Z_RS[inst]
        ya, zb = pl.ds(0, wa), pl.ds(wa, CW - wa)

        def copy(j):
            if j == 0:
                a, b, dev = s1.at[i, :, :, ya], r1.at[i, :, :, ya], dev_y
            elif j == 1:
                a, b, dev = s1.at[i, :, :, zb], r1.at[i, :, :, zb], dev_z
            elif j == 2:
                a, b, dev = s2.at[i, :, ya], r2.at[i, :, ya], dev_z
            else:
                a, b, dev = s2.at[i, :, zb], r2.at[i, :, zb], dev_y
            return send(a, b, rs_s.at[inst, i, j], rs_r.at[inst, i, j], dev)

        return copy

    def rs_send(inst, i, dest):
        c = rs_copies(inst, i)
        wa = CW - Z_RS[inst]
        step = L // 4

        def rows_of(j):
            def rows(q):
                return part(q * L + j * step, step)

            here = mul_of(j, step)
            s1[i, 0, here, 0:wa] = acc[rows(t_y), 0:wa].astype(bf16)
            k2[i, here, 0:wa] = acc[rows(t_z), 0:wa]
            if wa < CW:
                s1[i, 0, here, wa:CW] = acc[rows(t_z), wa:CW].astype(bf16)
                k2[i, here, wa:CW] = acc[rows(t_y), wa:CW]
            s1[i, 1, here] = acc[rows(t_d), :].astype(bf16)
            dest[here, mul_of(i, CW)] = acc[rows(t), :]

        loop(4, rows_of)
        c(0).start()
        if wa < CW:
            c(1).start()

    def rs_fwd(inst, i, dest):
        c = rs_copies(inst, i)
        wa = CW - Z_RS[inst]
        c(0).wait_recv()
        s2[i, :, 0:wa] = (k2[i, :, 0:wa] + r1[i, 1, :, 0:wa].astype(f32)).astype(bf16)
        c(2).start()
        if wa < CW:
            c(1).wait_recv()
            s2[i, :, wa:CW] = (k2[i, :, wa:CW] + r1[i, 1, :, wa:CW].astype(f32)).astype(bf16)
            c(3).start()
        dest[:, mul_of(i, CW)] += r1[i, 0].astype(f32)

    def rs_done(inst, i, dest):
        c = rs_copies(inst, i)
        c(2).wait_recv()
        if Z_RS[inst]:
            c(3).wait_recv()
        dest[:, mul_of(i, CW)] += r2[i].astype(f32)

    def rs(inst, dest, compute, between=lambda i: None, extra=lambda i: None):
        def first(i):
            compute(i)
            rs_send(inst, i, dest)
            extra(i)

            @pl.when(i >= 2)
            def _():
                rs_fwd(inst, i - 2, dest)

        loop(CHUNKS, first)
        between(0)
        rs_fwd(inst, CHUNKS - 2, dest)
        between(1)
        rs_fwd(inst, CHUNKS - 1, dest)
        between(2)
        loop(CHUNKS, lambda i: rs_done(inst, i, dest))

        def wait(i):
            c = rs_copies(inst, i)
            for j in range(4):
                if j % 2 == 0 or Z_RS[inst]:
                    c(j).wait_send()

        loop(CHUNKS, wait)

    def qkv_region(s_, piece):
        return wqkv.at[part(s_ * (D // 2) + piece * (D // 4), D // 4)]

    def qkv_parts(s_, piece):
        rows, to = part(piece * (D // 4), D // 4), part(s_ * (D // 2) + piece * (D // 4), D // 4)
        for which, src in enumerate((wq_h, wk_h, wv_h)):
            for h in range(d.S):
                yield src.at[rows, part((h * TP + t) * HD, HD)], wqkv.at[to, pl.ds(which * ha + h * HD, HD)]

    def o_region(s_, piece):
        return wo.at[part(s_ * HD + piece * (HD // 2), HD // 2)]

    def o_parts(s_, piece):
        yield wo_h.at[part(t * HD + piece * (HD // 2), HD // 2)], o_region(s_, piece)

    SUBS = 4

    def gu_group(sub):
        n = D // 4 // SUBS

        def region(s_, piece):
            return wgu.at[part(s_ * (D // 2) + piece * (D // 4) + sub * n, n)]

        def parts(s_, piece):
            rows = part(piece * (D // 4) + sub * n, n)
            to = part(s_ * (D // 2) + piece * (D // 4) + sub * n, n)
            w = 2 * unit
            if not d.direct:
                yield wg_h.at[rows], wgu.at[to]
                return
            for m, src in enumerate((wg_h, wu_h)):
                for c in range(d.S * his):
                    yield src.at[rows, part((c * TP + t) * w, w)], wgu.at[to, pl.ds(m * fh + c * w, w)]

        return parts, region

    def d_group(sub):
        at = mul_of(sub, CW)
        n = fh // 4

        def region(s_, piece):
            return wd.at[part(((s_ * 2 + piece) if d.direct else (piece * 2 + s_)) * n, n), at]

        def parts(s_, piece):
            w = 2 * unit
            if not d.direct:
                yield wd_h.at[part(piece * n, n), at], region(s_, piece)
                return
            step = min(w, n)
            for e in range(n // step):
                first = piece * n + e * step
                src = (first // w) * (TP * w) + t * w + first % w
                yield wd_h.at[part(src, step), at], wd.at[part(s_ * (fh // 2) + first, step), at]

        return parts, region

    GU0, DN0 = 2, 2 + SUBS
    NG = DN0 + CHUNKS

    def group_of(k):
        if isinstance(k, int) and k < DN0:
            return ((qkv_parts, qkv_region), (o_parts, o_region))[k] if k < GU0 else gu_group(k - GU0)
        return d_group(k - DN0)

    def local_start(k):
        for piece in range(2):
            for src, dst in group_of(k)[0](s, piece):
                pltpu.make_async_copy(src, dst, w_l.at[k, piece]).start()

    def local_wait(k):
        for piece in range(2):
            here = group_of(k)[1](s, piece)
            pltpu.make_async_copy(here, here, w_l.at[k, piece]).wait()

    def cross_start(k):
        for src, dst in group_of(k)[0](s, core):
            send(src, dst, w_s.at[k], w_r.at[k], dev_x).start()

    def cross(k):
        here = group_of(k)[1](s, core)
        return send(here, here, w_s.at[k], w_r.at[k], dev_x)

    def share(k):
        here = group_of(k)[1](1 - s, core)
        return send(here, here, wf_s.at[k], wf_r.at[k], dev_c)

    def w_forward(k):
        cross(k).wait_recv()
        share(k).start()

    def w_ready(k):
        local_wait(k)
        share(k).wait_recv()

    own_x = pltpu.make_async_copy(x_h, xall.at[blk(t)], loc.at[0])
    own_cot = pltpu.make_async_copy(cot_h, cot, loc.at[1])
    own_gain = pltpu.make_async_copy(gain_v, gbuf.at[s], loc.at[2])
    far_gain = send(gain_v, gbuf.at[s], w_s.at[NG], w_r.at[NG], dev_x)
    own_x.start()
    local_start(0)
    own_gain.start()
    own_cot.start()

    barrier = pltpu.get_barrier_semaphore()

    def greet(q):
        @pl.when(q != r)
        def _():
            pl.semaphore_signal(barrier, inc=1, device_id=(s, q), device_id_type=pl.DeviceIdType.MESH)

    loop(d.R, greet)
    pl.semaphore_signal(barrier, inc=1, device_id=dev_x, device_id_type=pl.DeviceIdType.MESH)
    pl.semaphore_wait(barrier, d.R)

    ag_start(xall, 0, 0, x_h)
    cross_start(0)
    ag_start(xall, 0, 1, x_h)
    far_gain.start()
    for k in range(1, NG):
        cross_start(k)
    for k in range(1, NG):
        local_start(k)

    for i in range(CHUNKS):
        ag_fwd(xall, 0, i)
        if i + 2 < CHUNKS:
            ag_start(xall, 0, i + 2, x_h)
    w_forward(0)
    own_x.wait()
    own_gain.wait()
    far_gain.wait_recv()
    for q in range(2):
        gat[:, q * (D // 2):(q + 1) * (D // 2)] = gbuf[q, :, 2 * HD:2 * HD + D // 2]
        gml[:, q * (D // 2):(q + 1) * (D // 2)] = gbuf[q, :, 2 * HD + D // 2:]
    gsum[...] = jnp.zeros_like(gsum)
    for i in range(CHUNKS):
        ag_done(xall, 0, i)
    ag_drain(xall, 0)
    w_ready(0)

    qk[:, 0:ha] = dot_nn(xall[...], wqkv[:, 0:ha])
    qk[:, ha:2 * ha] = dot_nn(xall[...], wqkv[:, ha:2 * ha])
    vb[...] = dot_nn(xall[...], wqkv[:, 2 * ha:]).astype(bf16)

    row8 = lax.broadcasted_iota(jnp.int32, (8, 2 * ha), 0)
    col8 = lax.broadcasted_iota(jnp.int32, (8, 2 * ha), 1)
    pick = jnp.where((row8 < 4) == (col8 < ha), 1.0, 0.0).astype(f32)
    HIGH = lax.Precision.HIGHEST

    def stat_sum(k, values, between=lambda: None):
        def sequence(b):
            stat[k, :, blk(b)] = dot_nt(pick, values(blk(b)), HIGH)

        loop(TP, sequence)
        copies = [send(stat.at[k], statr.at[k, j], st_s.at[k, j], st_r.at[k, j], dev)
                  for j, dev in enumerate((dev_y, dev_z, dev_d))]
        for c in copies:
            c.start()
        between()
        for c in copies:
            c.wait_recv()
        for c in copies:
            c.wait_send()
        return stat[k] + statr[k, 0] + statr[k, 1] + statr[k, 2]

    def squares(rows):
        v = qk[rows, :]
        return v * v

    stat[2] = lax.rsqrt(stat_sum(0, squares) / d.att + eps_norm)

    def columns(k, b):
        flat = stat[k, :, blk(b)]
        wide = jnp.concatenate([flat] * (L // 8), axis=0).T
        return wide[:, 0:1], wide[:, 4:5]

    def gain_of(which, h):
        return gbuf[h, :, which * HD:(which + 1) * HD]

    inv = 1.0 / math.sqrt(HD)
    heads = ha // HD

    def attend(b):
        rows = blk(b)
        scale = columns(2, b)
        cos, sin = cos_v[...], sin_v[...]
        above = lax.broadcasted_iota(jnp.int32, (L, L), 0) < lax.broadcasted_iota(jnp.int32, (L, L), 1)
        for h in range(heads):
            rot = []
            for which in range(2):
                at = pl.ds(which * ha + h * HD, HD)
                normed = qk[rows, at] * scale[which] * gain_of(which, h)
                turned = (normed * cos + pltpu.roll(normed, HD // 2, 1) * sin).astype(bf16)
                qkrot[rows, at] = turned
                rot.append(turned)
            scores = jnp.where(above, -jnp.inf, dot_nt(rot[0], rot[1]) * inv)
            peak = jnp.max(scores, axis=-1, keepdims=True)
            log_total = peak + jnp.log(jnp.sum(jnp.exp(scores - peak), axis=-1, keepdims=True))
            p = jnp.exp(scores - log_total)
            probs[b * heads + h] = p
            head = pl.ds(h * HD, HD)
            mixed[rows, head] = dot_nn(p.astype(bf16), vb[rows, head]).astype(bf16)

    loop(TP, attend)
    w_forward(1)
    w_ready(1)

    def attn_chunk(i):
        acc[...] = dot_nn(mixed[...], wo[:, mul_of(i, CW)])

    def attn_between(i):
        if i == 2:
            w_forward(GU0)

    rs(0, abuf, attn_chunk, attn_between)

    BL = 16

    def residual_rows(j):
        rows = mul_of(j, BL)
        a = abuf[rows, :]
        scale = lax.rsqrt(jnp.mean(a * a, axis=-1, keepdims=True) + eps_norm)
        mine = part(t * L + j * BL, BL)
        res = xall[mine, :].astype(f32) + a * scale * gat[...]
        cbuf[rows, :] = res
        rall[mine, :] = res.astype(bf16)

    loop(L // BL, residual_rows)
    NT = 256

    def turn(i):
        return ((i // 2 + s) % 2) * 2 + i % 2

    def gate_up(i):
        chunk = mul_of(turn(i), CW)

        def tile(n):
            at = mul_of(n, NT)
            value = dot_nn(rall[:, chunk], wgu[chunk, at])
            gu[:, at] = value if i == 0 else gu[:, at] + value

        loop(2 * fh // NT, tile)

    ag_start(rall, 1, turn(0))
    ag_start(rall, 1, turn(1))
    w_forward(GU0 + 1)
    ag_fwd(rall, 1, turn(0))
    ag_start(rall, 1, turn(2))
    ag_fwd(rall, 1, turn(1))
    ag_start(rall, 1, turn(3))
    for k in range(GU0, DN0):
        local_wait(k)
    ag_done(rall, 1, turn(0))
    w_forward(GU0 + 2)
    gate_up(0)
    ag_fwd(rall, 1, turn(2))
    ag_done(rall, 1, turn(1))
    ag_fwd(rall, 1, turn(3))
    gate_up(1)
    ag_done(rall, 1, turn(2))
    w_forward(GU0 + 3)
    for k in range(GU0, DN0):
        share(k).wait_recv()
    gate_up(2)
    ag_done(rall, 1, turn(3))
    gate_up(3)
    ag_drain(rall, 1)

    def hidden(n):
        g_at, u_at = mul_of(n, NT), part(fh + n * NT, NT)

        def rows_of(j):
            rows = mul_of(j, 64)
            g, u = gu[rows, g_at], gu[rows, u_at]
            hid[rows, g_at] = (g * jax.nn.sigmoid(g) * u).astype(bf16)

        loop(T // 64, rows_of)

    loop(fh // NT, hidden)
    def down_chunk(i):
        w_forward(DN0 + i)
        w_ready(DN0 + i)
        acc[...] = dot_nn(hid[...], wd[:, mul_of(i, CW)])

    rs(1, bbuf, down_chunk)
    own_cot.wait()

    def output_rows(j):
        rows = mul_of(j, BL)
        dn = bbuf[rows, :]
        scale = lax.rsqrt(jnp.mean(dn * dn, axis=-1, keepdims=True) + eps_norm)
        outb[rows, :] = (cbuf[rows, :] + dn * scale * gml[...]).astype(bf16)
        co = cot[rows, :].astype(f32)
        weighted = co * gml[...]
        inner = jnp.mean(weighted * dn, axis=-1, keepdims=True)
        gd = scale * weighted - dn * scale**3 * inner
        gdall[part(t * L + j * BL, BL), :] = gd.astype(bf16)
        gsum[:, D:2 * D] += jnp.sum(co * dn * scale, axis=0, keepdims=True)

    loop(L // BL, output_rows)
    put_out = pltpu.make_async_copy(outb, out_h, loc.at[3])
    put_out.start()
    half_q = 3 * ha // 2

    def by_cols(left, right, width):
        def make(row, n, core_, i):
            return dot_tn(left[:, part(row, n)], right[:, mul_of(core_, width)])
        return make

    def down_grad(row, n, core_, i):
        start = (row // unit) * 2 * unit + core_ * unit if d.direct else core_ * (fh // 2) + row
        return dot_tn(hid[:, part(start, n)], gdall[:, mul_of(i, CW)])

    ND, NG2, NQ, NO = range(4)
    sets = (
        (down_grad, rc_d, rx_d, rh_d, fh // 2, 128, 128, CHUNKS, stage_d),
        (by_cols(rall, gg2, fh), rc_gu, rx_gu, rh_gu, D, 256, 128, 1, stage),
        (by_cols(xall, gqkv, half_q), rc_q, rx_q, rh_q, D, 256, 256, 1, stage),
        (by_cols(mixed, gaall, D // 2), rc_o, rx_o, None, ha, 128, 128, 1, stage),
    )
    top = hi // (his // 2)

    def half_of(k):
        return sets[k][4] // 2

    def tiles_of(k):
        return half_of(k) // sets[k][5]

    def moves_of(k):
        return half_of(k) // sets[k][6]

    def place(k, j, n):
        count = half_of(k) // n
        if count < 2:
            return j * n
        return ((j + (1 - top) * (count // 2)) % count) * n

    def whole_row(k, j):
        tiles = tiles_of(k)
        late = j // tiles
        return (late * s + (1 - late) * (1 - s)) * half_of(k) + place(k, j % tiles, sets[k][5])

    def cols(k, i):
        return mul_of(i, CW) if sets[k][7] > 1 else pl.ds(0, sets[k][1].shape[1])

    def core_copy(k, j, i, slot):
        buf, n, st = sets[k][1], sets[k][5], sets[k][8]
        row = whole_row(k, j)
        w = CW if sets[k][7] > 1 else buf.shape[1]
        return send(st.at[slot, 0:n, 0:w], buf.at[part(row, n), cols(k, i)], stg_s.at[0 if k == ND else 1, slot],
                    c_r.at[k, (row // n) * sets[k][7] + i], dev_c)

    def give_down(late, i):
        def tile(j):
            slot = 4 * (i % 2) + j
            if i >= 2:
                core_copy(ND, j, i - 2, slot).wait_send()
            stage_d[slot] = down_grad(whole_row(ND, j), 128, 1 - core, i).astype(bf16)
            core_copy(ND, j, i, slot).start()

        n = tiles_of(ND)
        loop(n * (late + 1), tile, n * late)

    before = {NG2: None, NO: NG2, NQ: NO}

    def give(k, j):
        make, buf, n = sets[k][0], sets[k][1], sets[k][5]
        slot = j % 2
        if before[k] is not None:
            @pl.when(j < 2)
            def _():
                core_copy(before[k], j, 0, slot).wait_send()

        if 2 * tiles_of(k) > 2:
            @pl.when(j >= 2)
            def _():
                core_copy(k, j, 0, slot).wait_send()

        stage[slot, 0:n, 0:buf.shape[1]] = make(whole_row(k, j), n, 1 - core, 0).astype(bf16)
        core_copy(k, j, 0, slot).start()

    def x_copy(k, q):
        _, buf, far, _, _, _, m, _, _ = sets[k]
        i, j = q // moves_of(k), q % moves_of(k)
        row = place(k, j, m)
        return send(buf.at[part((1 - s) * half_of(k) + row, m), cols(k, i)], far.at[part(row, m), cols(k, i)],
                    x_s.at[k, q], x_r.at[k, q], dev_x)

    def take(k, j, i=0):
        make, buf, n, m = sets[k][0], sets[k][1], sets[k][5], sets[k][6]
        rows, at = part(whole_row(k, j), n), cols(k, i)
        core_copy(k, j, i, 0).wait_recv()
        buf[rows, at] = (make(whole_row(k, j), n, core, i) + buf[rows, at].astype(f32)).astype(bf16)

        @pl.when(j < tiles_of(k))
        def _():
            for e in range(n // m):
                x_copy(k, i * moves_of(k) + j * (n // m) + e).start()

    def takes(k, j0, j1, i=0):
        loop(j1, lambda j: take(k, j, i), j0)

    def gives(k, j0, j1):
        loop(j1, lambda j: give(k, j), j0)

    def hi_first(k, q):
        _, buf, _, back, _, _, m, _, _ = sets[k]
        per = moves_of(k) // 2
        i, j = q // per, q % per
        other = hi + (his // 2) * (1 - 2 * top)
        return send(buf.at[part(s * half_of(k) + place(k, j, m), m), cols(k, i)], back.at[mul_of(j, m), cols(k, i)],
                    h0_s.at[k, q], h0_r.at[k, q], (s, rep(other, t, core)))

    edge = tz == top
    relays = (relay_d, relay_gu, relay_q)

    def relay_in(k, q):
        _, buf, _, _, _, _, m, _, _ = sets[k]
        per = moves_of(k) // 2
        i, j = q // per, q % per
        return send(buf.at[part(s * half_of(k) + place(k, j, m), m), cols(k, i)], relays[k].at[mul_of(j, m), cols(k, i)],
                    rl_s.at[k, q], rl_r.at[k, q], dev_z)

    def relay_out(k, q):
        _, _, _, back, _, _, m, _, _ = sets[k]
        per = moves_of(k) // 2
        i, j = q // per, q % per
        other = hi + (his // 2) * (1 - 2 * top)
        at = (mul_of(j, m), cols(k, i))
        return send(relays[k].at[at], back.at[at], rf_s.at[k, q], h0_r.at[k, q], (s, rep(other, t_z, core)))

    def hi_send(k, q):
        @pl.when(edge)
        def _():
            relay_in(k, q).start()

        @pl.when(jnp.logical_not(edge))
        def _():
            hi_first(k, q).start()

    def relay(k, q0, q1):
        @pl.when(jnp.logical_not(edge))
        def _():
            def piece(q):
                relay_in(k, q).wait_recv()
                relay_out(k, q).start()

            loop(q1, piece, q0)

    def add_rows(buf, row, far, far_row, n, at, final=None):
        step = min(n, 64)

        def rows_of(j):
            rows = part(row + j * step, step)
            ours, theirs_ = buf[rows, at], far[part(far_row + j * step, step), at]
            if final is None:
                buf[rows, at] = ours + theirs_
            else:
                final[mul_of(j, step), at] = ours.astype(f32) + theirs_.astype(f32)

        loop(n // step, rows_of)

    def x_add(k, q0, q1):
        _, buf, far, _, _, _, m, _, _ = sets[k]

        def piece(q):
            i, j = q // moves_of(k), q % moves_of(k)
            row = place(k, j, m)
            x_copy(k, q).wait_recv()
            add_rows(buf, s * half_of(k) + row, far, row, m, cols(k, i))
            if k != NO:
                @pl.when(j < moves_of(k) // 2)
                def _():
                    hi_send(k, i * (moves_of(k) // 2) + j)

        loop(q1, piece, q0)

    def hi_later(k):
        half = half_of(k)
        base, size, at, out = top * (half // 2), half // 2, half // 2, []
        for level in range(1, d.levels):
            size //= 2
            weight = his >> (level + 1)
            bit = (hi // weight) % 2
            out.append((level - 1, base + (1 - bit) * size, base + bit * size, size, at, hi + weight * (1 - 2 * bit)))
            base = base + bit * size
            at += size
        return out, base, size

    def hi_copy(k, step):
        level, far_row, _, size, at, other = step
        return send(sets[k][1].at[part(s * half_of(k) + far_row, size)], sets[k][3].at[pl.ds(at, size)],
                    h_s.at[k, level], h_r.at[k, level], (s, rep(other, t, core)))

    def hi_finish(k, final=None, then=None):
        _, buf, _, back, _, _, m, chunks, _ = sets[k]
        per = moves_of(k) // 2
        last = final if d.levels == 1 else None

        def piece(q):
            i, j = q // per, q % per
            hi_first(k, q).wait_recv()
            add_rows(buf, s * half_of(k) + place(k, j + per, m), back, j * m, m, cols(k, i), last)
            if then is not None and d.levels == 1:
                loop(m // d.own, lambda e: then(k, q * (m // d.own) + e))

        assert last is None or per == 1
        loop(per * chunks, piece)
        later = hi_later(k)[0]
        for step in later:
            hi_copy(k, step).start()
            hi_copy(k, step).wait_recv()
            add_rows(buf, s * half_of(k) + step[2], back, step[4], step[3], pl.ds(0, buf.shape[1]),
                     final if step is later[-1] else None)

    me = t * CORES + core

    def kept(k, slot):
        return gg2.at[part(slot * d.own, d.own), pl.ds(0, fh) if k == NG2 else pl.ds(fh, half_q)]

    def keep_piece(k, p):
        base = hi_later(k)[1]
        src = sets[k][1].at[part(s * half_of(k) + base + p * d.own, d.own)]

        @pl.when(me != p)
        def _():
            send(src, kept(k, me), a_s.at[k - 1, p], a_r.at[k - 1, me], (s, rep(hi, p // CORES, p % CORES))).start()

        @pl.when(me == p)
        def _():
            pltpu.make_async_copy(src, kept(k, me), a_r.at[k - 1, me]).start()

    def keep_start(k):
        loop(TP * CORES, lambda p: keep_piece(k, p))

    def keep_out(k, p):
        rows = part(p * d.own, d.own)
        if k == NQ:
            for c in range(3):
                e = (p % CORES) * 3 + c
                yield (gg2.at[rows, pl.ds(fh + c * HD, HD)],
                       qkv_h.at[e // 2, :, part(((e % 2) * TP + p // CORES) * HD, HD)])
        elif d.direct:
            w = 2 * unit
            for c in range(d.S * his):
                yield gg2.at[rows, pl.ds(c * w, w)], gu_h.at[p % CORES, :, part((c * TP + p // CORES) * w, w)]
        else:
            yield gg2.at[rows, pl.ds(0, fh)], gu_h.at[p]

    def keep_wait(k):
        def piece(p):
            pltpu.make_async_copy(kept(k, p), kept(k, p), a_r.at[k - 1, p]).wait()
            for src, dst in keep_out(k, p):
                pltpu.make_async_copy(src, dst, ko.at[k - 1, p]).start()

        loop(TP * CORES, piece)

    def keep_end(k):
        def piece(p):
            pltpu.make_async_copy(kept(k, p), kept(k, p), ko.at[k - 1, p]).wait()

            @pl.when(me != p)
            def _():
                send(kept(k, p), kept(k, p), a_s.at[k - 1, p], a_r.at[k - 1, me], (s, rep(hi, p // CORES, p % CORES))).wait_send()

        loop(TP * CORES, piece)

    partners = [dev_y, dev_z, dev_c, dev_x]
    for level in range(d.levels):
        weight = his >> (level + 1)
        bit = (hi // weight) % 2
        partners.append((s, rep(hi + weight * (1 - 2 * bit), t, core)))

    def gain_copy(n):
        return send(gsum, grecv.at[n], gn_s.at[n], gn_r.at[n], partners[n])

    def gain_step(n):
        if n:
            gain_copy(n - 1).wait_send()
            gain_copy(n - 1).wait_recv()
            gsum[...] += grecv[n - 1]
        if n < len(partners):
            gain_copy(n).start()

    ag_start(gdall, 2, 0)
    ag_start(gdall, 2, 1)
    ag_fwd(gdall, 2, 0)
    ag_start(gdall, 2, 2)
    ag_fwd(gdall, 2, 1)
    ag_start(gdall, 2, 3)
    def grad_hidden(i):
        chunk = pl.ds(i * CW, CW)

        def tile(n):
            at = mul_of(n, NT)
            value = dot_nt(gdall[:, chunk], wd[at, chunk])
            acc[:, at] = value if i == 0 else acc[:, at] + value
            value = dot_nt(gdall[:, chunk], wd[part(CW + n * NT, NT), chunk]).reshape(TP, L, NT)
            k2[:, :, at] = value if i == 0 else k2[:, :, at] + value

        loop(CW // NT, tile)

    for i in range(CHUNKS):
        ag_done(gdall, 2, i)
        if i + 2 < CHUNKS:
            ag_fwd(gdall, 2, i + 2)
        give_down(0, i)
        grad_hidden(i)
        if i:
            takes(ND, 0, 2, i - 1)
    ag_drain(gdall, 2)

    def hidden_back(half):
        step = L // 2

        def tile(n):
            at = mul_of(n, NT)
            g_at, u_at = part(half * CW + n * NT, NT), part(fh + half * CW + n * NT, NT)

            def rows_of(j):
                rows = mul_of(j, step)
                g, u = gu[rows, g_at], gu[rows, u_at]
                gh = k2[j // 2, mul_of(j % 2, step), at] if half else acc[rows, at]
                sig = jax.nn.sigmoid(g)
                gg2[rows, g_at] = (gh * u * sig * (1.0 + g * (1.0 - sig))).astype(bf16)
                gg2[rows, u_at] = (gh * (g * sig)).astype(bf16)

            loop(T // step, rows_of)

        loop(CW // NT, tile)

    hidden_back(0)
    hidden_back(1)
    takes(ND, 0, 2, CHUNKS - 1)

    def res_chunk(i):
        acc[...] = dot_nt(gg2[...], wgu[mul_of(i, CW), :])

    def res_extra(i):
        give(NG2, i)

        @pl.when(i > 0)
        def _():
            take(NG2, i - 1)

    def res_between(i):
        if i == 0:
            take(NG2, 3)
            give_down(1, 0)
            give_down(1, 1)
        elif i == 1:
            give_down(1, 2)
            give_down(1, 3)
        else:
            for c in range(CHUNKS):
                takes(ND, 2, 4, c)
            x_add(ND, 0, 4)
            gives(NG2, 4, 8)

    rs(2, cbuf, res_chunk, res_between, res_extra)

    def attn_grad_rows(j):
        rows = mul_of(j, BL)
        gr = cbuf[rows, :] + cot[rows, :].astype(f32)
        cbuf[rows, :] = gr
        a = abuf[rows, :]
        scale = lax.rsqrt(jnp.mean(a * a, axis=-1, keepdims=True) + eps_norm)
        weighted = gr * gat[...]
        inner = jnp.mean(weighted * a, axis=-1, keepdims=True)
        ga = scale * weighted - a * scale**3 * inner
        gaall[part(t * L + j * BL, BL), :] = ga.astype(bf16)
        gsum[:, 0:D] += jnp.sum(gr * a * scale, axis=0, keepdims=True)

    loop(L // BL, attn_grad_rows)

    def attend_back(b):
        rows = blk(b)
        acc[rows, 0:ha] = dot_nt(gaall[rows, :], wo[...])
        scale = columns(2, b)
        cos, sin = cos_v[...], sin_v[...]
        for h in range(heads):
            head = pl.ds(h * HD, HD)
            gm = acc[rows, head].astype(bf16)
            p = probs[b * heads + h]
            gqkv[rows, pl.ds(2 * ha + h * HD, HD)] = dot_tn(p.astype(bf16), gm).astype(bf16)
            gp = dot_nt(gm, vb[rows, head])
            gs = p * (gp - jnp.sum(p * gp, axis=-1, keepdims=True))
            gs = (gs * inv).astype(bf16)
            turned = (dot_nn(gs, qkrot[rows, pl.ds(ha + h * HD, HD)]), dot_tn(gs, qkrot[rows, head]))
            for which in range(2):
                at = pl.ds(which * ha + h * HD, HD)
                gn = turned[which] * cos - pltpu.roll(turned[which], HD // 2, 1) * sin
                field = qk[rows, at]
                spot = part(2 * D + which * d.att + t * ha + h * HD, HD)
                gsum[:, spot] += jnp.sum(gn * field * scale[which], axis=0, keepdims=True)
                gu[rows, at] = gn * gain_of(which, h)

    for i in range(CHUNKS):
        ag_start(gaall, 3, i)
    attend_back(t)
    ag_fwd(gaall, 3, 0)
    takes(NG2, 4, 6)
    ag_fwd(gaall, 3, 1)
    takes(NG2, 6, 8)
    ag_fwd(gaall, 3, 2)
    ag_fwd(gaall, 3, 3)
    x_add(ND, 4, 8)
    relay(ND, 0, 2)
    x_add(NG2, 0, 1)
    loop(2, lambda j: attend_back(t_y + j * (t_z - t_y)))
    for i in range(CHUNKS):
        ag_done(gaall, 3, i)
    attend_back(t_d)
    gain_step(0)
    gives(NO, 0, 2)
    relay(ND, 2, 4)
    ag_drain(gaall, 3)

    def products(rows):
        return gu[rows, 0:2 * ha] * qk[rows, :]

    def in_stat():
        takes(NO, 0, 2)

    stat[3] = stat_sum(1, products, in_stat) / d.att
    gain_step(1)
    x_add(NG2, 1, 3)

    def qk_back(b):
        rows = blk(b)
        scale, inner = columns(2, b), columns(3, b)
        for which in range(2):
            at = pl.ds(which * ha, ha)
            sc = scale[which]
            gqkv[rows, at] = (sc * gu[rows, at] - qk[rows, at] * (sc**3 * inner[which])).astype(bf16)

    loop(TP, qk_back)
    gain_step(2)

    def in_chunk(i):
        acc[...] = dot_nt(gqkv[...], wqkv[mul_of(i, CW), :])

    def in_extra(i):
        give(NQ, i)

        @pl.when(i == 2)
        def _():
            x_add(NG2, 3, 4)

        @pl.when(i > 0)
        def _():
            take(NQ, i - 1)

    def in_between(i):
        if i == 0:
            take(NQ, 3)
            relay(NG2, 0, 2)
            gives(NQ, 4, 8)
            gain_step(3)
        elif i == 1:
            takes(NQ, 4, 8)
            relay(NG2, 2, 3)
        else:
            x_add(NQ, 0, 2)
            gain_step(4)
            relay(NG2, 3, 4)
            x_add(NG2, 4, 8)
            hi_finish(ND, abuf)
            pltpu.make_async_copy(abuf.at[0:unit], down_h, loc.at[4]).start()

    rs(3, bbuf, in_chunk, in_between, in_extra)

    def input_rows(j):
        rows = mul_of(j, BL)
        bbuf[rows, :] += cbuf[rows, :]

    loop(L // BL, input_rows)
    put_gin = pltpu.make_async_copy(bbuf, gin_h, loc.at[5])
    put_gin.start()

    x_add(NQ, 2, 4)
    relay(NQ, 0, 2)
    x_add(NO, 0, 1)
    hi_finish(NG2, None, keep_piece)
    if d.levels > 1:
        keep_start(NG2)

    for p in range(d.pieces):
        o_pc[p] = rc_o[part(s * HD + p * d.own_o, d.own_o), :]
    o_slot = hi * CORES + core

    def o_start(p):
        goal = t * d.pieces + p

        @pl.when(goal != r)
        def _():
            send(o_pc.at[p], o_h.at[o_slot], o_s.at[p], o_r.at[o_slot], (s, goal)).start()

        @pl.when(goal == r)
        def _():
            pltpu.make_async_copy(o_pc.at[p], o_h.at[o_slot], o_r.at[o_slot]).start()

    loop(d.pieces, o_start)
    hi_finish(NQ)
    keep_start(NQ)
    for n in range(5, len(partners) + 1):
        gain_step(n)
    gg_o[...] = gsum[...]

    keep_wait(NG2)
    keep_wait(NQ)
    keep_end(NG2)
    keep_end(NQ)

    def o_wait(q):
        pltpu.make_async_copy(o_pc.at[0], o_pc.at[0], o_r.at[q]).wait()

    loop(his * CORES, o_wait)

    def o_sent(p):
        goal = t * d.pieces + p

        @pl.when(goal != r)
        def _():
            send(o_pc.at[p], o_h.at[o_slot], o_s.at[p], o_r.at[o_slot], (s, goal)).wait_send()

    loop(d.pieces, o_sent)
    far_gain.wait_send()
    for k in range(NG):
        cross(k).wait_send()
        share(k).wait_send()
    for i in range(CHUNKS - 2, CHUNKS):
        loop(2 * tiles_of(ND), lambda j: core_copy(ND, j, i, 4 * (i % 2) + j).wait_send())
    for slot in range(2):
        core_copy(NQ, slot, 0, slot).wait_send()
    for k in range(4):
        loop(moves_of(k) * sets[k][7], lambda q: x_copy(k, q).wait_send())
    for k in range(3):
        @pl.when(edge)
        def _():
            loop(moves_of(k) // 2 * sets[k][7], lambda q: relay_in(k, q).wait_send())

        @pl.when(jnp.logical_not(edge))
        def _():
            loop(moves_of(k) // 2 * sets[k][7], lambda q: (hi_first(k, q).wait_send(), relay_out(k, q).wait_send()))

        for step in hi_later(k)[0]:
            hi_copy(k, step).wait_send()
    put_out.wait()
    put_gin.wait()
    pltpu.make_async_copy(abuf.at[0:unit], down_h, loc.at[4]).wait()


def body(shards, replicas, x_in, cotangent, w_query, w_key, w_value, w_out, w_gate, w_up, w_down,
         gain_query, gain_key, gain_attn, gain_mlp):
    seqs, length, width = x_in.shape
    assert seqs == 1
    d = Dims(length, width, w_query.shape[1], w_gate.shape[1], shards, replicas)
    r = lax.axis_index("replica")
    s = lax.axis_index("shard")
    t = (r // CORES) % TP

    def at(array, axis, index):
        return lax.dynamic_index_in_dim(array, index, axis, keepdims=False)

    def hidden_cols(w):
        picked = at(w.reshape(w.shape[0], d.S, d.his, TP, CORES, d.unit), 3, t)
        return picked.transpose(0, 3, 1, 2, 4).reshape(w.shape[0], d.fh)

    if not d.direct:
        w_gate = jnp.concatenate([hidden_cols(w_gate), hidden_cols(w_up)], axis=1)
        w_down = at(w_down.reshape(d.his, TP, CORES, d.unit, width), 1, t).transpose(1, 0, 2, 3).reshape(-1, width)
    gain = jnp.concatenate([at(gain_query.reshape(TP, HD), 0, t), at(gain_key.reshape(TP, HD), 0, t),
                            gain_attn, gain_mlp]).astype(f32)[None]
    cos, sin = rope_tables(length, HD // 2)
    cos = np.concatenate([cos, cos], axis=1)
    sin = np.concatenate([-sin, sin], axis=1)

    L, D, T, ha, fh = d.L, d.D, d.T, d.ha, d.fh
    CW = D // CHUNKS
    vm = pltpu.VMEM
    dma = pltpu.SemaphoreType.DMA
    any_ = pl.BlockSpec(memory_space=pl.ANY)
    vmem = pl.BlockSpec(memory_space=pltpu.VMEM)
    hi_rows = lambda n: max(n - n // d.his, 16)
    steps = 4 + d.levels
    later = max(d.levels - 1, 1)
    scratch = [
        vm((D, 3 * ha), bf16), vm((ha, D), bf16), vm((D, 2 * fh), bf16), vm((fh, D), bf16),
        vm((2, 1, d.gains), f32), vm((1, D), f32), vm((1, D), f32),
        vm((T, D), bf16), vm((T, D), bf16), vm((T, D), bf16), vm((T, D), bf16), vm((L, D), bf16),
        vm((T, 2 * ha), f32), vm((T, ha), bf16), vm((T, 2 * ha), bf16), vm((TP * ha // HD, L, L), f32),
        vm((T, ha), bf16), vm((T, 3 * ha), bf16), vm((4, 8, T), f32), vm((2, 3, 8, T), f32),
        vm((T, 2 * fh), f32), vm((T, fh), bf16), vm((T, 2 * fh), bf16),
        vm((L, D), f32), vm((L, D), f32), vm((L, D), f32), vm((L, D), bf16),
        vm((T, CW), f32), vm((CHUNKS, 2, L, CW), bf16), vm((CHUNKS, L, CW), bf16),
        vm((CHUNKS, 2, L, CW), bf16), vm((CHUNKS, L, CW), bf16), vm((CHUNKS, L, CW), f32),
        vm((8, 128, CW), bf16), vm((2, 256, fh), bf16),
        vm((D, fh), bf16), vm((fh // 2, D), bf16), vm((D, 3 * ha // 2), bf16), vm((ha, D // 2), bf16),
        vm((D // 2, fh), bf16), vm((fh // 4, D), bf16), vm((D // 2, 3 * ha // 2), bf16), vm((ha // 2, D // 2), bf16),
        vm((hi_rows(D // 2), fh), bf16), vm((hi_rows(fh // 4), D), bf16), vm((hi_rows(D // 2), 3 * ha // 2), bf16),
        vm((d.pieces, d.own_o, D // 2), bf16),
        vm((1, d.ggs), f32), vm((steps, 1, d.ggs), f32),
        dma((4, CHUNKS, 4)), dma((4, CHUNKS, 4)), dma((4, CHUNKS, 4)), dma((4, CHUNKS, 4)),
        dma((11,)), dma((11,)), dma((10,)), dma((10,)), dma((10, 2)), dma((6,)), dma((2, 3)), dma((2, 3)),
        dma((2, 8)), dma((4, 16)), dma((4, 8)), dma((4, 8)), dma((3, 4)), dma((3, 4)), dma((3, 4)), dma((3, 4)), dma((3, 4)),
        dma((3, later)), dma((3, later)),
        dma((2, TP * CORES)), dma((2, TP * CORES)), dma((2, TP * CORES)), dma((d.pieces,)), dma((d.his * CORES,)), dma((steps,)), dma((steps,)),
    ]
    struct = jax.ShapeDtypeStruct
    gu_shape = (2, d.own, d.ff) if d.direct else (TP * CORES, d.own, fh)
    results = pl.pallas_call(
        functools.partial(kernel, d),
        out_shape=(
            struct((L, D), bf16), struct((L, D), f32), struct(gu_shape, bf16), struct((3, d.own, d.att), bf16),
            struct((d.unit, D), f32), struct((d.his * CORES, d.own_o, D // 2), bf16),
            struct((fh // 8, D), bf16), struct((D // 4, fh), bf16), struct((D // 4, 3 * ha // 2), bf16),
            struct((1, d.ggs), f32),
        ),
        in_specs=[any_] * 9 + [vmem] * 3,
        out_specs=(any_,) * 9 + (vmem,),
        scratch_shapes=scratch,
        compiler_params=pltpu.CompilerParams(
            collective_id=0, has_side_effects=True, vmem_limit_bytes=67043328),
        name="layer",
    )(x_in[0], cotangent[0], w_query, w_key, w_value, w_out, w_gate, w_up, w_down, gain, cos, sin)
    out, gin, gu, qkv, down, o = results[:6]
    gg = results[-1]

    def hidden_out(k):
        if d.direct:
            return gu[k].astype(f32)
        block = gu.reshape(TP, CORES, d.own, fh)[:, k]
        spread = block.reshape(TP, d.own, CORES, d.S, d.his, d.unit).transpose(1, 3, 4, 0, 2, 5)
        return spread.reshape(d.own, d.ff).astype(f32)

    o = o.reshape(d.his, CORES, d.own_o, D // 2).astype(f32).sum(0).transpose(1, 0, 2).reshape(d.own_o, D)
    gg = gg[0]
    here = s * d.R + r

    def share(vec):
        n = vec.shape[0] // (d.S * d.R)
        return lax.dynamic_slice_in_dim(vec, here * n, n)

    def head_gain(vec):
        return share(vec.reshape(TP, d.S, HD).transpose(1, 0, 2).reshape(-1))

    return (
        out[None], gin[None], qkv[0].astype(f32), qkv[1].astype(f32), qkv[2].astype(f32), o,
        hidden_out(0), hidden_out(1), down,
        head_gain(gg[2 * D:2 * D + d.att]), head_gain(gg[2 * D + d.att:]), share(gg[:D]), share(gg[D:2 * D]),
    )


def solution(mesh):
    both = ("shard", "replica")
    token = P(both, None, None)
    weight = P("shard", None)
    return jax.shard_map(
        functools.partial(body, mesh.shape["shard"], mesh.shape["replica"]),
        mesh=mesh,
        in_specs=(token, token) + (weight,) * 7 + (P("shard"),) * 4,
        out_specs=(token, token) + (P(both, None),) * 7 + (P(both),) * 4,
        check_vma=False,
    )
```

```python
import functools
import math

import jax
import jax.numpy as jnp
import numpy as np
from jax import lax
from jax.experimental import pallas as pl
from jax.experimental.pallas import tpu as pltpu
from jax.sharding import PartitionSpec as P

HD = 128
TP = 4
CORES = 2
CHUNKS = 4
Z_AG = (256, 256, 256, 0)
Z_RS = (256, 256, 256, 128)

eps_norm = 1e-06
rope_theta = 500000.0

bf16 = jnp.bfloat16
f32 = jnp.float32


def rope_tables(length, half):
    position = np.arange(length).astype(np.float32)[:, None]
    exponent = np.arange(half).astype(np.float32) * np.float32(1.0 / half)
    angle = position * np.float32(rope_theta) ** (-exponent)
    return (np.cos(angle).astype(np.float32), np.sin(angle).astype(np.float32))


def dot_nn(left, right):
    return lax.dot_general(left, right, (((1,), (0,)), ((), ())), preferred_element_type=f32)


def dot_nt(left, right, precision=None):
    return lax.dot_general(
        left, right, (((1,), (1,)), ((), ())), preferred_element_type=f32, precision=precision)


def dot_tn(left, right):
    return lax.dot_general(left, right, (((0,), (0,)), ((), ())), preferred_element_type=f32)


def mul_of(index, step):
    return pl.ds(pl.multiple_of(index * step, step), step)


def loop(count, step, start=0):
    lax.fori_loop(start, count, lambda i, c: (step(i), c)[1], 0)


class Dims:
    def __init__(self, length, width, att, ff, shards, replicas):
        self.L, self.D, self.att, self.ff = length, width, att, ff
        self.S, self.R = shards, replicas
        self.his = replicas // (TP * CORES)
        self.T = TP * length
        self.ha = att // TP
        self.fh = ff // TP
        self.unit = ff // (shards * replicas)
        self.own = width // (shards * replicas)
        self.own_o = att // (shards * replicas)
        self.pieces = HD // self.own_o
        self.levels = self.his.bit_length() - 1
        self.gains = 2 * HD + width
        self.ggs = 2 * width + 2 * att
        self.direct = self.unit % 128 == 0
        assert shards == 2 and self.his == 1 << self.levels and self.levels > 0 and self.ha == shards * HD
        assert self.fh == 2 * (width // CHUNKS)


def kernel(
    d,
    x_h, cot_h, wq_h, wk_h, wv_h, wo_h, wg_h, wu_h, wd_h, gain_v, cos_v, sin_v,
    out_h, gin_h, gu_h, qkv_h, down_h, o_h, relay_d, relay_gu, relay_q, gg_o,
    wqkv, wo, wgu, wd, gbuf, gat, gml,
    xall, rall, gdall, gaall, cot,
    qk, vb, qkrot, probs, mixed, gqkv, stat, statr,
    gu, hid, gg2,
    abuf, bbuf, cbuf, outb,
    acc, s1, s2, r1, r2, k2,
    stage_d, stage, rc_gu, rc_d, rc_q, rc_o, rx_gu, rx_d, rx_q, rx_o, rh_gu, rh_d, rh_q, o_pc,
    gsum, grecv,
    ag_s, ag_r, rs_s, rs_r, w_s, w_r, wf_s, wf_r, w_l, loc, st_s, st_r,
    stg_s, c_r, x_s, x_r, h0_s, h0_r, rl_s, rl_r, rf_s, h_s, h_r, a_s, a_r, ko, o_s, o_r, gn_s, gn_r,
):
    L, D, T, ha, fh, his, unit = d.L, d.D, d.T, d.ha, d.fh, d.his, d.unit
    CW = D // CHUNKS
    HW = CW // 2
    s = lax.axis_index("shard")
    r = lax.axis_index("replica")
    hi, t, core = r // (TP * CORES), (r // CORES) % TP, r % CORES
    tz, ty = t // 2, t % 2
    t_y, t_z, t_d = tz * 2 + 1 - ty, (1 - tz) * 2 + ty, (1 - tz) * 2 + 1 - ty

    def rep(hi_, t_, core_):
        return hi_ * (TP * CORES) + t_ * CORES + core_

    dev_y, dev_z, dev_d = ((s, rep(hi, q, core)) for q in (t_y, t_z, t_d))
    dev_x = (1 - s, r)
    dev_c = (s, rep(hi, t, 1 - core))

    def send(src, dst, ssem, rsem, dev):
        return pltpu.make_async_remote_copy(
            src_ref=src, dst_ref=dst, send_sem=ssem, recv_sem=rsem, device_id=dev,
            device_id_type=pl.DeviceIdType.MESH)

    def blk(q):
        return mul_of(q, L)

    def part(base, n):
        return pl.ds(pl.multiple_of(base, n), n)

    def ag_copies(buf, inst, i, src=None):
        own = buf.at[blk(t), mul_of(i, CW)]
        first = own if src is None else src.at[:, mul_of(i, CW)]
        wz = Z_AG[inst]
        fy = buf.at[blk(t_y), pl.ds(pl.multiple_of(i * CW + CW - wz, 128), wz)] if wz else None
        fz = buf.at[blk(t_z), pl.ds(pl.multiple_of(i * CW, 128), CW - wz)]
        ends = ((first, own, dev_y), (first, own, dev_z), (fy, fy, dev_z), (fz, fz, dev_y))

        def copy(j):
            return send(ends[j][0], ends[j][1], ag_s.at[inst, i, j], ag_r.at[inst, i, j], ends[j][2])

        return copy

    def ag_start(buf, inst, i, src=None):
        c = ag_copies(buf, inst, i, src)
        c(0).start()
        c(1).start()

    def ag_fwd(buf, inst, i):
        c = ag_copies(buf, inst, i)
        c(1).wait_recv()
        c(3).start()
        c(0).wait_recv()
        if Z_AG[inst]:
            c(2).start()

    def ag_done(buf, inst, i):
        c = ag_copies(buf, inst, i)
        if Z_AG[inst]:
            c(2).wait_recv()
        c(3).wait_recv()

    def ag_drain(buf, inst):
        def wait(i):
            c = ag_copies(buf, inst, i)
            for j in range(4):
                if j != 2 or Z_AG[inst]:
                    c(j).wait_send()

        loop(CHUNKS, wait)

    def ag(buf, inst, src=None, between=lambda i: None):
        ag_start(buf, inst, 0, src)
        ag_start(buf, inst, 1, src)
        for i in range(CHUNKS):
            ag_fwd(buf, inst, i)
            if i + 2 < CHUNKS:
                ag_start(buf, inst, i + 2, src)
            between(i)
        for i in range(CHUNKS):
            ag_done(buf, inst, i)
        ag_drain(buf, inst)

    def rs_copies(inst, i):
        wa = CW - Z_RS[inst]
        ya, zb = pl.ds(0, wa), pl.ds(wa, CW - wa)

        def copy(j):
            if j == 0:
                a, b, dev = s1.at[i, :, :, ya], r1.at[i, :, :, ya], dev_y
            elif j == 1:
                a, b, dev = s1.at[i, :, :, zb], r1.at[i, :, :, zb], dev_z
            elif j == 2:
                a, b, dev = s2.at[i, :, ya], r2.at[i, :, ya], dev_z
            else:
                a, b, dev = s2.at[i, :, zb], r2.at[i, :, zb], dev_y
            return send(a, b, rs_s.at[inst, i, j], rs_r.at[inst, i, j], dev)

        return copy

    def rs_send(inst, i, dest):
        c = rs_copies(inst, i)
        wa = CW - Z_RS[inst]
        step = L // 4

        def rows_of(j):
            def rows(q):
                return part(q * L + j * step, step)

            here = mul_of(j, step)
            s1[i, 0, here, 0:wa] = acc[rows(t_y), 0:wa].astype(bf16)
            k2[i, here, 0:wa] = acc[rows(t_z), 0:wa]
            if wa < CW:
                s1[i, 0, here, wa:CW] = acc[rows(t_z), wa:CW].astype(bf16)
                k2[i, here, wa:CW] = acc[rows(t_y), wa:CW]
            s1[i, 1, here] = acc[rows(t_d), :].astype(bf16)
            dest[here, mul_of(i, CW)] = acc[rows(t), :]

        loop(4, rows_of)
        c(0).start()
        if wa < CW:
            c(1).start()

    def rs_fwd(inst, i, dest):
        c = rs_copies(inst, i)
        wa = CW - Z_RS[inst]
        c(0).wait_recv()
        s2[i, :, 0:wa] = (k2[i, :, 0:wa] + r1[i, 1, :, 0:wa].astype(f32)).astype(bf16)
        c(2).start()
        if wa < CW:
            c(1).wait_recv()
            s2[i, :, wa:CW] = (k2[i, :, wa:CW] + r1[i, 1, :, wa:CW].astype(f32)).astype(bf16)
            c(3).start()
        dest[:, mul_of(i, CW)] += r1[i, 0].astype(f32)

    def rs_done(inst, i, dest):
        c = rs_copies(inst, i)
        c(2).wait_recv()
        if Z_RS[inst]:
            c(3).wait_recv()
        dest[:, mul_of(i, CW)] += r2[i].astype(f32)

    def rs(inst, dest, compute, between=lambda i: None, extra=lambda i: None):
        def first(i):
            compute(i)
            rs_send(inst, i, dest)
            extra(i)

            @pl.when(i >= 2)
            def _():
                rs_fwd(inst, i - 2, dest)

        loop(CHUNKS, first)
        between(0)
        rs_fwd(inst, CHUNKS - 2, dest)
        between(1)
        rs_fwd(inst, CHUNKS - 1, dest)
        between(2)
        loop(CHUNKS, lambda i: rs_done(inst, i, dest))

        def wait(i):
            c = rs_copies(inst, i)
            for j in range(4):
                if j % 2 == 0 or Z_RS[inst]:
                    c(j).wait_send()

        loop(CHUNKS, wait)

    def qkv_region(s_, piece):
        return wqkv.at[part(s_ * (D // 2) + piece * (D // 4), D // 4)]

    def qkv_parts(s_, piece):
        rows, to = part(piece * (D // 4), D // 4), part(s_ * (D // 2) + piece * (D // 4), D // 4)
        for which, src in enumerate((wq_h, wk_h, wv_h)):
            for h in range(d.S):
                yield src.at[rows, part((h * TP + t) * HD, HD)], wqkv.at[to, pl.ds(which * ha + h * HD, HD)]

    def o_region(s_, piece):
        return wo.at[part(s_ * HD + piece * (HD // 2), HD // 2)]

    def o_parts(s_, piece):
        yield wo_h.at[part(t * HD + piece * (HD // 2), HD // 2)], o_region(s_, piece)

    SUBS = 4

    def gu_group(sub):
        n = D // 4 // SUBS

        def region(s_, piece):
            return wgu.at[part(s_ * (D // 2) + piece * (D // 4) + sub * n, n)]

        def parts(s_, piece):
            rows = part(piece * (D // 4) + sub * n, n)
            to = part(s_ * (D // 2) + piece * (D // 4) + sub * n, n)
            w = 2 * unit
            if not d.direct:
                yield wg_h.at[rows], wgu.at[to]
                return
            for m, src in enumerate((wg_h, wu_h)):
                for c in range(d.S * his):
                    yield src.at[rows, part((c * TP + t) * w, w)], wgu.at[to, pl.ds(m * fh + c * w, w)]

        return parts, region

    def d_group(sub):
        at = mul_of(sub, CW)
        n = fh // 4

        def region(s_, piece):
            return wd.at[part(((s_ * 2 + piece) if d.direct else (piece * 2 + s_)) * n, n), at]

        def parts(s_, piece):
            w = 2 * unit
            if not d.direct:
                yield wd_h.at[part(piece * n, n), at], region(s_, piece)
                return
            step = min(w, n)
            for e in range(n // step):
                first = piece * n + e * step
                src = (first // w) * (TP * w) + t * w + first % w
                yield wd_h.at[part(src, step), at], wd.at[part(s_ * (fh // 2) + first, step), at]

        return parts, region

    GU0, DN0 = 2, 2 + SUBS
    NG = DN0 + CHUNKS

    def group_of(k):
        if isinstance(k, int) and k < DN0:
            return ((qkv_parts, qkv_region), (o_parts, o_region))[k] if k < GU0 else gu_group(k - GU0)
        return d_group(k - DN0)

    def local_start(k):
        for piece in range(2):
            for src, dst in group_of(k)[0](s, piece):
                pltpu.make_async_copy(src, dst, w_l.at[k, piece]).start()

    def local_wait(k):
        for piece in range(2):
            here = group_of(k)[1](s, piece)
            pltpu.make_async_copy(here, here, w_l.at[k, piece]).wait()

    def cross_start(k):
        for src, dst in group_of(k)[0](s, core):
            send(src, dst, w_s.at[k], w_r.at[k], dev_x).start()

    def cross(k):
        here = group_of(k)[1](s, core)
        return send(here, here, w_s.at[k], w_r.at[k], dev_x)

    def share(k):
        here = group_of(k)[1](1 - s, core)
        return send(here, here, wf_s.at[k], wf_r.at[k], dev_c)

    def w_forward(k):
        cross(k).wait_recv()
        share(k).start()

    def w_ready(k):
        local_wait(k)
        share(k).wait_recv()

    own_x = pltpu.make_async_copy(x_h, xall.at[blk(t)], loc.at[0])
    own_cot = pltpu.make_async_copy(cot_h, cot, loc.at[1])
    own_gain = pltpu.make_async_copy(gain_v, gbuf.at[s], loc.at[2])
    far_gain = send(gain_v, gbuf.at[s], w_s.at[NG], w_r.at[NG], dev_x)
    own_x.start()
    local_start(0)
    own_gain.start()
    own_cot.start()

    barrier = pltpu.get_barrier_semaphore()

    def greet(q):
        @pl.when(q != r)
        def _():
            pl.semaphore_signal(barrier, inc=1, device_id=(s, q), device_id_type=pl.DeviceIdType.MESH)

    loop(d.R, greet)
    pl.semaphore_signal(barrier, inc=1, device_id=dev_x, device_id_type=pl.DeviceIdType.MESH)
    pl.semaphore_wait(barrier, d.R)

    ag_start(xall, 0, 0, x_h)
    cross_start(0)
    ag_start(xall, 0, 1, x_h)
    far_gain.start()
    for k in range(1, NG):
        cross_start(k)
    for k in range(1, NG):
        local_start(k)

    for i in range(CHUNKS):
        ag_fwd(xall, 0, i)
        if i + 2 < CHUNKS:
            ag_start(xall, 0, i + 2, x_h)
    w_forward(0)
    own_x.wait()
    own_gain.wait()
    far_gain.wait_recv()
    for q in range(2):
        gat[:, q * (D // 2):(q + 1) * (D // 2)] = gbuf[q, :, 2 * HD:2 * HD + D // 2]
        gml[:, q * (D // 2):(q + 1) * (D // 2)] = gbuf[q, :, 2 * HD + D // 2:]
    gsum[...] = jnp.zeros_like(gsum)
    for i in range(CHUNKS):
        ag_done(xall, 0, i)
    ag_drain(xall, 0)
    w_ready(0)

    qk[:, 0:ha] = dot_nn(xall[...], wqkv[:, 0:ha])
    qk[:, ha:2 * ha] = dot_nn(xall[...], wqkv[:, ha:2 * ha])
    vb[...] = dot_nn(xall[...], wqkv[:, 2 * ha:]).astype(bf16)

    row8 = lax.broadcasted_iota(jnp.int32, (8, 2 * ha), 0)
    col8 = lax.broadcasted_iota(jnp.int32, (8, 2 * ha), 1)
    pick = jnp.where((row8 < 4) == (col8 < ha), 1.0, 0.0).astype(f32)
    HIGH = lax.Precision.HIGHEST

    def stat_sum(k, values, between=lambda: None):
        def sequence(b):
            stat[k, :, blk(b)] = dot_nt(pick, values(blk(b)), HIGH)

        loop(TP, sequence)
        copies = [send(stat.at[k], statr.at[k, j], st_s.at[k, j], st_r.at[k, j], dev)
                  for j, dev in enumerate((dev_y, dev_z, dev_d))]
        for c in copies:
            c.start()
        between()
        for c in copies:
            c.wait_recv()
        for c in copies:
            c.wait_send()
        return stat[k] + statr[k, 0] + statr[k, 1] + statr[k, 2]

    def squares(rows):
        v = qk[rows, :]
        return v * v

    stat[2] = lax.rsqrt(stat_sum(0, squares) / d.att + eps_norm)

    def columns(k, b):
        flat = stat[k, :, blk(b)]
        wide = jnp.concatenate([flat] * (L // 8), axis=0).T
        return wide[:, 0:1], wide[:, 4:5]

    def gain_of(which, h):
        return gbuf[h, :, which * HD:(which + 1) * HD]

    inv = 1.0 / math.sqrt(HD)
    heads = ha // HD

    def attend(b):
        rows = blk(b)
        scale = columns(2, b)
        cos, sin = cos_v[...], sin_v[...]
        above = lax.broadcasted_iota(jnp.int32, (L, L), 0) < lax.broadcasted_iota(jnp.int32, (L, L), 1)
        for h in range(heads):
            rot = []
            for which in range(2):
                at = pl.ds(which * ha + h * HD, HD)
                normed = qk[rows, at] * scale[which] * gain_of(which, h)
                turned = (normed * cos + pltpu.roll(normed, HD // 2, 1) * sin).astype(bf16)
                qkrot[rows, at] = turned
                rot.append(turned)
            scores = jnp.where(above, -jnp.inf, dot_nt(rot[0], rot[1]) * inv)
            peak = jnp.max(scores, axis=-1, keepdims=True)
            log_total = peak + jnp.log(jnp.sum(jnp.exp(scores - peak), axis=-1, keepdims=True))
            p = jnp.exp(scores - log_total)
            probs[b * heads + h] = p
            head = pl.ds(h * HD, HD)
            mixed[rows, head] = dot_nn(p.astype(bf16), vb[rows, head]).astype(bf16)

    loop(TP, attend)
    w_forward(1)
    w_ready(1)

    def attn_chunk(i):
        acc[...] = dot_nn(mixed[...], wo[:, mul_of(i, CW)])

    def attn_between(i):
        if i == 2:
            w_forward(GU0)

    rs(0, abuf, attn_chunk, attn_between)

    BL = 16

    def residual_rows(j):
        rows = mul_of(j, BL)
        a = abuf[rows, :]
        scale = lax.rsqrt(jnp.mean(a * a, axis=-1, keepdims=True) + eps_norm)
        mine = part(t * L + j * BL, BL)
        res = xall[mine, :].astype(f32) + a * scale * gat[...]
        cbuf[rows, :] = res
        rall[mine, :] = res.astype(bf16)

    loop(L // BL, residual_rows)
    NT = 256

    def turn(i):
        return ((i // 2 + s) % 2) * 2 + i % 2

    def gate_up(i):
        chunk = mul_of(turn(i), CW)

        def tile(n):
            at = mul_of(n, NT)
            value = dot_nn(rall[:, chunk], wgu[chunk, at])
            gu[:, at] = value if i == 0 else gu[:, at] + value

        loop(2 * fh // NT, tile)

    ag_start(rall, 1, turn(0))
    ag_start(rall, 1, turn(1))
    ag_start(rall, 1, turn(2))
    w_forward(GU0 + 1)
    ag_fwd(rall, 1, turn(0))
    ag_start(rall, 1, turn(3))
    ag_fwd(rall, 1, turn(1))
    for k in range(GU0, DN0):
        local_wait(k)
    ag_done(rall, 1, turn(0))
    w_forward(GU0 + 2)
    gate_up(0)
    ag_fwd(rall, 1, turn(2))
    ag_done(rall, 1, turn(1))
    ag_fwd(rall, 1, turn(3))
    gate_up(1)
    ag_done(rall, 1, turn(2))
    w_forward(GU0 + 3)
    for k in range(GU0, DN0):
        share(k).wait_recv()
    gate_up(2)
    ag_done(rall, 1, turn(3))
    gate_up(3)
    ag_drain(rall, 1)

    def hidden(n):
        g_at, u_at = mul_of(n, NT), part(fh + n * NT, NT)

        def rows_of(j):
            rows = mul_of(j, 64)
            g, u = gu[rows, g_at], gu[rows, u_at]
            hid[rows, g_at] = (g * jax.nn.sigmoid(g) * u).astype(bf16)

        loop(T // 64, rows_of)

    loop(fh // NT, hidden)
    def down_chunk(i):
        w_forward(DN0 + i)
        w_ready(DN0 + i)
        acc[...] = dot_nn(hid[...], wd[:, mul_of(i, CW)])

    rs(1, bbuf, down_chunk)
    own_cot.wait()

    def output_rows(j):
        rows = mul_of(j, BL)
        dn = bbuf[rows, :]
        scale = lax.rsqrt(jnp.mean(dn * dn, axis=-1, keepdims=True) + eps_norm)
        outb[rows, :] = (cbuf[rows, :] + dn * scale * gml[...]).astype(bf16)
        co = cot[rows, :].astype(f32)
        weighted = co * gml[...]
        inner = jnp.mean(weighted * dn, axis=-1, keepdims=True)
        gd = scale * weighted - dn * scale**3 * inner
        gdall[part(t * L + j * BL, BL), :] = gd.astype(bf16)
        gsum[:, D:2 * D] += jnp.sum(co * dn * scale, axis=0, keepdims=True)

    loop(L // BL, output_rows)
    put_out = pltpu.make_async_copy(outb, out_h, loc.at[3])
    put_out.start()
    half_q = 3 * ha // 2

    def by_cols(left, right, width):
        def make(row, n, core_, i):
            return dot_tn(left[:, part(row, n)], right[:, mul_of(core_, width)])
        return make

    def down_grad(row, n, core_, i):
        start = (row // unit) * 2 * unit + core_ * unit if d.direct else core_ * (fh // 2) + row
        return dot_tn(hid[:, part(start, n)], gdall[:, mul_of(i, CW)])

    ND, NG2, NQ, NO = range(4)
    sets = (
        (down_grad, rc_d, rx_d, rh_d, fh // 2, 128, 128, CHUNKS, stage_d),
        (by_cols(rall, gg2, fh), rc_gu, rx_gu, rh_gu, D, 256, 128, 1, stage),
        (by_cols(xall, gqkv, half_q), rc_q, rx_q, rh_q, D, 256, 256, 1, stage),
        (by_cols(mixed, gaall, D // 2), rc_o, rx_o, None, ha, 128, 128, 1, stage),
    )
    top = hi // (his // 2)

    def half_of(k):
        return sets[k][4] // 2

    def tiles_of(k):
        return half_of(k) // sets[k][5]

    def moves_of(k):
        return half_of(k) // sets[k][6]

    def place(k, j, n):
        count = half_of(k) // n
        if count < 2:
            return j * n
        return ((j + (1 - top) * (count // 2)) % count) * n

    def whole_row(k, j):
        tiles = tiles_of(k)
        late = j // tiles
        return (late * s + (1 - late) * (1 - s)) * half_of(k) + place(k, j % tiles, sets[k][5])

    def cols(k, i):
        return mul_of(i, CW) if sets[k][7] > 1 else pl.ds(0, sets[k][1].shape[1])

    def core_copy(k, j, i, slot):
        buf, n, st = sets[k][1], sets[k][5], sets[k][8]
        row = whole_row(k, j)
        w = CW if sets[k][7] > 1 else buf.shape[1]
        return send(st.at[slot, 0:n, 0:w], buf.at[part(row, n), cols(k, i)], stg_s.at[0 if k == ND else 1, slot],
                    c_r.at[k, (row // n) * sets[k][7] + i], dev_c)

    def give_down(late, i):
        def tile(j):
            slot = 4 * (i % 2) + j
            if i >= 2:
                core_copy(ND, j, i - 2, slot).wait_send()
            stage_d[slot] = down_grad(whole_row(ND, j), 128, 1 - core, i).astype(bf16)
            core_copy(ND, j, i, slot).start()

        n = tiles_of(ND)
        loop(n * (late + 1), tile, n * late)

    before = {NG2: None, NO: NG2, NQ: NO}

    def give(k, j):
        make, buf, n = sets[k][0], sets[k][1], sets[k][5]
        slot = j % 2
        if before[k] is not None:
            @pl.when(j < 2)
            def _():
                core_copy(before[k], j, 0, slot).wait_send()

        if 2 * tiles_of(k) > 2:
            @pl.when(j >= 2)
            def _():
                core_copy(k, j, 0, slot).wait_send()

        stage[slot, 0:n, 0:buf.shape[1]] = make(whole_row(k, j), n, 1 - core, 0).astype(bf16)
        core_copy(k, j, 0, slot).start()

    def x_copy(k, q):
        _, buf, far, _, _, _, m, _, _ = sets[k]
        i, j = q // moves_of(k), q % moves_of(k)
        row = place(k, j, m)
        return send(buf.at[part((1 - s) * half_of(k) + row, m), cols(k, i)], far.at[part(row, m), cols(k, i)],
                    x_s.at[k, q], x_r.at[k, q], dev_x)

    def take(k, j, i=0):
        make, buf, n, m = sets[k][0], sets[k][1], sets[k][5], sets[k][6]
        rows, at = part(whole_row(k, j), n), cols(k, i)
        core_copy(k, j, i, 0).wait_recv()
        buf[rows, at] = (make(whole_row(k, j), n, core, i) + buf[rows, at].astype(f32)).astype(bf16)

        @pl.when(j < tiles_of(k))
        def _():
            for e in range(n // m):
                x_copy(k, i * moves_of(k) + j * (n // m) + e).start()

    def takes(k, j0, j1, i=0):
        loop(j1, lambda j: take(k, j, i), j0)

    def gives(k, j0, j1):
        loop(j1, lambda j: give(k, j), j0)

    def hi_first(k, q):
        _, buf, _, back, _, _, m, _, _ = sets[k]
        per = moves_of(k) // 2
        i, j = q // per, q % per
        other = hi + (his // 2) * (1 - 2 * top)
        return send(buf.at[part(s * half_of(k) + place(k, j, m), m), cols(k, i)], back.at[mul_of(j, m), cols(k, i)],
                    h0_s.at[k, q], h0_r.at[k, q], (s, rep(other, t, core)))

    edge = tz == top
    relays = (relay_d, relay_gu, relay_q)

    def relay_in(k, q):
        _, buf, _, _, _, _, m, _, _ = sets[k]
        per = moves_of(k) // 2
        i, j = q // per, q % per
        return send(buf.at[part(s * half_of(k) + place(k, j, m), m), cols(k, i)], relays[k].at[mul_of(j, m), cols(k, i)],
                    rl_s.at[k, q], rl_r.at[k, q], dev_z)

    def relay_out(k, q):
        _, _, _, back, _, _, m, _, _ = sets[k]
        per = moves_of(k) // 2
        i, j = q // per, q % per
        other = hi + (his // 2) * (1 - 2 * top)
        at = (mul_of(j, m), cols(k, i))
        return send(relays[k].at[at], back.at[at], rf_s.at[k, q], h0_r.at[k, q], (s, rep(other, t_z, core)))

    def hi_send(k, q):
        @pl.when(edge)
        def _():
            relay_in(k, q).start()

        @pl.when(jnp.logical_not(edge))
        def _():
            hi_first(k, q).start()

    def relay(k, q0, q1):
        @pl.when(jnp.logical_not(edge))
        def _():
            def piece(q):
                relay_in(k, q).wait_recv()
                relay_out(k, q).start()

            loop(q1, piece, q0)

    def add_rows(buf, row, far, far_row, n, at, final=None):
        step = min(n, 64)

        def rows_of(j):
            rows = part(row + j * step, step)
            ours, theirs_ = buf[rows, at], far[part(far_row + j * step, step), at]
            if final is None:
                buf[rows, at] = ours + theirs_
            else:
                final[mul_of(j, step), at] = ours.astype(f32) + theirs_.astype(f32)

        loop(n // step, rows_of)

    def x_add(k, q0, q1):
        _, buf, far, _, _, _, m, _, _ = sets[k]

        def piece(q):
            i, j = q // moves_of(k), q % moves_of(k)
            row = place(k, j, m)
            x_copy(k, q).wait_recv()
            add_rows(buf, s * half_of(k) + row, far, row, m, cols(k, i))
            if k != NO:
                @pl.when(j < moves_of(k) // 2)
                def _():
                    hi_send(k, i * (moves_of(k) // 2) + j)

        loop(q1, piece, q0)

    def hi_later(k):
        half = half_of(k)
        base, size, at, out = top * (half // 2), half // 2, half // 2, []
        for level in range(1, d.levels):
            size //= 2
            weight = his >> (level + 1)
            bit = (hi // weight) % 2
            out.append((level - 1, base + (1 - bit) * size, base + bit * size, size, at, hi + weight * (1 - 2 * bit)))
            base = base + bit * size
            at += size
        return out, base, size

    def hi_copy(k, step):
        level, far_row, _, size, at, other = step
        return send(sets[k][1].at[part(s * half_of(k) + far_row, size)], sets[k][3].at[pl.ds(at, size)],
                    h_s.at[k, level], h_r.at[k, level], (s, rep(other, t, core)))

    def hi_finish(k, final=None, then=None):
        _, buf, _, back, _, _, m, chunks, _ = sets[k]
        per = moves_of(k) // 2
        last = final if d.levels == 1 else None

        def piece(q):
            i, j = q // per, q % per
            hi_first(k, q).wait_recv()
            add_rows(buf, s * half_of(k) + place(k, j + per, m), back, j * m, m, cols(k, i), last)
            if then is not None and d.levels == 1:
                loop(m // d.own, lambda e: then(k, q * (m // d.own) + e))

        assert last is None or per == 1
        loop(per * chunks, piece)
        later = hi_later(k)[0]
        for step in later:
            hi_copy(k, step).start()
            hi_copy(k, step).wait_recv()
            add_rows(buf, s * half_of(k) + step[2], back, step[4], step[3], pl.ds(0, buf.shape[1]),
                     final if step is later[-1] else None)

    me = t * CORES + core

    def kept(k, slot):
        return gg2.at[part(slot * d.own, d.own), pl.ds(0, fh) if k == NG2 else pl.ds(fh, half_q)]

    def keep_piece(k, p):
        base = hi_later(k)[1]
        src = sets[k][1].at[part(s * half_of(k) + base + p * d.own, d.own)]

        @pl.when(me != p)
        def _():
            send(src, kept(k, me), a_s.at[k - 1, p], a_r.at[k - 1, me], (s, rep(hi, p // CORES, p % CORES))).start()

        @pl.when(me == p)
        def _():
            pltpu.make_async_copy(src, kept(k, me), a_r.at[k - 1, me]).start()

    def keep_start(k):
        loop(TP * CORES, lambda p: keep_piece(k, p))

    def keep_out(k, p):
        rows = part(p * d.own, d.own)
        if k == NQ:
            for c in range(3):
                e = (p % CORES) * 3 + c
                yield (gg2.at[rows, pl.ds(fh + c * HD, HD)],
                       qkv_h.at[e // 2, :, part(((e % 2) * TP + p // CORES) * HD, HD)])
        elif d.direct:
            w = 2 * unit
            for c in range(d.S * his):
                yield gg2.at[rows, pl.ds(c * w, w)], gu_h.at[p % CORES, :, part((c * TP + p // CORES) * w, w)]
        else:
            yield gg2.at[rows, pl.ds(0, fh)], gu_h.at[p]

    def keep_wait(k):
        def piece(p):
            pltpu.make_async_copy(kept(k, p), kept(k, p), a_r.at[k - 1, p]).wait()
            for src, dst in keep_out(k, p):
                pltpu.make_async_copy(src, dst, ko.at[k - 1, p]).start()

        loop(TP * CORES, piece)

    def keep_end(k):
        def piece(p):
            pltpu.make_async_copy(kept(k, p), kept(k, p), ko.at[k - 1, p]).wait()

            @pl.when(me != p)
            def _():
                send(kept(k, p), kept(k, p), a_s.at[k - 1, p], a_r.at[k - 1, me], (s, rep(hi, p // CORES, p % CORES))).wait_send()

        loop(TP * CORES, piece)

    partners = [dev_y, dev_z, dev_c, dev_x]
    for level in range(d.levels):
        weight = his >> (level + 1)
        bit = (hi // weight) % 2
        partners.append((s, rep(hi + weight * (1 - 2 * bit), t, core)))

    def gain_copy(n):
        return send(gsum, grecv.at[n], gn_s.at[n], gn_r.at[n], partners[n])

    def gain_step(n):
        if n:
            gain_copy(n - 1).wait_send()
            gain_copy(n - 1).wait_recv()
            gsum[...] += grecv[n - 1]
        if n < len(partners):
            gain_copy(n).start()

    ag_start(gdall, 2, 0)
    ag_start(gdall, 2, 1)
    ag_start(gdall, 2, 2)
    ag_fwd(gdall, 2, 0)
    ag_start(gdall, 2, 3)
    ag_fwd(gdall, 2, 1)
    def grad_hidden(i):
        chunk = pl.ds(i * CW, CW)

        def tile(n):
            at = mul_of(n, NT)
            value = dot_nt(gdall[:, chunk], wd[at, chunk])
            acc[:, at] = value if i == 0 else acc[:, at] + value
            value = dot_nt(gdall[:, chunk], wd[part(CW + n * NT, NT), chunk]).reshape(TP, L, NT)
            k2[:, :, at] = value if i == 0 else k2[:, :, at] + value

        loop(CW // NT, tile)

    for i in range(CHUNKS):
        ag_done(gdall, 2, i)
        if i + 2 < CHUNKS:
            ag_fwd(gdall, 2, i + 2)
        give_down(0, i)
        grad_hidden(i)
        if i:
            takes(ND, 0, 2, i - 1)
    ag_drain(gdall, 2)

    def hidden_back(half):
        step = L // 2

        def tile(n):
            at = mul_of(n, NT)
            g_at, u_at = part(half * CW + n * NT, NT), part(fh + half * CW + n * NT, NT)

            def rows_of(j):
                rows = mul_of(j, step)
                g, u = gu[rows, g_at], gu[rows, u_at]
                gh = k2[j // 2, mul_of(j % 2, step), at] if half else acc[rows, at]
                sig = jax.nn.sigmoid(g)
                gg2[rows, g_at] = (gh * u * sig * (1.0 + g * (1.0 - sig))).astype(bf16)
                gg2[rows, u_at] = (gh * (g * sig)).astype(bf16)

            loop(T // step, rows_of)

        loop(CW // NT, tile)

    hidden_back(0)
    hidden_back(1)
    takes(ND, 0, 2, CHUNKS - 1)

    def res_chunk(i):
        acc[...] = dot_nt(gg2[...], wgu[mul_of(i, CW), :])

    def res_extra(i):
        give(NG2, i)

        @pl.when(i > 0)
        def _():
            take(NG2, i - 1)

    def res_between(i):
        if i == 0:
            take(NG2, 3)
            give_down(1, 0)
            give_down(1, 1)
        elif i == 1:
            give_down(1, 2)
            give_down(1, 3)
        else:
            for c in range(CHUNKS):
                takes(ND, 2, 4, c)
            x_add(ND, 0, 4)
            gives(NG2, 4, 8)

    rs(2, cbuf, res_chunk, res_between, res_extra)

    def attn_grad_rows(j):
        rows = mul_of(j, BL)
        gr = cbuf[rows, :] + cot[rows, :].astype(f32)
        cbuf[rows, :] = gr
        a = abuf[rows, :]
        scale = lax.rsqrt(jnp.mean(a * a, axis=-1, keepdims=True) + eps_norm)
        weighted = gr * gat[...]
        inner = jnp.mean(weighted * a, axis=-1, keepdims=True)
        ga = scale * weighted - a * scale**3 * inner
        gaall[part(t * L + j * BL, BL), :] = ga.astype(bf16)
        gsum[:, 0:D] += jnp.sum(gr * a * scale, axis=0, keepdims=True)

    loop(L // BL, attn_grad_rows)

    def attend_back(b):
        rows = blk(b)
        acc[rows, 0:ha] = dot_nt(gaall[rows, :], wo[...])
        scale = columns(2, b)
        cos, sin = cos_v[...], sin_v[...]
        for h in range(heads):
            head = pl.ds(h * HD, HD)
            gm = acc[rows, head].astype(bf16)
            p = probs[b * heads + h]
            gqkv[rows, pl.ds(2 * ha + h * HD, HD)] = dot_tn(p.astype(bf16), gm).astype(bf16)
            gp = dot_nt(gm, vb[rows, head])
            gs = p * (gp - jnp.sum(p * gp, axis=-1, keepdims=True))
            gs = (gs * inv).astype(bf16)
            turned = (dot_nn(gs, qkrot[rows, pl.ds(ha + h * HD, HD)]), dot_tn(gs, qkrot[rows, head]))
            for which in range(2):
                at = pl.ds(which * ha + h * HD, HD)
                gn = turned[which] * cos - pltpu.roll(turned[which], HD // 2, 1) * sin
                field = qk[rows, at]
                spot = part(2 * D + which * d.att + t * ha + h * HD, HD)
                gsum[:, spot] += jnp.sum(gn * field * scale[which], axis=0, keepdims=True)
                gu[rows, at] = gn * gain_of(which, h)

    for i in range(CHUNKS):
        ag_start(gaall, 3, i)
    attend_back(t)
    ag_fwd(gaall, 3, 0)
    takes(NG2, 4, 6)
    ag_fwd(gaall, 3, 1)
    takes(NG2, 6, 8)
    ag_fwd(gaall, 3, 2)
    ag_fwd(gaall, 3, 3)
    x_add(ND, 4, 8)
    relay(ND, 0, 2)
    x_add(NG2, 0, 1)
    loop(2, lambda j: attend_back(t_y + j * (t_z - t_y)))
    for i in range(CHUNKS):
        ag_done(gaall, 3, i)
    attend_back(t_d)
    gain_step(0)
    gives(NO, 0, 2)
    relay(ND, 2, 4)
    ag_drain(gaall, 3)

    def products(rows):
        return gu[rows, 0:2 * ha] * qk[rows, :]

    def in_stat():
        takes(NO, 0, 2)

    stat[3] = stat_sum(1, products, in_stat) / d.att
    gain_step(1)
    x_add(NG2, 1, 3)

    def qk_back(b):
        rows = blk(b)
        scale, inner = columns(2, b), columns(3, b)
        for which in range(2):
            at = pl.ds(which * ha, ha)
            sc = scale[which]
            gqkv[rows, at] = (sc * gu[rows, at] - qk[rows, at] * (sc**3 * inner[which])).astype(bf16)

    loop(TP, qk_back)
    gain_step(2)

    def in_chunk(i):
        acc[...] = dot_nt(gqkv[...], wqkv[mul_of(i, CW), :])

    def in_extra(i):
        give(NQ, i)

        @pl.when(i == 2)
        def _():
            x_add(NG2, 3, 4)

        @pl.when(i > 0)
        def _():
            take(NQ, i - 1)

    def in_between(i):
        if i == 0:
            take(NQ, 3)
            relay(NG2, 0, 2)
            gives(NQ, 4, 8)
            gain_step(3)
        elif i == 1:
            takes(NQ, 4, 8)
            relay(NG2, 2, 3)
        else:
            x_add(NQ, 0, 2)
            gain_step(4)
            relay(NG2, 3, 4)
            x_add(NG2, 4, 8)
            hi_finish(ND, abuf)
            pltpu.make_async_copy(abuf.at[0:unit], down_h, loc.at[4]).start()

    rs(3, bbuf, in_chunk, in_between, in_extra)

    def input_rows(j):
        rows = mul_of(j, BL)
        bbuf[rows, :] += cbuf[rows, :]

    loop(L // BL, input_rows)
    put_gin = pltpu.make_async_copy(bbuf, gin_h, loc.at[5])
    put_gin.start()

    x_add(NQ, 2, 4)
    relay(NQ, 0, 2)
    x_add(NO, 0, 1)
    hi_finish(NG2, None, keep_piece)
    if d.levels > 1:
        keep_start(NG2)

    for p in range(d.pieces):
        o_pc[p] = rc_o[part(s * HD + p * d.own_o, d.own_o), :]
    o_slot = hi * CORES + core

    def o_start(p):
        goal = t * d.pieces + p

        @pl.when(goal != r)
        def _():
            send(o_pc.at[p], o_h.at[o_slot], o_s.at[p], o_r.at[o_slot], (s, goal)).start()

        @pl.when(goal == r)
        def _():
            pltpu.make_async_copy(o_pc.at[p], o_h.at[o_slot], o_r.at[o_slot]).start()

    loop(d.pieces, o_start)
    hi_finish(NQ)
    keep_start(NQ)
    for n in range(5, len(partners) + 1):
        gain_step(n)
    gg_o[...] = gsum[...]

    keep_wait(NG2)
    keep_wait(NQ)
    keep_end(NG2)
    keep_end(NQ)

    def o_wait(q):
        pltpu.make_async_copy(o_pc.at[0], o_pc.at[0], o_r.at[q]).wait()

    loop(his * CORES, o_wait)

    def o_sent(p):
        goal = t * d.pieces + p

        @pl.when(goal != r)
        def _():
            send(o_pc.at[p], o_h.at[o_slot], o_s.at[p], o_r.at[o_slot], (s, goal)).wait_send()

    loop(d.pieces, o_sent)
    far_gain.wait_send()
    for k in range(NG):
        cross(k).wait_send()
        share(k).wait_send()
    for i in range(CHUNKS - 2, CHUNKS):
        loop(2 * tiles_of(ND), lambda j: core_copy(ND, j, i, 4 * (i % 2) + j).wait_send())
    for slot in range(2):
        core_copy(NQ, slot, 0, slot).wait_send()
    for k in range(4):
        loop(moves_of(k) * sets[k][7], lambda q: x_copy(k, q).wait_send())
    for k in range(3):
        @pl.when(edge)
        def _():
            loop(moves_of(k) // 2 * sets[k][7], lambda q: relay_in(k, q).wait_send())

        @pl.when(jnp.logical_not(edge))
        def _():
            loop(moves_of(k) // 2 * sets[k][7], lambda q: (hi_first(k, q).wait_send(), relay_out(k, q).wait_send()))

        for step in hi_later(k)[0]:
            hi_copy(k, step).wait_send()
    put_out.wait()
    put_gin.wait()
    pltpu.make_async_copy(abuf.at[0:unit], down_h, loc.at[4]).wait()


def body(shards, replicas, x_in, cotangent, w_query, w_key, w_value, w_out, w_gate, w_up, w_down,
         gain_query, gain_key, gain_attn, gain_mlp):
    seqs, length, width = x_in.shape
    assert seqs == 1
    d = Dims(length, width, w_query.shape[1], w_gate.shape[1], shards, replicas)
    r = lax.axis_index("replica")
    s = lax.axis_index("shard")
    t = (r // CORES) % TP

    def at(array, axis, index):
        return lax.dynamic_index_in_dim(array, index, axis, keepdims=False)

    def hidden_cols(w):
        picked = at(w.reshape(w.shape[0], d.S, d.his, TP, CORES, d.unit), 3, t)
        return picked.transpose(0, 3, 1, 2, 4).reshape(w.shape[0], d.fh)

    if not d.direct:
        w_gate = jnp.concatenate([hidden_cols(w_gate), hidden_cols(w_up)], axis=1)
        w_down = at(w_down.reshape(d.his, TP, CORES, d.unit, width), 1, t).transpose(1, 0, 2, 3).reshape(-1, width)
    gain = jnp.concatenate([at(gain_query.reshape(TP, HD), 0, t), at(gain_key.reshape(TP, HD), 0, t),
                            gain_attn, gain_mlp]).astype(f32)[None]
    cos, sin = rope_tables(length, HD // 2)
    cos = np.concatenate([cos, cos], axis=1)
    sin = np.concatenate([-sin, sin], axis=1)

    L, D, T, ha, fh = d.L, d.D, d.T, d.ha, d.fh
    CW = D // CHUNKS
    vm = pltpu.VMEM
    dma = pltpu.SemaphoreType.DMA
    any_ = pl.BlockSpec(memory_space=pl.ANY)
    vmem = pl.BlockSpec(memory_space=pltpu.VMEM)
    hi_rows = lambda n: max(n - n // d.his, 16)
    steps = 4 + d.levels
    later = max(d.levels - 1, 1)
    scratch = [
        vm((D, 3 * ha), bf16), vm((ha, D), bf16), vm((D, 2 * fh), bf16), vm((fh, D), bf16),
        vm((2, 1, d.gains), f32), vm((1, D), f32), vm((1, D), f32),
        vm((T, D), bf16), vm((T, D), bf16), vm((T, D), bf16), vm((T, D), bf16), vm((L, D), bf16),
        vm((T, 2 * ha), f32), vm((T, ha), bf16), vm((T, 2 * ha), bf16), vm((TP * ha // HD, L, L), f32),
        vm((T, ha), bf16), vm((T, 3 * ha), bf16), vm((4, 8, T), f32), vm((2, 3, 8, T), f32),
        vm((T, 2 * fh), f32), vm((T, fh), bf16), vm((T, 2 * fh), bf16),
        vm((L, D), f32), vm((L, D), f32), vm((L, D), f32), vm((L, D), bf16),
        vm((T, CW), f32), vm((CHUNKS, 2, L, CW), bf16), vm((CHUNKS, L, CW), bf16),
        vm((CHUNKS, 2, L, CW), bf16), vm((CHUNKS, L, CW), bf16), vm((CHUNKS, L, CW), f32),
        vm((8, 128, CW), bf16), vm((2, 256, fh), bf16),
        vm((D, fh), bf16), vm((fh // 2, D), bf16), vm((D, 3 * ha // 2), bf16), vm((ha, D // 2), bf16),
        vm((D // 2, fh), bf16), vm((fh // 4, D), bf16), vm((D // 2, 3 * ha // 2), bf16), vm((ha // 2, D // 2), bf16),
        vm((hi_rows(D // 2), fh), bf16), vm((hi_rows(fh // 4), D), bf16), vm((hi_rows(D // 2), 3 * ha // 2), bf16),
        vm((d.pieces, d.own_o, D // 2), bf16),
        vm((1, d.ggs), f32), vm((steps, 1, d.ggs), f32),
        dma((4, CHUNKS, 4)), dma((4, CHUNKS, 4)), dma((4, CHUNKS, 4)), dma((4, CHUNKS, 4)),
        dma((11,)), dma((11,)), dma((10,)), dma((10,)), dma((10, 2)), dma((6,)), dma((2, 3)), dma((2, 3)),
        dma((2, 8)), dma((4, 16)), dma((4, 8)), dma((4, 8)), dma((3, 4)), dma((3, 4)), dma((3, 4)), dma((3, 4)), dma((3, 4)),
        dma((3, later)), dma((3, later)),
        dma((2, TP * CORES)), dma((2, TP * CORES)), dma((2, TP * CORES)), dma((d.pieces,)), dma((d.his * CORES,)), dma((steps,)), dma((steps,)),
    ]
    struct = jax.ShapeDtypeStruct
    gu_shape = (2, d.own, d.ff) if d.direct else (TP * CORES, d.own, fh)
    results = pl.pallas_call(
        functools.partial(kernel, d),
        out_shape=(
            struct((L, D), bf16), struct((L, D), f32), struct(gu_shape, bf16), struct((3, d.own, d.att), bf16),
            struct((d.unit, D), f32), struct((d.his * CORES, d.own_o, D // 2), bf16),
            struct((fh // 8, D), bf16), struct((D // 4, fh), bf16), struct((D // 4, 3 * ha // 2), bf16),
            struct((1, d.ggs), f32),
        ),
        in_specs=[any_] * 9 + [vmem] * 3,
        out_specs=(any_,) * 9 + (vmem,),
        scratch_shapes=scratch,
        compiler_params=pltpu.CompilerParams(
            collective_id=0, has_side_effects=True, vmem_limit_bytes=67043328),
        name="layer",
    )(x_in[0], cotangent[0], w_query, w_key, w_value, w_out, w_gate, w_up, w_down, gain, cos, sin)
    out, gin, gu, qkv, down, o = results[:6]
    gg = results[-1]

    def hidden_out(k):
        if d.direct:
            return gu[k].astype(f32)
        block = gu.reshape(TP, CORES, d.own, fh)[:, k]
        spread = block.reshape(TP, d.own, CORES, d.S, d.his, d.unit).transpose(1, 3, 4, 0, 2, 5)
        return spread.reshape(d.own, d.ff).astype(f32)

    o = o.reshape(d.his, CORES, d.own_o, D // 2).astype(f32).sum(0).transpose(1, 0, 2).reshape(d.own_o, D)
    gg = gg[0]
    here = s * d.R + r

    def share(vec):
        n = vec.shape[0] // (d.S * d.R)
        return lax.dynamic_slice_in_dim(vec, here * n, n)

    def head_gain(vec):
        return share(vec.reshape(TP, d.S, HD).transpose(1, 0, 2).reshape(-1))

    return (
        out[None], gin[None], qkv[0].astype(f32), qkv[1].astype(f32), qkv[2].astype(f32), o,
        hidden_out(0), hidden_out(1), down,
        head_gain(gg[2 * D:2 * D + d.att]), head_gain(gg[2 * D + d.att:]), share(gg[:D]), share(gg[D:2 * D]),
    )


def solution(mesh):
    both = ("shard", "replica")
    token = P(both, None, None)
    weight = P("shard", None)
    return jax.shard_map(
        functools.partial(body, mesh.shape["shard"], mesh.shape["replica"]),
        mesh=mesh,
        in_specs=(token, token) + (weight,) * 7 + (P("shard"),) * 4,
        out_specs=(token, token) + (P(both, None),) * 7 + (P(both),) * 4,
        check_vma=False,
    )
```

```python
import functools
import math

import jax
import jax.numpy as jnp
import numpy as np
from jax import lax
from jax.experimental import pallas as pl
from jax.experimental.pallas import tpu as pltpu
from jax.sharding import PartitionSpec as P

HD = 128
TP = 4
CORES = 2
CHUNKS = 4
Z_AG = (256, 256, 256, 0)
Z_RS = (256, 256, 256, 128)

eps_norm = 1e-06
rope_theta = 500000.0

bf16 = jnp.bfloat16
f32 = jnp.float32


def rope_tables(length, half):
    position = np.arange(length).astype(np.float32)[:, None]
    exponent = np.arange(half).astype(np.float32) * np.float32(1.0 / half)
    angle = position * np.float32(rope_theta) ** (-exponent)
    return (np.cos(angle).astype(np.float32), np.sin(angle).astype(np.float32))


def dot_nn(left, right):
    return lax.dot_general(left, right, (((1,), (0,)), ((), ())), preferred_element_type=f32)


def dot_nt(left, right, precision=None):
    return lax.dot_general(
        left, right, (((1,), (1,)), ((), ())), preferred_element_type=f32, precision=precision)


def dot_tn(left, right):
    return lax.dot_general(left, right, (((0,), (0,)), ((), ())), preferred_element_type=f32)


def mul_of(index, step):
    return pl.ds(pl.multiple_of(index * step, step), step)


def loop(count, step, start=0):
    lax.fori_loop(start, count, lambda i, c: (step(i), c)[1], 0)


class Dims:
    def __init__(self, length, width, att, ff, shards, replicas):
        self.L, self.D, self.att, self.ff = length, width, att, ff
        self.S, self.R = shards, replicas
        self.his = replicas // (TP * CORES)
        self.T = TP * length
        self.ha = att // TP
        self.fh = ff // TP
        self.unit = ff // (shards * replicas)
        self.own = width // (shards * replicas)
        self.own_o = att // (shards * replicas)
        self.pieces = HD // self.own_o
        self.levels = self.his.bit_length() - 1
        self.gains = 2 * HD + width
        self.ggs = 2 * width + 2 * att
        self.direct = self.unit % 128 == 0
        assert shards == 2 and self.his == 1 << self.levels and self.levels > 0 and self.ha == shards * HD
        assert self.fh == 2 * (width // CHUNKS)


def kernel(
    d,
    x_h, cot_h, wq_h, wk_h, wv_h, wo_h, wg_h, wu_h, wd_h, gain_v, cos_v, sin_v,
    out_h, gin_h, gu_h, qkv_h, down_h, o_h, relay_d, relay_gu, relay_q, gg_o,
    wqkv, wo, wgu, wd, gbuf, gat, gml,
    xall, rall, gdall, gaall, cot,
    qk, vb, qkrot, probs, mixed, gqkv, stat, statr,
    gu, hid, gg2,
    abuf, bbuf, cbuf, outb,
    acc, s1, s2, r1, r2, k2,
    stage_d, stage, rc_gu, rc_d, rc_q, rc_o, rx_gu, rx_d, rx_q, rx_o, rh_gu, rh_d, rh_q, o_pc,
    gsum, grecv,
    ag_s, ag_r, rs_s, rs_r, w_s, w_r, wf_s, wf_r, w_l, loc, st_s, st_r,
    stg_s, c_r, x_s, x_r, h0_s, h0_r, rl_s, rl_r, rf_s, h_s, h_r, a_s, a_r, ko, o_s, o_r, gn_s, gn_r,
):
    L, D, T, ha, fh, his, unit = d.L, d.D, d.T, d.ha, d.fh, d.his, d.unit
    CW = D // CHUNKS
    HW = CW // 2
    s = lax.axis_index("shard")
    r = lax.axis_index("replica")
    hi, t, core = r // (TP * CORES), (r // CORES) % TP, r % CORES
    tz, ty = t // 2, t % 2
    t_y, t_z, t_d = tz * 2 + 1 - ty, (1 - tz) * 2 + ty, (1 - tz) * 2 + 1 - ty

    def rep(hi_, t_, core_):
        return hi_ * (TP * CORES) + t_ * CORES + core_

    dev_y, dev_z, dev_d = ((s, rep(hi, q, core)) for q in (t_y, t_z, t_d))
    dev_x = (1 - s, r)
    dev_c = (s, rep(hi, t, 1 - core))

    def send(src, dst, ssem, rsem, dev):
        return pltpu.make_async_remote_copy(
            src_ref=src, dst_ref=dst, send_sem=ssem, recv_sem=rsem, device_id=dev,
            device_id_type=pl.DeviceIdType.MESH)

    def blk(q):
        return mul_of(q, L)

    def part(base, n):
        return pl.ds(pl.multiple_of(base, n), n)

    def ag_copies(buf, inst, i, src=None):
        own = buf.at[blk(t), mul_of(i, CW)]
        first = own if src is None else src.at[:, mul_of(i, CW)]
        wz = Z_AG[inst]
        fy = buf.at[blk(t_y), pl.ds(pl.multiple_of(i * CW + CW - wz, 128), wz)] if wz else None
        fz = buf.at[blk(t_z), pl.ds(pl.multiple_of(i * CW, 128), CW - wz)]
        ends = ((first, own, dev_y), (first, own, dev_z), (fy, fy, dev_z), (fz, fz, dev_y))

        def copy(j):
            return send(ends[j][0], ends[j][1], ag_s.at[inst, i, j], ag_r.at[inst, i, j], ends[j][2])

        return copy

    def ag_start(buf, inst, i, src=None):
        c = ag_copies(buf, inst, i, src)
        c(0).start()
        c(1).start()

    def ag_fwd(buf, inst, i):
        c = ag_copies(buf, inst, i)
        c(1).wait_recv()
        c(3).start()
        c(0).wait_recv()
        if Z_AG[inst]:
            c(2).start()

    def ag_done(buf, inst, i):
        c = ag_copies(buf, inst, i)
        if Z_AG[inst]:
            c(2).wait_recv()
        c(3).wait_recv()

    def ag_drain(buf, inst):
        def wait(i):
            c = ag_copies(buf, inst, i)
            for j in range(4):
                if j != 2 or Z_AG[inst]:
                    c(j).wait_send()

        loop(CHUNKS, wait)

    def ag(buf, inst, src=None, between=lambda i: None):
        ag_start(buf, inst, 0, src)
        ag_start(buf, inst, 1, src)
        for i in range(CHUNKS):
            ag_fwd(buf, inst, i)
            if i + 2 < CHUNKS:
                ag_start(buf, inst, i + 2, src)
            between(i)
        for i in range(CHUNKS):
            ag_done(buf, inst, i)
        ag_drain(buf, inst)

    def rs_copies(inst, i):
        wa = CW - Z_RS[inst]
        ya, zb = pl.ds(0, wa), pl.ds(wa, CW - wa)

        def copy(j):
            if j == 0:
                a, b, dev = s1.at[i, :, :, ya], r1.at[i, :, :, ya], dev_y
            elif j == 1:
                a, b, dev = s1.at[i, :, :, zb], r1.at[i, :, :, zb], dev_z
            elif j == 2:
                a, b, dev = s2.at[i, :, ya], r2.at[i, :, ya], dev_z
            else:
                a, b, dev = s2.at[i, :, zb], r2.at[i, :, zb], dev_y
            return send(a, b, rs_s.at[inst, i, j], rs_r.at[inst, i, j], dev)

        return copy

    def rs_send(inst, i, dest):
        c = rs_copies(inst, i)
        wa = CW - Z_RS[inst]
        step = L // 4

        def rows_of(j):
            def rows(q):
                return part(q * L + j * step, step)

            here = mul_of(j, step)
            s1[i, 0, here, 0:wa] = acc[rows(t_y), 0:wa].astype(bf16)
            k2[i, here, 0:wa] = acc[rows(t_z), 0:wa]
            if wa < CW:
                s1[i, 0, here, wa:CW] = acc[rows(t_z), wa:CW].astype(bf16)
                k2[i, here, wa:CW] = acc[rows(t_y), wa:CW]
            s1[i, 1, here] = acc[rows(t_d), :].astype(bf16)
            dest[here, mul_of(i, CW)] = acc[rows(t), :]

        loop(4, rows_of)
        c(0).start()
        if wa < CW:
            c(1).start()

    def rs_fwd(inst, i, dest):
        c = rs_copies(inst, i)
        wa = CW - Z_RS[inst]
        c(0).wait_recv()
        s2[i, :, 0:wa] = (k2[i, :, 0:wa] + r1[i, 1, :, 0:wa].astype(f32)).astype(bf16)
        c(2).start()
        if wa < CW:
            c(1).wait_recv()
            s2[i, :, wa:CW] = (k2[i, :, wa:CW] + r1[i, 1, :, wa:CW].astype(f32)).astype(bf16)
            c(3).start()
        dest[:, mul_of(i, CW)] += r1[i, 0].astype(f32)

    def rs_done(inst, i, dest):
        c = rs_copies(inst, i)
        c(2).wait_recv()
        if Z_RS[inst]:
            c(3).wait_recv()
        dest[:, mul_of(i, CW)] += r2[i].astype(f32)

    def rs(inst, dest, compute, between=lambda i: None, extra=lambda i: None):
        def first(i):
            compute(i)
            rs_send(inst, i, dest)
            extra(i)

            @pl.when(i >= 2)
            def _():
                rs_fwd(inst, i - 2, dest)

        loop(CHUNKS, first)
        between(0)
        rs_fwd(inst, CHUNKS - 2, dest)
        between(1)
        rs_fwd(inst, CHUNKS - 1, dest)
        between(2)
        loop(CHUNKS, lambda i: rs_done(inst, i, dest))

        def wait(i):
            c = rs_copies(inst, i)
            for j in range(4):
                if j % 2 == 0 or Z_RS[inst]:
                    c(j).wait_send()

        loop(CHUNKS, wait)

    def qkv_region(s_, piece):
        return wqkv.at[part(s_ * (D // 2) + piece * (D // 4), D // 4)]

    def qkv_parts(s_, piece):
        rows, to = part(piece * (D // 4), D // 4), part(s_ * (D // 2) + piece * (D // 4), D // 4)
        for which, src in enumerate((wq_h, wk_h, wv_h)):
            for h in range(d.S):
                yield src.at[rows, part((h * TP + t) * HD, HD)], wqkv.at[to, pl.ds(which * ha + h * HD, HD)]

    def o_region(s_, piece):
        return wo.at[part(s_ * HD + piece * (HD // 2), HD // 2)]

    def o_parts(s_, piece):
        yield wo_h.at[part(t * HD + piece * (HD // 2), HD // 2)], o_region(s_, piece)

    SUBS = 4

    def gu_group(sub):
        n = D // 4 // SUBS

        def region(s_, piece):
            return wgu.at[part(s_ * (D // 2) + piece * (D // 4) + sub * n, n)]

        def parts(s_, piece):
            rows = part(piece * (D // 4) + sub * n, n)
            to = part(s_ * (D // 2) + piece * (D // 4) + sub * n, n)
            w = 2 * unit
            if not d.direct:
                yield wg_h.at[rows], wgu.at[to]
                return
            for m, src in enumerate((wg_h, wu_h)):
                for c in range(d.S * his):
                    yield src.at[rows, part((c * TP + t) * w, w)], wgu.at[to, pl.ds(m * fh + c * w, w)]

        return parts, region

    def d_group(sub):
        at = mul_of(sub, CW)
        n = fh // 4

        def region(s_, piece):
            return wd.at[part(((s_ * 2 + piece) if d.direct else (piece * 2 + s_)) * n, n), at]

        def parts(s_, piece):
            w = 2 * unit
            if not d.direct:
                yield wd_h.at[part(piece * n, n), at], region(s_, piece)
                return
            step = min(w, n)
            for e in range(n // step):
                first = piece * n + e * step
                src = (first // w) * (TP * w) + t * w + first % w
                yield wd_h.at[part(src, step), at], wd.at[part(s_ * (fh // 2) + first, step), at]

        return parts, region

    GU0, DN0 = 2, 2 + SUBS
    NG = DN0 + CHUNKS

    def group_of(k):
        if isinstance(k, int) and k < DN0:
            return ((qkv_parts, qkv_region), (o_parts, o_region))[k] if k < GU0 else gu_group(k - GU0)
        return d_group(k - DN0)

    def local_start(k):
        for piece in range(2):
            for src, dst in group_of(k)[0](s, piece):
                pltpu.make_async_copy(src, dst, w_l.at[k, piece]).start()

    def local_wait(k):
        for piece in range(2):
            here = group_of(k)[1](s, piece)
            pltpu.make_async_copy(here, here, w_l.at[k, piece]).wait()

    def cross_start(k):
        for src, dst in group_of(k)[0](s, core):
            send(src, dst, w_s.at[k], w_r.at[k], dev_x).start()

    def cross(k):
        here = group_of(k)[1](s, core)
        return send(here, here, w_s.at[k], w_r.at[k], dev_x)

    def share(k):
        here = group_of(k)[1](1 - s, core)
        return send(here, here, wf_s.at[k], wf_r.at[k], dev_c)

    def w_forward(k):
        cross(k).wait_recv()
        share(k).start()

    def w_ready(k):
        local_wait(k)
        share(k).wait_recv()

    own_x = pltpu.make_async_copy(x_h, xall.at[blk(t)], loc.at[0])
    own_cot = pltpu.make_async_copy(cot_h, cot, loc.at[1])
    own_gain = pltpu.make_async_copy(gain_v, gbuf.at[s], loc.at[2])
    far_gain = send(gain_v, gbuf.at[s], w_s.at[NG], w_r.at[NG], dev_x)
    own_x.start()
    local_start(0)
    own_gain.start()
    own_cot.start()

    barrier = pltpu.get_barrier_semaphore()

    def greet(q):
        @pl.when(q != r)
        def _():
            pl.semaphore_signal(barrier, inc=1, device_id=(s, q), device_id_type=pl.DeviceIdType.MESH)

    loop(d.R, greet)
    pl.semaphore_signal(barrier, inc=1, device_id=dev_x, device_id_type=pl.DeviceIdType.MESH)
    pl.semaphore_wait(barrier, d.R)

    ag_start(xall, 0, 0, x_h)
    cross_start(0)
    ag_start(xall, 0, 1, x_h)
    far_gain.start()
    for k in range(1, NG):
        cross_start(k)
    for k in range(1, NG):
        local_start(k)

    for i in range(CHUNKS):
        ag_fwd(xall, 0, i)
        if i + 2 < CHUNKS:
            ag_start(xall, 0, i + 2, x_h)
    w_forward(0)
    own_x.wait()
    own_gain.wait()
    far_gain.wait_recv()
    for q in range(2):
        gat[:, q * (D // 2):(q + 1) * (D // 2)] = gbuf[q, :, 2 * HD:2 * HD + D // 2]
        gml[:, q * (D // 2):(q + 1) * (D // 2)] = gbuf[q, :, 2 * HD + D // 2:]
    gsum[...] = jnp.zeros_like(gsum)
    for i in range(CHUNKS):
        ag_done(xall, 0, i)
    ag_drain(xall, 0)
    w_ready(0)

    qk[:, 0:ha] = dot_nn(xall[...], wqkv[:, 0:ha])
    qk[:, ha:2 * ha] = dot_nn(xall[...], wqkv[:, ha:2 * ha])
    vb[...] = dot_nn(xall[...], wqkv[:, 2 * ha:]).astype(bf16)

    row8 = lax.broadcasted_iota(jnp.int32, (8, 2 * ha), 0)
    col8 = lax.broadcasted_iota(jnp.int32, (8, 2 * ha), 1)
    pick = jnp.where((row8 < 4) == (col8 < ha), 1.0, 0.0).astype(f32)
    HIGH = lax.Precision.HIGHEST

    def stat_sum(k, values, between=lambda: None):
        def sequence(b):
            stat[k, :, blk(b)] = dot_nt(pick, values(blk(b)), HIGH)

        loop(TP, sequence)
        copies = [send(stat.at[k], statr.at[k, j], st_s.at[k, j], st_r.at[k, j], dev)
                  for j, dev in enumerate((dev_y, dev_z, dev_d))]
        for c in copies:
            c.start()
        between()
        for c in copies:
            c.wait_recv()
        for c in copies:
            c.wait_send()
        return stat[k] + statr[k, 0] + statr[k, 1] + statr[k, 2]

    def squares(rows):
        v = qk[rows, :]
        return v * v

    stat[2] = lax.rsqrt(stat_sum(0, squares) / d.att + eps_norm)

    def columns(k, b):
        flat = stat[k, :, blk(b)]
        wide = jnp.concatenate([flat] * (L // 8), axis=0).T
        return wide[:, 0:1], wide[:, 4:5]

    def gain_of(which, h):
        return gbuf[h, :, which * HD:(which + 1) * HD]

    inv = 1.0 / math.sqrt(HD)
    heads = ha // HD

    def attend(b):
        rows = blk(b)
        scale = columns(2, b)
        cos, sin = cos_v[...], sin_v[...]
        above = lax.broadcasted_iota(jnp.int32, (L, L), 0) < lax.broadcasted_iota(jnp.int32, (L, L), 1)
        for h in range(heads):
            rot = []
            for which in range(2):
                at = pl.ds(which * ha + h * HD, HD)
                normed = qk[rows, at] * scale[which] * gain_of(which, h)
                turned = (normed * cos + pltpu.roll(normed, HD // 2, 1) * sin).astype(bf16)
                qkrot[rows, at] = turned
                rot.append(turned)
            scores = jnp.where(above, -jnp.inf, dot_nt(rot[0], rot[1]) * inv)
            peak = jnp.max(scores, axis=-1, keepdims=True)
            log_total = peak + jnp.log(jnp.sum(jnp.exp(scores - peak), axis=-1, keepdims=True))
            p = jnp.exp(scores - log_total)
            probs[b * heads + h] = p
            head = pl.ds(h * HD, HD)
            mixed[rows, head] = dot_nn(p.astype(bf16), vb[rows, head]).astype(bf16)

    loop(TP, attend)
    w_forward(1)
    w_ready(1)

    def attn_chunk(i):
        acc[...] = dot_nn(mixed[...], wo[:, mul_of(i, CW)])

    def attn_between(i):
        if i == 2:
            w_forward(GU0)

    rs(0, abuf, attn_chunk, attn_between)

    BL = 16

    def residual_rows(j):
        rows = mul_of(j, BL)
        a = abuf[rows, :]
        scale = lax.rsqrt(jnp.mean(a * a, axis=-1, keepdims=True) + eps_norm)
        mine = part(t * L + j * BL, BL)
        res = xall[mine, :].astype(f32) + a * scale * gat[...]
        cbuf[rows, :] = res
        rall[mine, :] = res.astype(bf16)

    loop(L // BL, residual_rows)
    NT = 256

    def turn(i):
        return ((i // 2 + s) % 2) * 2 + i % 2

    def gate_up(i):
        chunk = mul_of(turn(i), CW)

        def tile(n):
            at = mul_of(n, NT)
            value = dot_nn(rall[:, chunk], wgu[chunk, at])
            gu[:, at] = value if i == 0 else gu[:, at] + value

        loop(2 * fh // NT, tile)

    ag_start(rall, 1, turn(0))
    ag_start(rall, 1, turn(1))
    w_forward(GU0 + 1)
    ag_fwd(rall, 1, turn(0))
    ag_start(rall, 1, turn(2))
    ag_fwd(rall, 1, turn(1))
    ag_start(rall, 1, turn(3))
    for k in range(GU0, DN0):
        local_wait(k)
    ag_done(rall, 1, turn(0))
    w_forward(GU0 + 2)
    gate_up(0)
    ag_fwd(rall, 1, turn(2))
    ag_done(rall, 1, turn(1))
    ag_fwd(rall, 1, turn(3))
    gate_up(1)
    ag_done(rall, 1, turn(2))
    w_forward(GU0 + 3)
    for k in range(GU0, DN0):
        share(k).wait_recv()
    gate_up(2)
    ag_done(rall, 1, turn(3))
    gate_up(3)
    ag_drain(rall, 1)

    def hidden(n):
        g_at, u_at = mul_of(n, NT), part(fh + n * NT, NT)

        def rows_of(j):
            rows = mul_of(j, 64)
            g, u = gu[rows, g_at], gu[rows, u_at]
            hid[rows, g_at] = (g * jax.nn.sigmoid(g) * u).astype(bf16)

        loop(T // 64, rows_of)

    loop(fh // NT, hidden)
    def down_chunk(i):
        w_forward(DN0 + i)
        w_ready(DN0 + i)
        acc[...] = dot_nn(hid[...], wd[:, mul_of(i, CW)])

    rs(1, bbuf, down_chunk)
    own_cot.wait()

    def output_rows(j):
        rows = mul_of(j, BL)
        dn = bbuf[rows, :]
        scale = lax.rsqrt(jnp.mean(dn * dn, axis=-1, keepdims=True) + eps_norm)
        outb[rows, :] = (cbuf[rows, :] + dn * scale * gml[...]).astype(bf16)
        co = cot[rows, :].astype(f32)
        weighted = co * gml[...]
        inner = jnp.mean(weighted * dn, axis=-1, keepdims=True)
        gd = scale * weighted - dn * scale**3 * inner
        gdall[part(t * L + j * BL, BL), :] = gd.astype(bf16)
        gsum[:, D:2 * D] += jnp.sum(co * dn * scale, axis=0, keepdims=True)

    loop(L // BL, output_rows)
    put_out = pltpu.make_async_copy(outb, out_h, loc.at[3])
    put_out.start()
    half_q = 3 * ha // 2

    def by_cols(left, right, width):
        def make(row, n, core_, i):
            return dot_tn(left[:, part(row, n)], right[:, mul_of(core_, width)])
        return make

    def down_grad(row, n, core_, i):
        start = (row // unit) * 2 * unit + core_ * unit if d.direct else core_ * (fh // 2) + row
        return dot_tn(hid[:, part(start, n)], gdall[:, mul_of(i, CW)])

    ND, NG2, NQ, NO = range(4)
    sets = (
        (down_grad, rc_d, rx_d, rh_d, fh // 2, 128, 128, CHUNKS, stage_d),
        (by_cols(rall, gg2, fh), rc_gu, rx_gu, rh_gu, D, 256, 128, 1, stage),
        (by_cols(xall, gqkv, half_q), rc_q, rx_q, rh_q, D, 256, 256, 1, stage),
        (by_cols(mixed, gaall, D // 2), rc_o, rx_o, None, ha, 128, 128, 1, stage),
    )
    top = hi // (his // 2)

    def half_of(k):
        return sets[k][4] // 2

    def tiles_of(k):
        return half_of(k) // sets[k][5]

    def moves_of(k):
        return half_of(k) // sets[k][6]

    def place(k, j, n):
        count = half_of(k) // n
        if count < 2:
            return j * n
        return ((j + (1 - top) * (count // 2)) % count) * n

    def whole_row(k, j):
        tiles = tiles_of(k)
        late = j // tiles
        return (late * s + (1 - late) * (1 - s)) * half_of(k) + place(k, j % tiles, sets[k][5])

    def cols(k, i):
        return mul_of(i, CW) if sets[k][7] > 1 else pl.ds(0, sets[k][1].shape[1])

    def core_copy(k, j, i, slot):
        buf, n, st = sets[k][1], sets[k][5], sets[k][8]
        row = whole_row(k, j)
        w = CW if sets[k][7] > 1 else buf.shape[1]
        return send(st.at[slot, 0:n, 0:w], buf.at[part(row, n), cols(k, i)], stg_s.at[0 if k == ND else 1, slot],
                    c_r.at[k, (row // n) * sets[k][7] + i], dev_c)

    def give_down(late, i):
        def tile(j):
            slot = 4 * (i % 2) + j
            if i >= 2:
                core_copy(ND, j, i - 2, slot).wait_send()
            stage_d[slot] = down_grad(whole_row(ND, j), 128, 1 - core, i).astype(bf16)
            core_copy(ND, j, i, slot).start()

        n = tiles_of(ND)
        loop(n * (late + 1), tile, n * late)

    before = {NG2: None, NO: NG2, NQ: NO}

    def give(k, j):
        make, buf, n = sets[k][0], sets[k][1], sets[k][5]
        slot = j % 2
        if before[k] is not None:
            @pl.when(j < 2)
            def _():
                core_copy(before[k], j, 0, slot).wait_send()

        if 2 * tiles_of(k) > 2:
            @pl.when(j >= 2)
            def _():
                core_copy(k, j, 0, slot).wait_send()

        stage[slot, 0:n, 0:buf.shape[1]] = make(whole_row(k, j), n, 1 - core, 0).astype(bf16)
        core_copy(k, j, 0, slot).start()

    def x_copy(k, q):
        _, buf, far, _, _, _, m, _, _ = sets[k]
        i, j = q // moves_of(k), q % moves_of(k)
        row = place(k, j, m)
        return send(buf.at[part((1 - s) * half_of(k) + row, m), cols(k, i)], far.at[part(row, m), cols(k, i)],
                    x_s.at[k, q], x_r.at[k, q], dev_x)

    def take(k, j, i=0):
        make, buf, n, m = sets[k][0], sets[k][1], sets[k][5], sets[k][6]
        rows, at = part(whole_row(k, j), n), cols(k, i)
        core_copy(k, j, i, 0).wait_recv()
        buf[rows, at] = (make(whole_row(k, j), n, core, i) + buf[rows, at].astype(f32)).astype(bf16)

        @pl.when(j < tiles_of(k))
        def _():
            for e in range(n // m):
                x_copy(k, i * moves_of(k) + j * (n // m) + e).start()

    def takes(k, j0, j1, i=0):
        loop(j1, lambda j: take(k, j, i), j0)

    def gives(k, j0, j1):
        loop(j1, lambda j: give(k, j), j0)

    def hi_first(k, q):
        _, buf, _, back, _, _, m, _, _ = sets[k]
        per = moves_of(k) // 2
        i, j = q // per, q % per
        other = hi + (his // 2) * (1 - 2 * top)
        return send(buf.at[part(s * half_of(k) + place(k, j, m), m), cols(k, i)], back.at[mul_of(j, m), cols(k, i)],
                    h0_s.at[k, q], h0_r.at[k, q], (s, rep(other, t, core)))

    edge = tz == top
    relays = (relay_d, relay_gu, relay_q)

    def relay_in(k, q):
        _, buf, _, _, _, _, m, _, _ = sets[k]
        per = moves_of(k) // 2
        i, j = q // per, q % per
        return send(buf.at[part(s * half_of(k) + place(k, j, m), m), cols(k, i)], relays[k].at[mul_of(j, m), cols(k, i)],
                    rl_s.at[k, q], rl_r.at[k, q], dev_z)

    def relay_out(k, q):
        _, _, _, back, _, _, m, _, _ = sets[k]
        per = moves_of(k) // 2
        i, j = q // per, q % per
        other = hi + (his // 2) * (1 - 2 * top)
        at = (mul_of(j, m), cols(k, i))
        return send(relays[k].at[at], back.at[at], rf_s.at[k, q], h0_r.at[k, q], (s, rep(other, t_z, core)))

    def hi_send(k, q):
        @pl.when(edge)
        def _():
            relay_in(k, q).start()

        @pl.when(jnp.logical_not(edge))
        def _():
            hi_first(k, q).start()

    def relay(k, q0, q1):
        @pl.when(jnp.logical_not(edge))
        def _():
            def piece(q):
                relay_in(k, q).wait_recv()
                relay_out(k, q).start()

            loop(q1, piece, q0)

    def add_rows(buf, row, far, far_row, n, at, final=None):
        step = min(n, 64)

        def rows_of(j):
            rows = part(row + j * step, step)
            ours, theirs_ = buf[rows, at], far[part(far_row + j * step, step), at]
            if final is None:
                buf[rows, at] = ours + theirs_
            else:
                final[mul_of(j, step), at] = ours.astype(f32) + theirs_.astype(f32)

        loop(n // step, rows_of)

    def x_add(k, q0, q1):
        _, buf, far, _, _, _, m, _, _ = sets[k]

        def piece(q):
            i, j = q // moves_of(k), q % moves_of(k)
            row = place(k, j, m)
            x_copy(k, q).wait_recv()
            add_rows(buf, s * half_of(k) + row, far, row, m, cols(k, i))
            if k != NO:
                @pl.when(j < moves_of(k) // 2)
                def _():
                    hi_send(k, i * (moves_of(k) // 2) + j)

        loop(q1, piece, q0)

    def hi_later(k):
        half = half_of(k)
        base, size, at, out = top * (half // 2), half // 2, half // 2, []
        for level in range(1, d.levels):
            size //= 2
            weight = his >> (level + 1)
            bit = (hi // weight) % 2
            out.append((level - 1, base + (1 - bit) * size, base + bit * size, size, at, hi + weight * (1 - 2 * bit)))
            base = base + bit * size
            at += size
        return out, base, size

    def hi_copy(k, step):
        level, far_row, _, size, at, other = step
        return send(sets[k][1].at[part(s * half_of(k) + far_row, size)], sets[k][3].at[pl.ds(at, size)],
                    h_s.at[k, level], h_r.at[k, level], (s, rep(other, t, core)))

    def hi_finish(k, final=None, then=None):
        _, buf, _, back, _, _, m, chunks, _ = sets[k]
        per = moves_of(k) // 2
        last = final if d.levels == 1 else None

        def piece(q):
            i, j = q // per, q % per
            hi_first(k, q).wait_recv()
            add_rows(buf, s * half_of(k) + place(k, j + per, m), back, j * m, m, cols(k, i), last)
            if then is not None and d.levels == 1:
                loop(m // d.own, lambda e: then(k, q * (m // d.own) + e))

        assert last is None or per == 1
        loop(per * chunks, piece)
        later = hi_later(k)[0]
        for step in later:
            hi_copy(k, step).start()
            hi_copy(k, step).wait_recv()
            add_rows(buf, s * half_of(k) + step[2], back, step[4], step[3], pl.ds(0, buf.shape[1]),
                     final if step is later[-1] else None)

    me = t * CORES + core

    def kept(k, slot):
        return gg2.at[part(slot * d.own, d.own), pl.ds(0, fh) if k == NG2 else pl.ds(fh, half_q)]

    def keep_piece(k, p):
        base = hi_later(k)[1]
        src = sets[k][1].at[part(s * half_of(k) + base + p * d.own, d.own)]

        @pl.when(me != p)
        def _():
            send(src, kept(k, me), a_s.at[k - 1, p], a_r.at[k - 1, me], (s, rep(hi, p // CORES, p % CORES))).start()

        @pl.when(me == p)
        def _():
            pltpu.make_async_copy(src, kept(k, me), a_r.at[k - 1, me]).start()

    def keep_start(k):
        loop(TP * CORES, lambda p: keep_piece(k, p))

    def keep_out(k, p):
        rows = part(p * d.own, d.own)
        if k == NQ:
            for c in range(3):
                e = (p % CORES) * 3 + c
                yield (gg2.at[rows, pl.ds(fh + c * HD, HD)],
                       qkv_h.at[e // 2, :, part(((e % 2) * TP + p // CORES) * HD, HD)])
        elif d.direct:
            w = 2 * unit
            for c in range(d.S * his):
                yield gg2.at[rows, pl.ds(c * w, w)], gu_h.at[p % CORES, :, part((c * TP + p // CORES) * w, w)]
        else:
            yield gg2.at[rows, pl.ds(0, fh)], gu_h.at[p]

    def keep_wait(k):
        def piece(p):
            pltpu.make_async_copy(kept(k, p), kept(k, p), a_r.at[k - 1, p]).wait()
            for src, dst in keep_out(k, p):
                pltpu.make_async_copy(src, dst, ko.at[k - 1, p]).start()

        loop(TP * CORES, piece)

    def keep_end(k):
        def piece(p):
            pltpu.make_async_copy(kept(k, p), kept(k, p), ko.at[k - 1, p]).wait()

            @pl.when(me != p)
            def _():
                send(kept(k, p), kept(k, p), a_s.at[k - 1, p], a_r.at[k - 1, me], (s, rep(hi, p // CORES, p % CORES))).wait_send()

        loop(TP * CORES, piece)

    partners = [dev_y, dev_z, dev_c, dev_x]
    for level in range(d.levels):
        weight = his >> (level + 1)
        bit = (hi // weight) % 2
        partners.append((s, rep(hi + weight * (1 - 2 * bit), t, core)))

    def gain_copy(n):
        return send(gsum, grecv.at[n], gn_s.at[n], gn_r.at[n], partners[n])

    def gain_step(n):
        if n:
            gain_copy(n - 1).wait_send()
            gain_copy(n - 1).wait_recv()
            gsum[...] += grecv[n - 1]
        if n < len(partners):
            gain_copy(n).start()

    ag_start(gdall, 2, 0)
    ag_start(gdall, 2, 1)
    ag_fwd(gdall, 2, 0)
    ag_start(gdall, 2, 2)
    ag_fwd(gdall, 2, 1)
    ag_start(gdall, 2, 3)
    def grad_hidden(i):
        chunk = pl.ds(i * CW, CW)

        def tile(n):
            at = mul_of(n, NT)
            value = dot_nt(gdall[:, chunk], wd[at, chunk])
            acc[:, at] = value if i == 0 else acc[:, at] + value
            value = dot_nt(gdall[:, chunk], wd[part(CW + n * NT, NT), chunk]).reshape(TP, L, NT)
            k2[:, :, at] = value if i == 0 else k2[:, :, at] + value

        loop(CW // NT, tile)

    for i in range(CHUNKS):
        ag_done(gdall, 2, i)
        if i + 2 < CHUNKS:
            ag_fwd(gdall, 2, i + 2)
        give_down(0, i)
        grad_hidden(i)
        if i:
            takes(ND, 0, 2, i - 1)
    ag_drain(gdall, 2)

    def hidden_back(half):
        step = L // 2

        def tile(n):
            at = mul_of(n, NT)
            g_at, u_at = part(half * CW + n * NT, NT), part(fh + half * CW + n * NT, NT)

            def rows_of(j):
                rows = mul_of(j, step)
                g, u = gu[rows, g_at], gu[rows, u_at]
                gh = k2[j // 2, mul_of(j % 2, step), at] if half else acc[rows, at]
                sig = jax.nn.sigmoid(g)
                gg2[rows, g_at] = (gh * u * sig * (1.0 + g * (1.0 - sig))).astype(bf16)
                gg2[rows, u_at] = (gh * (g * sig)).astype(bf16)

            loop(T // step, rows_of)

        loop(CW // NT, tile)

    hidden_back(0)
    hidden_back(1)
    takes(ND, 0, 2, CHUNKS - 1)

    def res_chunk(i):
        acc[...] = dot_nt(gg2[...], wgu[mul_of(i, CW), :])

    def res_extra(i):
        give(NG2, i)

        @pl.when(i > 0)
        def _():
            take(NG2, i - 1)

    def res_between(i):
        if i == 0:
            take(NG2, 3)
            give_down(1, 0)
            give_down(1, 1)
        elif i == 1:
            give_down(1, 2)
            give_down(1, 3)
        else:
            for c in range(CHUNKS):
                takes(ND, 2, 4, c)
            x_add(ND, 0, 4)
            gives(NG2, 4, 8)

    rs(2, cbuf, res_chunk, res_between, res_extra)

    def attn_grad_rows(j):
        rows = mul_of(j, BL)
        gr = cbuf[rows, :] + cot[rows, :].astype(f32)
        cbuf[rows, :] = gr
        a = abuf[rows, :]
        scale = lax.rsqrt(jnp.mean(a * a, axis=-1, keepdims=True) + eps_norm)
        weighted = gr * gat[...]
        inner = jnp.mean(weighted * a, axis=-1, keepdims=True)
        ga = scale * weighted - a * scale**3 * inner
        gaall[part(t * L + j * BL, BL), :] = ga.astype(bf16)
        gsum[:, 0:D] += jnp.sum(gr * a * scale, axis=0, keepdims=True)

    loop(L // BL, attn_grad_rows)

    def attend_back(b):
        rows = blk(b)
        acc[rows, 0:ha] = dot_nt(gaall[rows, :], wo[...])
        scale = columns(2, b)
        cos, sin = cos_v[...], sin_v[...]
        for h in range(heads):
            head = pl.ds(h * HD, HD)
            gm = acc[rows, head].astype(bf16)
            p = probs[b * heads + h]
            gqkv[rows, pl.ds(2 * ha + h * HD, HD)] = dot_tn(p.astype(bf16), gm).astype(bf16)
            gp = dot_nt(gm, vb[rows, head])
            gs = p * (gp - jnp.sum(p * gp, axis=-1, keepdims=True))
            gs = (gs * inv).astype(bf16)
            turned = (dot_nn(gs, qkrot[rows, pl.ds(ha + h * HD, HD)]), dot_tn(gs, qkrot[rows, head]))
            for which in range(2):
                at = pl.ds(which * ha + h * HD, HD)
                gn = turned[which] * cos - pltpu.roll(turned[which], HD // 2, 1) * sin
                field = qk[rows, at]
                spot = part(2 * D + which * d.att + t * ha + h * HD, HD)
                gsum[:, spot] += jnp.sum(gn * field * scale[which], axis=0, keepdims=True)
                gu[rows, at] = gn * gain_of(which, h)

    for i in range(CHUNKS):
        ag_start(gaall, 3, i)
    attend_back(t)
    ag_fwd(gaall, 3, 0)
    takes(NG2, 4, 6)
    ag_fwd(gaall, 3, 1)
    takes(NG2, 6, 8)
    ag_fwd(gaall, 3, 2)
    ag_fwd(gaall, 3, 3)
    x_add(ND, 4, 8)
    relay(ND, 0, 2)
    x_add(NG2, 0, 1)
    loop(2, lambda j: attend_back(t_y + j * (t_z - t_y)))
    for i in range(CHUNKS):
        ag_done(gaall, 3, i)
    attend_back(t_d)
    gain_step(0)
    gives(NO, 0, 2)
    relay(ND, 2, 4)
    ag_drain(gaall, 3)

    def products(rows):
        return gu[rows, 0:2 * ha] * qk[rows, :]

    def in_stat():
        takes(NO, 0, 2)

    stat[3] = stat_sum(1, products, in_stat) / d.att
    gain_step(1)
    x_add(NG2, 1, 3)

    def qk_back(b):
        rows = blk(b)
        scale, inner = columns(2, b), columns(3, b)
        for which in range(2):
            at = pl.ds(which * ha, ha)
            sc = scale[which]
            gqkv[rows, at] = (sc * gu[rows, at] - qk[rows, at] * (sc**3 * inner[which])).astype(bf16)

    loop(TP, qk_back)
    gain_step(2)

    def in_chunk(i):
        acc[...] = dot_nt(gqkv[...], wqkv[mul_of(i, CW), :])

    def in_extra(i):
        give(NQ, i)

        @pl.when(i == 2)
        def _():
            x_add(NG2, 3, 4)

        @pl.when(i > 0)
        def _():
            take(NQ, i - 1)

    def in_between(i):
        if i == 0:
            take(NQ, 3)
            relay(NG2, 0, 2)
            gives(NQ, 4, 8)
            gain_step(3)
        elif i == 1:
            takes(NQ, 4, 8)
            relay(NG2, 2, 3)
        else:
            x_add(NQ, 0, 2)
            gain_step(4)
            relay(NG2, 3, 4)
            x_add(NG2, 4, 8)
            hi_finish(ND, abuf)
            pltpu.make_async_copy(abuf.at[0:unit], down_h, loc.at[4]).start()

    rs(3, bbuf, in_chunk, in_between, in_extra)

    def input_rows(j):
        rows = mul_of(j, BL)
        bbuf[rows, :] += cbuf[rows, :]

    loop(L // BL, input_rows)
    put_gin = pltpu.make_async_copy(bbuf, gin_h, loc.at[5])
    put_gin.start()

    x_add(NQ, 2, 4)
    relay(NQ, 0, 2)
    x_add(NO, 0, 1)

    for p in range(d.pieces):
        o_pc[p] = rc_o[part(s * HD + p * d.own_o, d.own_o), :]
    o_slot = hi * CORES + core

    def o_start(p):
        goal = t * d.pieces + p

        @pl.when(goal != r)
        def _():
            send(o_pc.at[p], o_h.at[o_slot], o_s.at[p], o_r.at[o_slot], (s, goal)).start()

        @pl.when(goal == r)
        def _():
            pltpu.make_async_copy(o_pc.at[p], o_h.at[o_slot], o_r.at[o_slot]).start()

    loop(d.pieces, o_start)
    hi_finish(NG2, None, keep_piece)
    if d.levels > 1:
        keep_start(NG2)
    hi_finish(NQ)
    keep_start(NQ)
    for n in range(5, len(partners) + 1):
        gain_step(n)
    gg_o[...] = gsum[...]

    keep_wait(NG2)
    keep_wait(NQ)
    keep_end(NG2)
    keep_end(NQ)

    def o_wait(q):
        pltpu.make_async_copy(o_pc.at[0], o_pc.at[0], o_r.at[q]).wait()

    loop(his * CORES, o_wait)

    def o_sent(p):
        goal = t * d.pieces + p

        @pl.when(goal != r)
        def _():
            send(o_pc.at[p], o_h.at[o_slot], o_s.at[p], o_r.at[o_slot], (s, goal)).wait_send()

    loop(d.pieces, o_sent)
    far_gain.wait_send()
    for k in range(NG):
        cross(k).wait_send()
        share(k).wait_send()
    for i in range(CHUNKS - 2, CHUNKS):
        loop(2 * tiles_of(ND), lambda j: core_copy(ND, j, i, 4 * (i % 2) + j).wait_send())
    for slot in range(2):
        core_copy(NQ, slot, 0, slot).wait_send()
    for k in range(4):
        loop(moves_of(k) * sets[k][7], lambda q: x_copy(k, q).wait_send())
    for k in range(3):
        @pl.when(edge)
        def _():
            loop(moves_of(k) // 2 * sets[k][7], lambda q: relay_in(k, q).wait_send())

        @pl.when(jnp.logical_not(edge))
        def _():
            loop(moves_of(k) // 2 * sets[k][7], lambda q: (hi_first(k, q).wait_send(), relay_out(k, q).wait_send()))

        for step in hi_later(k)[0]:
            hi_copy(k, step).wait_send()
    put_out.wait()
    put_gin.wait()
    pltpu.make_async_copy(abuf.at[0:unit], down_h, loc.at[4]).wait()


def body(shards, replicas, x_in, cotangent, w_query, w_key, w_value, w_out, w_gate, w_up, w_down,
         gain_query, gain_key, gain_attn, gain_mlp):
    seqs, length, width = x_in.shape
    assert seqs == 1
    d = Dims(length, width, w_query.shape[1], w_gate.shape[1], shards, replicas)
    r = lax.axis_index("replica")
    s = lax.axis_index("shard")
    t = (r // CORES) % TP

    def at(array, axis, index):
        return lax.dynamic_index_in_dim(array, index, axis, keepdims=False)

    def hidden_cols(w):
        picked = at(w.reshape(w.shape[0], d.S, d.his, TP, CORES, d.unit), 3, t)
        return picked.transpose(0, 3, 1, 2, 4).reshape(w.shape[0], d.fh)

    if not d.direct:
        w_gate = jnp.concatenate([hidden_cols(w_gate), hidden_cols(w_up)], axis=1)
        w_down = at(w_down.reshape(d.his, TP, CORES, d.unit, width), 1, t).transpose(1, 0, 2, 3).reshape(-1, width)
    gain = jnp.concatenate([at(gain_query.reshape(TP, HD), 0, t), at(gain_key.reshape(TP, HD), 0, t),
                            gain_attn, gain_mlp]).astype(f32)[None]
    cos, sin = rope_tables(length, HD // 2)
    cos = np.concatenate([cos, cos], axis=1)
    sin = np.concatenate([-sin, sin], axis=1)

    L, D, T, ha, fh = d.L, d.D, d.T, d.ha, d.fh
    CW = D // CHUNKS
    vm = pltpu.VMEM
    dma = pltpu.SemaphoreType.DMA
    any_ = pl.BlockSpec(memory_space=pl.ANY)
    vmem = pl.BlockSpec(memory_space=pltpu.VMEM)
    hi_rows = lambda n: max(n - n // d.his, 16)
    steps = 4 + d.levels
    later = max(d.levels - 1, 1)
    scratch = [
        vm((D, 3 * ha), bf16), vm((ha, D), bf16), vm((D, 2 * fh), bf16), vm((fh, D), bf16),
        vm((2, 1, d.gains), f32), vm((1, D), f32), vm((1, D), f32),
        vm((T, D), bf16), vm((T, D), bf16), vm((T, D), bf16), vm((T, D), bf16), vm((L, D), bf16),
        vm((T, 2 * ha), f32), vm((T, ha), bf16), vm((T, 2 * ha), bf16), vm((TP * ha // HD, L, L), f32),
        vm((T, ha), bf16), vm((T, 3 * ha), bf16), vm((4, 8, T), f32), vm((2, 3, 8, T), f32),
        vm((T, 2 * fh), f32), vm((T, fh), bf16), vm((T, 2 * fh), bf16),
        vm((L, D), f32), vm((L, D), f32), vm((L, D), f32), vm((L, D), bf16),
        vm((T, CW), f32), vm((CHUNKS, 2, L, CW), bf16), vm((CHUNKS, L, CW), bf16),
        vm((CHUNKS, 2, L, CW), bf16), vm((CHUNKS, L, CW), bf16), vm((CHUNKS, L, CW), f32),
        vm((8, 128, CW), bf16), vm((2, 256, fh), bf16),
        vm((D, fh), bf16), vm((fh // 2, D), bf16), vm((D, 3 * ha // 2), bf16), vm((ha, D // 2), bf16),
        vm((D // 2, fh), bf16), vm((fh // 4, D), bf16), vm((D // 2, 3 * ha // 2), bf16), vm((ha // 2, D // 2), bf16),
        vm((hi_rows(D // 2), fh), bf16), vm((hi_rows(fh // 4), D), bf16), vm((hi_rows(D // 2), 3 * ha // 2), bf16),
        vm((d.pieces, d.own_o, D // 2), bf16),
        vm((1, d.ggs), f32), vm((steps, 1, d.ggs), f32),
        dma((4, CHUNKS, 4)), dma((4, CHUNKS, 4)), dma((4, CHUNKS, 4)), dma((4, CHUNKS, 4)),
        dma((11,)), dma((11,)), dma((10,)), dma((10,)), dma((10, 2)), dma((6,)), dma((2, 3)), dma((2, 3)),
        dma((2, 8)), dma((4, 16)), dma((4, 8)), dma((4, 8)), dma((3, 4)), dma((3, 4)), dma((3, 4)), dma((3, 4)), dma((3, 4)),
        dma((3, later)), dma((3, later)),
        dma((2, TP * CORES)), dma((2, TP * CORES)), dma((2, TP * CORES)), dma((d.pieces,)), dma((d.his * CORES,)), dma((steps,)), dma((steps,)),
    ]
    struct = jax.ShapeDtypeStruct
    gu_shape = (2, d.own, d.ff) if d.direct else (TP * CORES, d.own, fh)
    results = pl.pallas_call(
        functools.partial(kernel, d),
        out_shape=(
            struct((L, D), bf16), struct((L, D), f32), struct(gu_shape, bf16), struct((3, d.own, d.att), bf16),
            struct((d.unit, D), f32), struct((d.his * CORES, d.own_o, D // 2), bf16),
            struct((fh // 8, D), bf16), struct((D // 4, fh), bf16), struct((D // 4, 3 * ha // 2), bf16),
            struct((1, d.ggs), f32),
        ),
        in_specs=[any_] * 9 + [vmem] * 3,
        out_specs=(any_,) * 9 + (vmem,),
        scratch_shapes=scratch,
        compiler_params=pltpu.CompilerParams(
            collective_id=0, has_side_effects=True, vmem_limit_bytes=67043328),
        name="layer",
    )(x_in[0], cotangent[0], w_query, w_key, w_value, w_out, w_gate, w_up, w_down, gain, cos, sin)
    out, gin, gu, qkv, down, o = results[:6]
    gg = results[-1]

    def hidden_out(k):
        if d.direct:
            return gu[k].astype(f32)
        block = gu.reshape(TP, CORES, d.own, fh)[:, k]
        spread = block.reshape(TP, d.own, CORES, d.S, d.his, d.unit).transpose(1, 3, 4, 0, 2, 5)
        return spread.reshape(d.own, d.ff).astype(f32)

    o = o.reshape(d.his, CORES, d.own_o, D // 2).astype(f32).sum(0).transpose(1, 0, 2).reshape(d.own_o, D)
    gg = gg[0]
    here = s * d.R + r

    def share(vec):
        n = vec.shape[0] // (d.S * d.R)
        return lax.dynamic_slice_in_dim(vec, here * n, n)

    def head_gain(vec):
        return share(vec.reshape(TP, d.S, HD).transpose(1, 0, 2).reshape(-1))

    return (
        out[None], gin[None], qkv[0].astype(f32), qkv[1].astype(f32), qkv[2].astype(f32), o,
        hidden_out(0), hidden_out(1), down,
        head_gain(gg[2 * D:2 * D + d.att]), head_gain(gg[2 * D + d.att:]), share(gg[:D]), share(gg[D:2 * D]),
    )


def solution(mesh):
    both = ("shard", "replica")
    token = P(both, None, None)
    weight = P("shard", None)
    return jax.shard_map(
        functools.partial(body, mesh.shape["shard"], mesh.shape["replica"]),
        mesh=mesh,
        in_specs=(token, token) + (weight,) * 7 + (P("shard"),) * 4,
        out_specs=(token, token) + (P(both, None),) * 7 + (P(both),) * 4,
        check_vma=False,
    )
```
